16 devices in a mesh: cp: 16 (over z, y, x, core).
Axes of the slice: x: 2, y: 2, z: 2, core: 2. Of those that a mesh axis runs over, the one named last changes fastest.
Arguments:
- queries: bfloat16 [4096, 16, 192], P('cp')
- latent: bfloat16 [4096, 512], P('cp')
- key_rope: bfloat16 [4096, 64], P('cp')
- w_uk: bfloat16 [512, 16, 128], replicated
- w_uv: bfloat16 [512, 16, 128], replicated
- d_out: bfloat16 [4096, 16, 128], P('cp')
Outputs:
- output 1: bfloat16 [4096, 16, 128], P('cp')
- output 2: bfloat16 [4096, 16, 192], P('cp')
- output 3: bfloat16 [4096, 512], P('cp')
- output 4: bfloat16 [4096, 64], P('cp')
- output 5: float32 [512, 16, 128], replicated
- output 6: float32 [512, 16, 128], replicated
All inputs are finite; a program needn't handle non-finite values.
Results may differ from the reference program's by a relative error of at most 0.016657.
Values are sent between devices in bfloat16 or wider.
A program may use at most 1 GiB of HBM per device.

```python
import math
import jax
import jax.numpy as jnp
from jax import lax

TOK_DEV = 256
N_DEV = 16
N_HEADS = 16
LATENT = 512
NOPE_DIM = 128
ROPE_DIM = 64
V_DIM = 128

SEQ_LEN = TOK_DEV * N_DEV
QK_DIM = NOPE_DIM + ROPE_DIM
SOFT_SCALE = 1.0 / math.sqrt(QK_DIM)
Q_SPREAD = math.sqrt(0.75 * math.log(SEQ_LEN))


def setup_inputs(seed: int = 0) -> dict:
    rng_keys = jax.random.split(jax.random.key(seed), 6)
    queries = jax.random.normal(rng_keys[0], (SEQ_LEN, N_HEADS, QK_DIM), jnp.float32) * Q_SPREAD
    latent = jax.random.normal(rng_keys[1], (SEQ_LEN, LATENT), jnp.float32)
    key_rope = jax.random.normal(rng_keys[2], (SEQ_LEN, ROPE_DIM), jnp.float32)
    w_uk = jax.random.normal(rng_keys[3], (LATENT, N_HEADS, NOPE_DIM), jnp.float32) * LATENT ** -0.5
    w_uv = jax.random.normal(rng_keys[4], (LATENT, N_HEADS, V_DIM), jnp.float32) * LATENT ** -0.5
    d_out = jax.random.normal(rng_keys[5], (SEQ_LEN, N_HEADS, V_DIM), jnp.float32)
    return {
        "queries": queries.astype(jnp.bfloat16),
        "latent": latent.astype(jnp.bfloat16),
        "key_rope": key_rope.astype(jnp.bfloat16),
        "w_uk": w_uk.astype(jnp.bfloat16),
        "w_uv": w_uv.astype(jnp.bfloat16),
        "d_out": d_out.astype(jnp.bfloat16),
    }


def decompress(latent, w_uk, w_uv):
    lat_f = latent.astype(jnp.float32)
    k_nope = jnp.einsum("tl,lhd->thd", lat_f, w_uk.astype(jnp.float32)).astype(jnp.bfloat16)
    values = jnp.einsum("tl,lhd->thd", lat_f, w_uv.astype(jnp.float32)).astype(jnp.bfloat16)
    return k_nope, values


def attend(queries, latent, key_rope, w_uk, w_uv):
    k_nope, values = decompress(latent, w_uk, w_uv)
    k_f = k_nope.astype(jnp.float32)
    v_f = values.astype(jnp.float32)
    r_f = key_rope.astype(jnp.float32)
    key_pos = jnp.arange(SEQ_LEN)

    def block_rows(blk_pair):
        q_blk, q_start = blk_pair
        q_f = q_blk.astype(jnp.float32)
        scores = (jnp.einsum("qhd,khd->hqk", q_f[:, :, :NOPE_DIM], k_f)
                  + jnp.einsum("qhd,kd->hqk", q_f[:, :, NOPE_DIM:], r_f)) * SOFT_SCALE
        q_pos = q_start + jnp.arange(TOK_DEV)
        visible = key_pos[None, :] <= q_pos[:, None]
        scores = jnp.where(visible[None], scores, -1e30)
        attn_prob = jax.nn.softmax(scores, axis=-1)
        return jnp.einsum("hqk,khd->qhd", attn_prob, v_f)

    q_blocks = queries.reshape(N_DEV, TOK_DEV, N_HEADS, QK_DIM)
    q_starts = jnp.arange(N_DEV) * TOK_DEV
    out_rows = lax.map(jax.checkpoint(block_rows), (q_blocks, q_starts))
    return out_rows.reshape(SEQ_LEN, N_HEADS, V_DIM).astype(jnp.bfloat16)


def reference(queries, latent, key_rope, w_uk, w_uv, d_out):
    attn_out, pull_back = jax.vjp(attend, queries, latent, key_rope, w_uk.astype(jnp.float32), w_uv.astype(jnp.float32))
    d_query, d_latent, d_key_rope, d_w_uk, d_w_uv = pull_back(d_out)
    return (attn_out, d_query.astype(jnp.bfloat16), d_latent.astype(jnp.bfloat16), d_key_rope.astype(jnp.bfloat16), d_w_uk, d_w_uv)
```

```python
import math
import jax
import jax.numpy as jnp
from jax import lax
from jax.experimental import pallas as pl
from jax.experimental.pallas import tpu as pltpu
from jax.sharding import PartitionSpec as P

MESH = pl.DeviceIdType.MESH
BF16 = jnp.bfloat16
F32 = jnp.float32

N = 16
T = 256
L = 512
D = 128
R = 64
QK = D + R
TK = 512
NT = 8
C_CHUNK = 96
W_CHUNK = 344
SCALE = 1.0 / math.sqrt(QK)
EXP_C = SCALE * math.log2(math.e)


def nt_dot(a, b):
    return lax.dot_general(a, b, (((1,), (1,)), ((), ())), preferred_element_type=F32)


def nn_dot(a, b):
    return lax.dot_general(a, b, (((1,), (0,)), ((), ())), preferred_element_type=F32)


def flip(x, bit):
    return x + bit * (1 - 2 * lax.rem(lax.div(x, bit), 2))


def xor(x, s):
    for bit in (1, 2, 4, 8):
        on = lax.rem(lax.div(s, bit), 2)
        x = x + on * bit * (1 - 2 * lax.rem(lax.div(x, bit), 2))
    return x


def fold(x, reduce):
    return reduce(x.reshape(x.shape[0] // 8, 8, x.shape[1]), axis=0)


def transpose(x):
    return jnp.transpose(x, (1, 0))


class Gather:
    def __init__(self, me, own, buf, chunk, send_sem, recv_sem, sib_send, sib_recv):
        self.me, self.own, self.buf, self.chunk = me, own, buf, chunk
        self.send_sem, self.recv_sem = send_sem, recv_sem
        self.sib_send, self.sib_recv = sib_send, sib_recv

    def axes(self, k):
        out = []
        for t in range(3):
            axis = lax.rem(k + t, 3)
            out.append(2 + axis * (axis + 1))
        return out

    def make(self, k, masks, mask, target, send_sem, recv_sem):
        src = self.me
        for bit in masks:
            src = flip(src, bit)
        rows = pl.ds(k * self.chunk, self.chunk)
        slot = k * 8 + lax.div(mask, 2)
        first = self.own.at[rows, :] if not masks else self.buf.at[src, rows, :]
        return pltpu.make_async_remote_copy(
            src_ref=first, dst_ref=self.buf.at[src, rows, :], send_sem=send_sem.at[slot], recv_sem=recv_sem.at[slot],
            device_id=(target,), device_id_type=MESH)

    def hop(self, k, masks, bit):
        return self.make(k, masks, sum(masks) + bit, flip(self.me, bit), self.send_sem, self.recv_sem)

    def sib(self, k, masks):
        return self.make(k, masks, sum(masks), flip(self.me, 1), self.sib_send, self.sib_recv)

    def arrived(self, k, masks):
        self.make(k, masks, sum(masks), flip(self.me, 1), self.send_sem, self.recv_sem).wait_recv()

    def stage0(self):
        for t in range(3):
            def send(k, carry):
                self.hop(k, (), self.axes(k)[t]).start()
                return carry
            lax.fori_loop(0, 3, send, 0)

        def send_sib(k, carry):
            self.sib(k, ()).start()
            return carry
        lax.fori_loop(0, 3, send_sib, 0)

    def stage1(self):
        def step(k, carry):
            a, b, c = self.axes(k)
            self.arrived(k, (a,))
            self.hop(k, (a,), b).start()
            self.hop(k, (a,), c).start()
            self.sib(k, (a,)).start()
            return carry
        lax.fori_loop(0, 3, step, 0)

    def stage2(self):
        for both in (False, True):
            def step(k, carry):
                a, b, c = self.axes(k)
                masks = (a, b) if both else (b,)
                self.arrived(k, masks)
                self.hop(k, masks, c).start()
                self.sib(k, masks).start()
                return carry
            lax.fori_loop(0, 3, step, 0)

    def stage3(self):
        for extra in range(4):
            def step(k, carry):
                a, b, c = self.axes(k)
                masks = ((c,), (a, c), (b, c), (a, b, c))[extra]
                self.arrived(k, masks)
                self.sib(k, masks).start()
                return carry
            lax.fori_loop(0, 3, step, 0)

    def finish(self):
        sibling = flip(self.me, 1)

        def step(n, carry):
            k, half = lax.div(n, 8), lax.rem(n, 8)
            rows = pl.ds(k * self.chunk, self.chunk)
            ref = self.buf.at[xor(sibling, 2 * half), rows, :]
            pltpu.make_async_remote_copy(
                src_ref=ref, dst_ref=ref, send_sem=self.sib_send.at[n], recv_sem=self.sib_recv.at[n],
                device_id=(sibling,), device_id_type=MESH).wait_recv()
            return carry
        lax.fori_loop(0, 24, step, 0)

    def drain(self):
        def step(n, carry):
            k, half = lax.div(n, 8), lax.rem(n, 8)
            rows = pl.ds(k * self.chunk, self.chunk)
            ref = self.buf.at[xor(self.me, 2 * half), rows, :]
            pltpu.make_async_remote_copy(
                src_ref=ref, dst_ref=ref, send_sem=self.sib_send.at[n], recv_sem=self.sib_recv.at[n],
                device_id=(flip(self.me, 1),), device_id_type=MESH).wait_send()

            @pl.when(half > 0)
            def _():
                pltpu.make_async_remote_copy(
                    src_ref=ref, dst_ref=ref, send_sem=self.send_sem.at[n], recv_sem=self.recv_sem.at[n],
                    device_id=(flip(self.me, 1),), device_id_type=MESH).wait_send()
            return carry
        lax.fori_loop(0, 24, step, 0)


def kernel(qt_ref, do_ref, c_ref, rt_ref, wuk_ref, wuv_ref,
           o_ref, dq_ref, dc_ref, drt_ref, dw_ref,
           in_q, in_do, stage_o, stage_dq, stage_g, in_g, call, kcat, kt, v, vt, sbuf, qz, dk, dv, ot, dqt, wuk, wuv, dw_own,
           q_send, q_recv, do_send, do_recv, o_send, o_recv, dq_send, dq_recv, g_send, g_recv, local_sem,
           c_send, c_recv, cs_send, cs_recv, w_send, w_recv, ws_send, ws_recv):
    me = lax.axis_index("cp")

    loads = [
        pltpu.make_async_copy(wuk_ref, wuk, local_sem.at[0]),
        pltpu.make_async_copy(wuv_ref, wuv, local_sem.at[1]),
        pltpu.make_async_copy(c_ref, call.at[me, pl.ds(0, T), :], local_sem.at[2]),
        pltpu.make_async_copy(rt_ref.at[pl.ds(0, 32), :], call.at[me, pl.ds(T, 32), pl.ds(0, T)], local_sem.at[3]),
        pltpu.make_async_copy(rt_ref.at[pl.ds(32, 32), :], call.at[me, pl.ds(T, 32), pl.ds(T, T)], local_sem.at[4]),
    ]
    for load in loads[::-1]:
        load.start()

    barrier = pltpu.get_barrier_semaphore()

    def hello(s, carry):
        pl.semaphore_signal(barrier, inc=1, device_id=(xor(me, s),), device_id_type=MESH)
        return carry

    lax.fori_loop(1, N, hello, 0)
    for load in loads[2:]:
        load.wait()
    pl.semaphore_wait(barrier, N - 1)

    def send(src, dst, s, send_sem, recv_sem):
        return pltpu.make_async_remote_copy(
            src_ref=src, dst_ref=dst.at[me], send_sem=send_sem.at[s], recv_sem=recv_sem.at[me],
            device_id=(xor(me, s),), device_id_type=MESH)

    def take(src, dst, other, send_sem, recv_sem):
        pltpu.make_async_remote_copy(
            src_ref=src, dst_ref=dst.at[other], send_sem=send_sem.at[0], recv_sem=recv_sem.at[other],
            device_id=(flip(me, 1),), device_id_type=MESH).wait_recv()

    gather_c = Gather(me, call.at[me], call, C_CHUNK, c_send, c_recv, cs_send, cs_recv)
    gather_c.stage0()
    pltpu.make_async_copy(qt_ref.at[me], in_q.at[me], q_recv.at[me]).start()
    pltpu.make_async_copy(do_ref.at[me], in_do.at[me], do_recv.at[me]).start()
    dk[...] = jnp.zeros_like(dk)
    dv[...] = jnp.zeros_like(dv)
    qz[...] = jnp.zeros_like(qz)
    dw_own[...] = jnp.zeros_like(dw_own)
    gather_c.stage1()
    gather_c.stage2()

    def send_q(s, carry):
        other = xor(me, s)
        send(qt_ref.at[other], in_q, s, q_send, q_recv).start()
        send(do_ref.at[other], in_do, s, do_send, do_recv).start()
        return carry

    lax.fori_loop(1, N, send_q, 0)
    for load in loads[:2]:
        load.wait()
    gather_c.stage3()
    gather_c.finish()

    lanes = pl.ds(pl.multiple_of(me * D, D), D)

    def make_kv(jt, carry):
        wcat = jnp.concatenate([wuk[:, lanes], wuv[:, lanes]], axis=1)
        for half in range(2):
            j = jt * 2 + half
            rows = pl.ds(half * T, T)
            kv = nn_dot(call[j, pl.ds(0, T), :], wcat)
            rt = jnp.concatenate([call[j, pl.ds(T, 32), pl.ds(0, T)], call[j, pl.ds(T, 32), pl.ds(T, T)]], axis=0)
            rtz = jnp.concatenate([rt.astype(F32), jnp.zeros((R, T), F32)], axis=0)
            kcat[jt, rows, pl.ds(0, D)] = kv[:, :D].astype(BF16)
            kcat[jt, rows, pl.ds(D, D)] = transpose(rtz).astype(BF16)
            v[jt, rows, :] = kv[:, D:].astype(BF16)
            kvt = transpose(kv).astype(BF16)
            kt[jt, pl.ds(0, D), rows] = kvt[:D]
            kt[jt, pl.ds(D, R), rows] = rt
            vt[jt, :, rows] = kvt[D:]
        return carry

    lax.fori_loop(0, NT, make_kv, 0)

    def q_step(s, carry):
        i = xor(me, s)
        take(qt_ref.at[i], in_q, i, q_send, q_recv)
        take(do_ref.at[i], in_do, i, do_send, do_recv)
        last = lax.div(i, 2)
        qz[pl.ds(0, QK), :] = in_q[i]

        def score_tile(jt, top):
            sc = nn_dot(kcat[jt], qz[...])
            sbuf[jt] = sc
            return jnp.maximum(top, fold(sc, jnp.max))

        top = lax.fori_loop(0, last, score_tile, jnp.full((8, T), -1e30, F32))
        sc = nn_dot(kcat[last], qz[...])
        ahead = lax.broadcasted_iota(jnp.int32, sc.shape, 0) - lax.broadcasted_iota(jnp.int32, sc.shape, 1)
        sc = jnp.where(ahead <= i * T - last * TK, sc, -1e30)
        sbuf[last] = sc
        top = jnp.maximum(top, fold(sc, jnp.max))
        top = jnp.max(top, axis=0, keepdims=True) * EXP_C

        ot[...] = jnp.zeros_like(ot)

        def soft_tile(jt, total):
            e = jnp.exp2(sbuf[jt] * EXP_C - top)
            sbuf[jt] = e
            ot[...] += nn_dot(vt[jt], e.astype(BF16))
            return total + fold(e, jnp.sum)

        total = lax.fori_loop(0, last + 1, soft_tile, jnp.zeros((8, T), F32))
        inv = 1.0 / jnp.sum(total, axis=0, keepdims=True)
        o_t = ot[...] * inv
        stage_o[s] = transpose(o_t).astype(BF16)

        @pl.when(s > 0)
        def _():
            send(stage_o.at[s], o_ref, s, o_send, o_recv).start()

        do_t = transpose(in_do[i].astype(F32))
        delta = jnp.sum(o_t * do_t, axis=0, keepdims=True)
        dqt[...] = jnp.zeros_like(dqt)

        def back_tile(jt, c):
            do = in_do[i]
            dp = nt_dot(v[jt], do)
            p = sbuf[jt] * inv
            ds = (p * (dp - delta)).astype(BF16)
            dv[jt] += nn_dot(p.astype(BF16), do)
            dk[jt] += nt_dot(ds, qz[...])
            dqt[...] += nn_dot(kt[jt], ds)
            return c

        lax.fori_loop(0, last + 1, back_tile, 0)
        stage_dq[s] = (dqt[...] * SCALE).astype(BF16)

        @pl.when(s > 0)
        def _():
            send(stage_dq.at[s], dq_ref, s, dq_send, dq_recv).start()

        return carry

    lax.fori_loop(0, N, q_step, 0)
    pltpu.make_async_copy(stage_o.at[0], o_ref.at[me], o_recv.at[me]).start()
    pltpu.make_async_copy(stage_dq.at[0], dq_ref.at[me], dq_recv.at[me]).start()

    def grad_kv(s, carry):
        i = xor(me, s)
        rows = pl.ds(pl.multiple_of(lax.rem(i, 2) * T, T), T)
        key = dk[lax.div(i, 2), rows, :] * SCALE
        stage_g[s, pl.ds(0, T), pl.ds(0, D)] = key[:, :D].astype(BF16)
        stage_g[s, pl.ds(0, T), pl.ds(D, D)] = dv[lax.div(i, 2), rows, :].astype(BF16)
        stage_g[s, pl.ds(T, R), :] = transpose(key[:, D:])[:R].astype(BF16)

        @pl.when(s > 0)
        def _():
            send(stage_g.at[s], in_g, s, g_send, g_recv).start()

        return carry

    lax.fori_loop(0, N, grad_kv, 0)
    pltpu.make_async_copy(stage_g.at[0], in_g.at[me], g_recv.at[me]).start()

    def grad_w(s, acc):
        both_t = transpose(stage_g[s, pl.ds(0, T), :].astype(F32)).astype(BF16)
        return acc + nn_dot(both_t, call[xor(me, s), pl.ds(0, T), :])

    dwt = lax.fori_loop(0, N, grad_w, jnp.zeros((2 * D, L), F32))
    dw_own[pl.ds(0, L), :] = transpose(dwt[:D])
    dw_own[pl.ds(L, L), :] = transpose(dwt[D:])
    own_w = pltpu.make_async_copy(dw_own, dw_ref.at[me], local_sem.at[5])
    own_w.start()
    gather_w = Gather(me, dw_own, dw_ref, W_CHUNK, w_send, w_recv, ws_send, ws_recv)
    gather_w.stage0()
    gather_w.stage1()
    gather_w.stage2()

    def take_g(h, carry):
        take(stage_g.at[0], in_g, h, g_send, g_recv)
        return carry

    lax.fori_loop(0, N, take_g, 0)

    def latent_grad(h, acc):
        cols = pl.ds(pl.multiple_of(h * D, D), D)
        wcat = jnp.concatenate([wuk[:, cols], wuv[:, cols]], axis=1)
        return acc + nt_dot(in_g[h, pl.ds(0, T), :], wcat)

    dc_ref[...] = lax.fori_loop(0, N, latent_grad, jnp.zeros((T, L), F32)).astype(BF16)

    def rope_grad(h, acc):
        return acc + in_g[h, pl.ds(T, R), :].astype(F32)

    drt_ref[...] = lax.fori_loop(0, N, rope_grad, jnp.zeros((R, T), F32)).astype(BF16)

    gather_w.stage3()
    gather_w.finish()
    own_w.wait()

    def take_o(h, carry):
        take(stage_o.at[0], o_ref, h, o_send, o_recv)
        take(stage_dq.at[0], dq_ref, h, dq_send, dq_recv)
        return carry

    lax.fori_loop(0, N, take_o, 0)

    def drain(s, carry):
        other = xor(me, s)
        send(qt_ref.at[other], in_q, s, q_send, q_recv).wait_send()
        send(do_ref.at[other], in_do, s, do_send, do_recv).wait_send()
        send(stage_o.at[s], o_ref, s, o_send, o_recv).wait_send()
        send(stage_dq.at[s], dq_ref, s, dq_send, dq_recv).wait_send()
        send(stage_g.at[s], in_g, s, g_send, g_recv).wait_send()
        return carry

    lax.fori_loop(1, N, drain, 0)
    gather_c.drain()
    gather_w.drain()


def solution(mesh):
    seq_spec = P("cp")

    def local_step(queries, latent, key_rope, w_uk, w_uv, d_out):
        any_spec = pl.BlockSpec(memory_space=pl.ANY)
        vmem_spec = pl.BlockSpec(memory_space=pltpu.VMEM)
        dma = pltpu.SemaphoreType.DMA
        o_all, dq_all, dc, drt, dw = pl.pallas_call(
            kernel,
            name="mla_core",
            out_shape=(jax.ShapeDtypeStruct((N, T, D), BF16),
                       jax.ShapeDtypeStruct((N, QK, T), BF16),
                       jax.ShapeDtypeStruct((T, L), BF16),
                       jax.ShapeDtypeStruct((R, T), BF16),
                       jax.ShapeDtypeStruct((N, 3 * W_CHUNK, D), F32)),
            in_specs=[any_spec] * 6,
            out_specs=(any_spec, any_spec, vmem_spec, vmem_spec, any_spec),
            scratch_shapes=[
                pltpu.VMEM((N, QK, T), BF16),
                pltpu.VMEM((N, T, D), BF16),
                pltpu.VMEM((N, T, D), BF16),
                pltpu.VMEM((N, QK, T), BF16),
                pltpu.VMEM((N, T + R, 2 * D), BF16),
                pltpu.VMEM((N, T + R, 2 * D), BF16),
                pltpu.VMEM((N, 3 * C_CHUNK, L), BF16),
                pltpu.VMEM((NT, TK, 2 * D), BF16),
                pltpu.VMEM((NT, QK, TK), BF16),
                pltpu.VMEM((NT, TK, D), BF16),
                pltpu.VMEM((NT, D, TK), BF16),
                pltpu.VMEM((NT, TK, T), F32),
                pltpu.VMEM((2 * D, T), BF16),
                pltpu.VMEM((NT, TK, 2 * D), F32),
                pltpu.VMEM((NT, TK, D), F32),
                pltpu.VMEM((D, T), F32),
                pltpu.VMEM((QK, T), F32),
                pltpu.VMEM((L, N * D), BF16),
                pltpu.VMEM((L, N * D), BF16),
                pltpu.VMEM((3 * W_CHUNK, D), F32),
            ] + [dma((N,))] * 10 + [dma((6,))] + [dma((24,))] * 8,
            compiler_params=pltpu.CompilerParams(
                collective_id=0, has_side_effects=True, vmem_limit_bytes=60 * 1024 * 1024),
        )(jnp.transpose(queries, (1, 2, 0)), jnp.transpose(d_out, (1, 0, 2)), latent, jnp.transpose(key_rope, (1, 0)),
          w_uk.reshape(L, N * D), w_uv.reshape(L, N * D))

        d_w = jnp.transpose(dw[:, :2 * L], (1, 0, 2))
        return (jnp.transpose(o_all, (1, 0, 2)), jnp.transpose(dq_all, (2, 0, 1)), dc, jnp.transpose(drt, (1, 0)),
                d_w[:L], d_w[L:])

    return jax.shard_map(local_step, mesh=mesh,
                         in_specs=(seq_spec, seq_spec, seq_spec, P(), P(), seq_spec),
                         out_specs=(seq_spec, seq_spec, seq_spec, seq_spec, P(), P()),
                         check_vma=False)
```

```python
import math
import jax
import jax.numpy as jnp
from jax import lax
from jax.experimental import pallas as pl
from jax.experimental.pallas import tpu as pltpu
from jax.sharding import PartitionSpec as P

MESH = pl.DeviceIdType.MESH
BF16 = jnp.bfloat16
F32 = jnp.float32

N = 16
T = 256
L = 512
D = 128
R = 64
QK = D + R
TK = 512
NT = 8
C_CHUNK = 96
W_CHUNK = 176
NP = 72
ORDER = (0, 7, 3, 4, 5, 2, 6, 1)
TABLE = sum(chip << (3 * n) for n, chip in enumerate(ORDER))
SCALE = 1.0 / math.sqrt(QK)
EXP_C = SCALE * math.log2(math.e)


def nt_dot(a, b):
    return lax.dot_general(a, b, (((1,), (1,)), ((), ())), preferred_element_type=F32)


def nn_dot(a, b):
    return lax.dot_general(a, b, (((1,), (0,)), ((), ())), preferred_element_type=F32)


def flip(x, bit):
    return x + bit * (1 - 2 * lax.rem(lax.div(x, bit), 2))


def xor(x, s):
    for bit in (1, 2, 4, 8):
        on = lax.rem(lax.div(s, bit), 2)
        x = x + on * bit * (1 - 2 * lax.rem(lax.div(x, bit), 2))
    return x


def partner(n):
    k = lax.div(n, 2)
    power = (1 + 7 * lax.rem(k, 2)) * (1 + 63 * lax.rem(lax.div(k, 2), 2)) * (1 + 4095 * lax.div(k, 4))
    return 2 * lax.rem(lax.div(TABLE, power), 8) + lax.rem(n, 2)


def fold(x, reduce):
    return reduce(x.reshape(x.shape[0] // 8, 8, x.shape[1]), axis=0)


def transpose(x):
    return jnp.transpose(x, (1, 0))


class Gather:
    def __init__(self, me, own, view, chunk, send_sem, recv_sem, sib_send, sib_recv):
        self.me, self.own, self.view, self.chunk = me, own, view, chunk
        self.send_sem, self.recv_sem = send_sem, recv_sem
        self.sib_send, self.sib_recv = sib_send, sib_recv

    def axes(self, k):
        out = []
        for t in range(3):
            axis = lax.rem(k + t, 3)
            out.append(2 + axis * (axis + 1))
        return out

    def make(self, k, masks, mask, target, send_sem, recv_sem):
        src = self.me
        for bit in masks:
            src = flip(src, bit)
        rows = pl.ds(k * self.chunk, self.chunk)
        slot = k * 8 + lax.div(mask, 2)
        first = self.own.at[rows, :] if not masks else self.view(src, rows)
        return pltpu.make_async_remote_copy(
            src_ref=first, dst_ref=self.view(src, rows), send_sem=send_sem.at[slot], recv_sem=recv_sem.at[slot],
            device_id=(target,), device_id_type=MESH)

    def hop(self, k, masks, bit):
        return self.make(k, masks, sum(masks) + bit, flip(self.me, bit), self.send_sem, self.recv_sem)

    def sib(self, k, masks):
        return self.make(k, masks, sum(masks), flip(self.me, 1), self.sib_send, self.sib_recv)

    def arrived(self, k, masks):
        self.make(k, masks, sum(masks), flip(self.me, 1), self.send_sem, self.recv_sem).wait_recv()

    def stage0(self):
        for t in range(3):
            def send(k, carry):
                self.hop(k, (), self.axes(k)[t]).start()
                return carry
            lax.fori_loop(0, 3, send, 0)

        def send_sib(k, carry):
            self.sib(k, ()).start()
            return carry
        lax.fori_loop(0, 3, send_sib, 0)

    def stage1(self):
        def step(k, carry):
            a, b, c = self.axes(k)
            self.arrived(k, (a,))
            self.hop(k, (a,), b).start()
            self.hop(k, (a,), c).start()
            self.sib(k, (a,)).start()
            return carry
        lax.fori_loop(0, 3, step, 0)

    def stage2(self):
        for both in (False, True):
            def step(k, carry):
                a, b, c = self.axes(k)
                masks = (a, b) if both else (b,)
                self.arrived(k, masks)
                self.hop(k, masks, c).start()
                self.sib(k, masks).start()
                return carry
            lax.fori_loop(0, 3, step, 0)

    def stage3(self):
        for extra in range(4):
            def step(k, carry):
                a, b, c = self.axes(k)
                masks = ((c,), (a, c), (b, c), (a, b, c))[extra]
                self.arrived(k, masks)
                self.sib(k, masks).start()
                return carry
            lax.fori_loop(0, 3, step, 0)

    def finish(self):
        sibling = flip(self.me, 1)

        def step(n, carry):
            k, half = lax.div(n, 8), lax.rem(n, 8)
            rows = pl.ds(k * self.chunk, self.chunk)
            ref = self.view(xor(sibling, 2 * half), rows)
            pltpu.make_async_remote_copy(
                src_ref=ref, dst_ref=ref, send_sem=self.sib_send.at[n], recv_sem=self.sib_recv.at[n],
                device_id=(sibling,), device_id_type=MESH).wait_recv()
            return carry
        lax.fori_loop(0, 24, step, 0)

    def drain(self):
        def step(n, carry):
            k, half = lax.div(n, 8), lax.rem(n, 8)
            rows = pl.ds(k * self.chunk, self.chunk)
            ref = self.view(xor(self.me, 2 * half), rows)
            pltpu.make_async_remote_copy(
                src_ref=ref, dst_ref=ref, send_sem=self.sib_send.at[n], recv_sem=self.sib_recv.at[n],
                device_id=(flip(self.me, 1),), device_id_type=MESH).wait_send()

            @pl.when(half > 0)
            def _():
                pltpu.make_async_remote_copy(
                    src_ref=ref, dst_ref=ref, send_sem=self.send_sem.at[n], recv_sem=self.recv_sem.at[n],
                    device_id=(flip(self.me, 1),), device_id_type=MESH).wait_send()
            return carry
        lax.fori_loop(0, 24, step, 0)


def kernel(qt_ref, do_ref, c_ref, rt_ref, wuk_ref, wuv_ref,
           o_ref, dq_ref, dc_ref, drt_ref, dwk_ref, dwv_ref,
           in_q, in_do, stage_o, stage_dq, stage_v, stage_k, in_v, in_k, call, kcat, kt, v, vt, sbuf, prob, qz, dk, dv,
           ot, dqt, delta, dct, wuk, wuv, dwk_own, dwv_own,
           q_send, q_recv, do_send, do_recv, o_send, o_recv, dq_send, dq_recv, v_send, v_recv, k_send, k_recv, local_sem,
           c_send, c_recv, cs_send, cs_recv, gk_send, gk_recv, gks_send, gks_recv, gv_send, gv_recv, gvs_send, gvs_recv):
    me = lax.axis_index("cp")

    loads = [
        pltpu.make_async_copy(wuk_ref, wuk, local_sem.at[0]),
        pltpu.make_async_copy(wuv_ref, wuv, local_sem.at[1]),
        pltpu.make_async_copy(c_ref, call.at[me, pl.ds(0, T), :], local_sem.at[2]),
        pltpu.make_async_copy(rt_ref.at[pl.ds(0, 32), :], call.at[me, pl.ds(T, 32), pl.ds(0, T)], local_sem.at[3]),
        pltpu.make_async_copy(rt_ref.at[pl.ds(32, 32), :], call.at[me, pl.ds(T, 32), pl.ds(T, T)], local_sem.at[4]),
    ]
    for load in loads[::-1]:
        load.start()

    barrier = pltpu.get_barrier_semaphore()

    def hello(s, carry):
        pl.semaphore_signal(barrier, inc=1, device_id=(xor(me, s),), device_id_type=MESH)
        return carry

    lax.fori_loop(1, N, hello, 0)
    for load in loads[2:]:
        load.wait()
    pl.semaphore_wait(barrier, N - 1)

    def send(src, dst, n, send_sem, recv_sem):
        return pltpu.make_async_remote_copy(
            src_ref=src, dst_ref=dst.at[me], send_sem=send_sem.at[n], recv_sem=recv_sem.at[me],
            device_id=(xor(me, partner(n)),), device_id_type=MESH)

    def take(src, dst, other, send_sem, recv_sem):
        pltpu.make_async_remote_copy(
            src_ref=src, dst_ref=dst.at[other], send_sem=send_sem.at[0], recv_sem=recv_sem.at[other],
            device_id=(flip(me, 1),), device_id_type=MESH).wait_recv()

    gather_c = Gather(me, call.at[me], lambda src, rows: call.at[src, rows, :], C_CHUNK, c_send, c_recv, cs_send, cs_recv)
    gather_c.stage0()
    pltpu.make_async_copy(qt_ref.at[me], in_q.at[me], q_recv.at[me]).start()
    pltpu.make_async_copy(do_ref.at[me], in_do.at[me], do_recv.at[me]).start()
    dk[...] = jnp.zeros_like(dk)
    dv[...] = jnp.zeros_like(dv)
    qz[...] = jnp.zeros_like(qz)
    dwk_own[...] = jnp.zeros_like(dwk_own)
    dwv_own[...] = jnp.zeros_like(dwv_own)
    gather_c.stage1()
    gather_c.stage2()

    def send_q(n, carry):
        other = xor(me, partner(n))
        send(qt_ref.at[other], in_q, n, q_send, q_recv).start()
        send(do_ref.at[other], in_do, n, do_send, do_recv).start()
        return carry

    lax.fori_loop(1, N, send_q, 0)
    for load in loads[:2]:
        load.wait()
    gather_c.stage3()
    gather_c.finish()

    lanes = pl.ds(pl.multiple_of(me * D, D), D)

    def make_kv(jt, carry):
        wcat = jnp.concatenate([wuk[:, lanes], wuv[:, lanes]], axis=1)
        for half in range(2):
            j = jt * 2 + half
            rows = pl.ds(half * T, T)
            kv = nn_dot(call[j, pl.ds(0, T), :], wcat)
            rt = jnp.concatenate([call[j, pl.ds(T, 32), pl.ds(0, T)], call[j, pl.ds(T, 32), pl.ds(T, T)]], axis=0)
            rtz = jnp.concatenate([rt.astype(F32), jnp.zeros((R, T), F32)], axis=0)
            kcat[jt, rows, pl.ds(0, D)] = kv[:, :D].astype(BF16)
            kcat[jt, rows, pl.ds(D, D)] = transpose(rtz).astype(BF16)
            v[jt, rows, :] = kv[:, D:].astype(BF16)
            kvt = transpose(kv).astype(BF16)
            kt[jt, pl.ds(0, D), rows] = kvt[:D]
            kt[jt, pl.ds(D, R), rows] = rt
            vt[jt, :, rows] = kvt[D:]
        return carry

    lax.fori_loop(0, NT, make_kv, 0)

    def first_prob(i):
        half = lax.div(i, 2)
        return (half + lax.rem(i, 2)) * (half + 1)

    def forward(n, carry):
        i = xor(me, partner(n))
        take(qt_ref.at[i], in_q, i, q_send, q_recv)
        take(do_ref.at[i], in_do, i, do_send, do_recv)
        last = lax.div(i, 2)
        base = first_prob(i)
        qz[pl.ds(0, QK), :] = in_q[i]

        def score_tile(jt, top):
            sc = nn_dot(kcat[jt], qz[...])
            sbuf[jt] = sc
            return jnp.maximum(top, fold(sc, jnp.max))

        top = lax.fori_loop(0, last, score_tile, jnp.full((8, T), -1e30, F32))
        sc = nn_dot(kcat[last], qz[...])
        ahead = lax.broadcasted_iota(jnp.int32, sc.shape, 0) - lax.broadcasted_iota(jnp.int32, sc.shape, 1)
        sc = jnp.where(ahead <= i * T - last * TK, sc, -1e30)
        sbuf[last] = sc
        top = jnp.maximum(top, fold(sc, jnp.max))
        top = jnp.max(top, axis=0, keepdims=True) * EXP_C

        ot[...] = jnp.zeros_like(ot)

        def soft_tile(jt, total):
            e = jnp.exp2(sbuf[jt] * EXP_C - top)
            sbuf[jt] = e
            ot[...] += nn_dot(vt[jt], e.astype(BF16))
            return total + fold(e, jnp.sum)

        total = lax.fori_loop(0, last + 1, soft_tile, jnp.zeros((8, T), F32))
        inv = 1.0 / jnp.sum(total, axis=0, keepdims=True)
        o_t = ot[...] * inv
        stage_o[n] = transpose(o_t).astype(BF16)

        @pl.when(n > 0)
        def _():
            send(stage_o.at[n], o_ref, n, o_send, o_recv).start()

        do_t = transpose(in_do[i].astype(F32))
        delta[n] = jnp.broadcast_to(jnp.sum(o_t * do_t, axis=0, keepdims=True), (8, T))

        def value_tile(jt, c):
            p = (sbuf[jt] * inv).astype(BF16)
            prob[base + jt] = p
            dv[jt] += nn_dot(p, in_do[i])
            return c

        lax.fori_loop(0, last + 1, value_tile, 0)
        return carry

    lax.fori_loop(0, N, forward, 0)
    pltpu.make_async_copy(stage_o.at[0], o_ref.at[me], o_recv.at[me]).start()

    def block_rows(i):
        return pl.ds(pl.multiple_of(lax.rem(i, 2) * T, T), T)

    def grad_v(n, carry):
        i = xor(me, partner(n))
        stage_v[n] = transpose(dv[lax.div(i, 2), block_rows(i), :]).astype(BF16)

        @pl.when(n > 0)
        def _():
            send(stage_v.at[n], in_v, n, v_send, v_recv).start()

        return carry

    def weight_grad(stage, own):
        def step(m, acc):
            lhs = jnp.concatenate([stage[4 * m + r, pl.ds(0, D), :] for r in range(4)], axis=1)
            rhs = jnp.concatenate([call[xor(me, partner(4 * m + r)), pl.ds(0, T), :] for r in range(4)], axis=0)
            return acc + nn_dot(lhs, rhs)

        dwt = lax.fori_loop(0, 4, step, jnp.zeros((D, L), F32))
        own[pl.ds(0, L), :] = transpose(dwt)

    lax.fori_loop(0, N, grad_v, 0)
    pltpu.make_async_copy(stage_v.at[0], in_v.at[me], v_recv.at[me]).start()
    weight_grad(stage_v, dwv_own)
    gather_v = Gather(me, dwv_own, lambda src, rows: dwv_ref.at[rows, src, 0, :], W_CHUNK, gv_send, gv_recv, gvs_send, gvs_recv)
    all_rows = pl.ds(0, 3 * W_CHUNK)
    own_v = pltpu.make_async_copy(dwv_own, gather_v.view(me, all_rows), local_sem.at[5])
    own_v.start()
    gather_v.stage0()

    def backward(n, carry):
        i = xor(me, partner(n))
        last = lax.div(i, 2)
        base = first_prob(i)
        qz[pl.ds(0, QK), :] = in_q[i]
        dqt[...] = jnp.zeros_like(dqt)
        row_delta = delta[n, pl.ds(0, 1), :]

        def back_tile(jt, c):
            dp = nt_dot(v[jt], in_do[i])
            ds = (prob[base + jt].astype(F32) * (dp - row_delta)).astype(BF16)
            dk[jt] += nt_dot(ds, qz[...])
            dqt[...] += nn_dot(kt[jt], ds)
            return c

        lax.fori_loop(0, last + 1, back_tile, 0)
        stage_dq[n] = (dqt[...] * SCALE).astype(BF16)

        @pl.when(n > 0)
        def _():
            send(stage_dq.at[n], dq_ref, n, dq_send, dq_recv).start()

        @pl.when(n == 4)
        def _():
            gather_v.stage1()

        @pl.when(n == 8)
        def _():
            gather_v.stage2()

        @pl.when(n == 12)
        def _():
            gather_v.stage3()

        return carry

    lax.fori_loop(0, N, backward, 0)
    pltpu.make_async_copy(stage_dq.at[0], dq_ref.at[me], dq_recv.at[me]).start()

    def grad_k(n, carry):
        i = xor(me, partner(n))
        key = transpose(dk[lax.div(i, 2), block_rows(i), :] * SCALE)
        stage_k[n] = key[:QK].astype(BF16)
        return carry

    lax.fori_loop(0, N, grad_k, 0)
    pltpu.make_async_copy(stage_k.at[0], in_k.at[me], k_recv.at[me]).start()

    def send_k(n, carry):
        send(stage_k.at[n], in_k, n, k_send, k_recv).start()
        return carry

    lax.fori_loop(1, 4, send_k, 0)
    weight_grad(stage_k, dwk_own)
    gather_k = Gather(me, dwk_own, lambda src, rows: dwk_ref.at[rows, src, 0, :], W_CHUNK, gk_send, gk_recv, gks_send, gks_recv)
    own_k = pltpu.make_async_copy(dwk_own, gather_k.view(me, all_rows), local_sem.at[6])
    own_k.start()
    gather_k.stage0()
    lax.fori_loop(4, 8, send_k, 0)

    dct[...] = jnp.zeros_like(dct)

    def latent_from_v(h, carry):
        take(stage_v.at[0], in_v, h, v_send, v_recv)
        cols = pl.ds(pl.multiple_of(h * D, D), D)
        dct[...] += nn_dot(wuv[:, cols], in_v[h])
        return carry

    lax.fori_loop(0, N, latent_from_v, 0)
    gather_k.stage1()
    lax.fori_loop(8, N, send_k, 0)
    gather_k.stage2()

    def latent_from_k(n, acc):
        h = xor(me, partner(n))
        take(stage_k.at[0], in_k, h, k_send, k_recv)
        cols = pl.ds(pl.multiple_of(h * D, D), D)
        dct[...] += nn_dot(wuk[:, cols], in_k[h, pl.ds(0, D), :])
        return acc + in_k[h, pl.ds(D, R), :].astype(F32)

    drt_ref[...] = lax.fori_loop(0, N, latent_from_k, jnp.zeros((R, T), F32)).astype(BF16)
    dc_ref[...] = transpose(dct[...]).astype(BF16)

    gather_k.stage3()
    gather_v.finish()
    gather_k.finish()
    own_v.wait()
    own_k.wait()

    def take_o(h, carry):
        take(stage_o.at[0], o_ref, h, o_send, o_recv)
        take(stage_dq.at[0], dq_ref, h, dq_send, dq_recv)
        return carry

    lax.fori_loop(0, N, take_o, 0)

    def drain(n, carry):
        other = xor(me, partner(n))
        send(qt_ref.at[other], in_q, n, q_send, q_recv).wait_send()
        send(do_ref.at[other], in_do, n, do_send, do_recv).wait_send()
        send(stage_o.at[n], o_ref, n, o_send, o_recv).wait_send()
        send(stage_dq.at[n], dq_ref, n, dq_send, dq_recv).wait_send()
        send(stage_v.at[n], in_v, n, v_send, v_recv).wait_send()
        send(stage_k.at[n], in_k, n, k_send, k_recv).wait_send()
        return carry

    lax.fori_loop(1, N, drain, 0)
    gather_c.drain()
    gather_v.drain()
    gather_k.drain()


def solution(mesh):
    seq_spec = P("cp")

    def local_step(queries, latent, key_rope, w_uk, w_uv, d_out):
        any_spec = pl.BlockSpec(memory_space=pl.ANY)
        vmem_spec = pl.BlockSpec(memory_space=pltpu.VMEM)
        dma = pltpu.SemaphoreType.DMA
        o_all, dq_all, dc, drt, dwk, dwv = pl.pallas_call(
            kernel,
            name="mla_core",
            out_shape=(jax.ShapeDtypeStruct((N, T, D), BF16),
                       jax.ShapeDtypeStruct((N, QK, T), BF16),
                       jax.ShapeDtypeStruct((T, L), BF16),
                       jax.ShapeDtypeStruct((R, T), BF16),
                       jax.ShapeDtypeStruct((3 * W_CHUNK, N, 1, D), F32),
                       jax.ShapeDtypeStruct((3 * W_CHUNK, N, 1, D), F32)),
            in_specs=[any_spec] * 6,
            out_specs=(any_spec, any_spec, vmem_spec, vmem_spec, any_spec, any_spec),
            scratch_shapes=[
                pltpu.VMEM((N, QK, T), BF16),
                pltpu.VMEM((N, T, D), BF16),
                pltpu.VMEM((N, T, D), BF16),
                pltpu.VMEM((N, QK, T), BF16),
                pltpu.VMEM((N, D, T), BF16),
                pltpu.VMEM((N, QK, T), BF16),
                pltpu.VMEM((N, D, T), BF16),
                pltpu.VMEM((N, QK, T), BF16),
                pltpu.VMEM((N, 3 * C_CHUNK, L), BF16),
                pltpu.VMEM((NT, TK, 2 * D), BF16),
                pltpu.VMEM((NT, QK, TK), BF16),
                pltpu.VMEM((NT, TK, D), BF16),
                pltpu.VMEM((NT, D, TK), BF16),
                pltpu.VMEM((NT, TK, T), F32),
                pltpu.VMEM((NP, TK, T), BF16),
                pltpu.VMEM((2 * D, T), BF16),
                pltpu.VMEM((NT, TK, 2 * D), F32),
                pltpu.VMEM((NT, TK, D), F32),
                pltpu.VMEM((D, T), F32),
                pltpu.VMEM((QK, T), F32),
                pltpu.VMEM((N, 8, T), F32),
                pltpu.VMEM((L, T), F32),
                pltpu.VMEM((L, N * D), BF16),
                pltpu.VMEM((L, N * D), BF16),
                pltpu.VMEM((3 * W_CHUNK, D), F32),
                pltpu.VMEM((3 * W_CHUNK, D), F32),
            ] + [dma((N,))] * 12 + [dma((7,))] + [dma((24,))] * 12,
            compiler_params=pltpu.CompilerParams(
                collective_id=0, has_side_effects=True, vmem_limit_bytes=67043328),
        )(jnp.transpose(queries, (1, 2, 0)), jnp.transpose(d_out, (1, 0, 2)), latent, jnp.transpose(key_rope, (1, 0)),
          w_uk.reshape(L, N * D), w_uv.reshape(L, N * D))

        return (jnp.transpose(o_all, (1, 0, 2)), jnp.transpose(dq_all, (2, 0, 1)), dc, jnp.transpose(drt, (1, 0)),
                dwk[:L].reshape(L, N, D), dwv[:L].reshape(L, N, D))

    return jax.shard_map(local_step, mesh=mesh,
                         in_specs=(seq_spec, seq_spec, seq_spec, P(), P(), seq_spec),
                         out_specs=(seq_spec, seq_spec, seq_spec, seq_spec, P(), P()),
                         check_vma=False)
```

```python
import math
import jax
import jax.numpy as jnp
from jax import lax
from jax.experimental import pallas as pl
from jax.experimental.pallas import tpu as pltpu
from jax.sharding import PartitionSpec as P

MESH = pl.DeviceIdType.MESH
BF16 = jnp.bfloat16
F32 = jnp.float32

N = 16
T = 256
L = 512
D = 128
R = 64
QK = D + R
TK = 512
NT = 8
C_CHUNK = 96
W_CHUNK = 176
NP = 72
ORDER = (0, 7, 3, 4, 5, 2, 6, 1)
TABLE = sum(chip << (3 * n) for n, chip in enumerate(ORDER))
SCALE = 1.0 / math.sqrt(QK)
EXP_C = SCALE * math.log2(math.e)


def nt_dot(a, b):
    return lax.dot_general(a, b, (((1,), (1,)), ((), ())), preferred_element_type=F32)


def nn_dot(a, b):
    return lax.dot_general(a, b, (((1,), (0,)), ((), ())), preferred_element_type=F32)


def flip(x, bit):
    return x + bit * (1 - 2 * lax.rem(lax.div(x, bit), 2))


def xor(x, s):
    for bit in (1, 2, 4, 8):
        on = lax.rem(lax.div(s, bit), 2)
        x = x + on * bit * (1 - 2 * lax.rem(lax.div(x, bit), 2))
    return x


def partner(n):
    k = lax.div(n, 2)
    power = (1 + 7 * lax.rem(k, 2)) * (1 + 63 * lax.rem(lax.div(k, 2), 2)) * (1 + 4095 * lax.div(k, 4))
    return 2 * lax.rem(lax.div(TABLE, power), 8) + lax.rem(n, 2)


def fold(x, reduce):
    return reduce(x.reshape(x.shape[0] // 8, 8, x.shape[1]), axis=0)


def transpose(x):
    return jnp.transpose(x, (1, 0))


class Gather:
    def __init__(self, me, own, view, chunk, send_sem, recv_sem, sib_send, sib_recv):
        self.me, self.own, self.view, self.chunk = me, own, view, chunk
        self.send_sem, self.recv_sem = send_sem, recv_sem
        self.sib_send, self.sib_recv = sib_send, sib_recv

    def axes(self, k):
        out = []
        for t in range(3):
            axis = lax.rem(k + t, 3)
            out.append(2 + axis * (axis + 1))
        return out

    def make(self, k, masks, mask, target, send_sem, recv_sem):
        src = self.me
        for bit in masks:
            src = flip(src, bit)
        rows = pl.ds(k * self.chunk, self.chunk)
        slot = k * 8 + lax.div(mask, 2)
        first = self.own.at[rows, :] if not masks else self.view(src, rows)
        return pltpu.make_async_remote_copy(
            src_ref=first, dst_ref=self.view(src, rows), send_sem=send_sem.at[slot], recv_sem=recv_sem.at[slot],
            device_id=(target,), device_id_type=MESH)

    def hop(self, k, masks, bit):
        return self.make(k, masks, sum(masks) + bit, flip(self.me, bit), self.send_sem, self.recv_sem)

    def sib(self, k, masks):
        return self.make(k, masks, sum(masks), flip(self.me, 1), self.sib_send, self.sib_recv)

    def arrived(self, k, masks):
        self.make(k, masks, sum(masks), flip(self.me, 1), self.send_sem, self.recv_sem).wait_recv()

    def stage0(self):
        for t in range(3):
            def send(k, carry):
                self.hop(k, (), self.axes(k)[t]).start()
                return carry
            lax.fori_loop(0, 3, send, 0)

        def send_sib(k, carry):
            self.sib(k, ()).start()
            return carry
        lax.fori_loop(0, 3, send_sib, 0)

    def stage1(self):
        def step(k, carry):
            a, b, c = self.axes(k)
            self.arrived(k, (a,))
            self.hop(k, (a,), b).start()
            self.hop(k, (a,), c).start()
            self.sib(k, (a,)).start()
            return carry
        lax.fori_loop(0, 3, step, 0)

    def stage2(self):
        for both in (False, True):
            def step(k, carry):
                a, b, c = self.axes(k)
                masks = (a, b) if both else (b,)
                self.arrived(k, masks)
                self.hop(k, masks, c).start()
                self.sib(k, masks).start()
                return carry
            lax.fori_loop(0, 3, step, 0)

    def stage3(self):
        for extra in range(4):
            def step(k, carry):
                a, b, c = self.axes(k)
                masks = ((c,), (a, c), (b, c), (a, b, c))[extra]
                self.arrived(k, masks)
                self.sib(k, masks).start()
                return carry
            lax.fori_loop(0, 3, step, 0)

    def finish(self):
        sibling = flip(self.me, 1)

        def step(n, carry):
            k, half = lax.div(n, 8), lax.rem(n, 8)
            rows = pl.ds(k * self.chunk, self.chunk)
            ref = self.view(xor(sibling, 2 * half), rows)
            pltpu.make_async_remote_copy(
                src_ref=ref, dst_ref=ref, send_sem=self.sib_send.at[n], recv_sem=self.sib_recv.at[n],
                device_id=(sibling,), device_id_type=MESH).wait_recv()
            return carry
        lax.fori_loop(0, 24, step, 0)

    def drain(self):
        def step(n, carry):
            k, half = lax.div(n, 8), lax.rem(n, 8)
            rows = pl.ds(k * self.chunk, self.chunk)
            ref = self.view(xor(self.me, 2 * half), rows)
            pltpu.make_async_remote_copy(
                src_ref=ref, dst_ref=ref, send_sem=self.sib_send.at[n], recv_sem=self.sib_recv.at[n],
                device_id=(flip(self.me, 1),), device_id_type=MESH).wait_send()

            @pl.when(half > 0)
            def _():
                pltpu.make_async_remote_copy(
                    src_ref=ref, dst_ref=ref, send_sem=self.send_sem.at[n], recv_sem=self.recv_sem.at[n],
                    device_id=(flip(self.me, 1),), device_id_type=MESH).wait_send()
            return carry
        lax.fori_loop(0, 24, step, 0)


def kernel(qt_ref, do_ref, c_ref, rt_ref, wuk_ref, wuv_ref,
           o_ref, dq_ref, dc_ref, drt_ref, dwk_ref, dwv_ref,
           in_q, in_do, stage_o, stage_dq, stage_v, stage_k, in_v, in_k, call, kcat, kt, v, vt, sbuf, prob, qz, dk, dv,
           ot, dqt, delta, dct, wuk, wuv, dwk_own, dwv_own,
           q_send, q_recv, do_send, do_recv, o_send, o_recv, dq_send, dq_recv, v_send, v_recv, k_send, k_recv, local_sem,
           c_send, c_recv, cs_send, cs_recv, gk_send, gk_recv, gks_send, gks_recv, gv_send, gv_recv, gvs_send, gvs_recv):
    me = lax.axis_index("cp")

    loads = [
        pltpu.make_async_copy(wuk_ref, wuk, local_sem.at[0]),
        pltpu.make_async_copy(wuv_ref, wuv, local_sem.at[1]),
        pltpu.make_async_copy(c_ref, call.at[me, pl.ds(0, T), :], local_sem.at[2]),
        pltpu.make_async_copy(rt_ref.at[pl.ds(0, 32), :], call.at[me, pl.ds(T, 32), pl.ds(0, T)], local_sem.at[3]),
        pltpu.make_async_copy(rt_ref.at[pl.ds(32, 32), :], call.at[me, pl.ds(T, 32), pl.ds(T, T)], local_sem.at[4]),
    ]
    for load in loads[::-1]:
        load.start()

    barrier = pltpu.get_barrier_semaphore()

    def hello(s, carry):
        pl.semaphore_signal(barrier, inc=1, device_id=(xor(me, s),), device_id_type=MESH)
        return carry

    lax.fori_loop(1, N, hello, 0)
    for load in loads[2:]:
        load.wait()
    pl.semaphore_wait(barrier, N - 1)

    def send(src, dst, n, send_sem, recv_sem):
        return pltpu.make_async_remote_copy(
            src_ref=src, dst_ref=dst.at[me], send_sem=send_sem.at[n], recv_sem=recv_sem.at[me],
            device_id=(xor(me, partner(n)),), device_id_type=MESH)

    def take(src, dst, other, send_sem, recv_sem):
        pltpu.make_async_remote_copy(
            src_ref=src, dst_ref=dst.at[other], send_sem=send_sem.at[0], recv_sem=recv_sem.at[other],
            device_id=(flip(me, 1),), device_id_type=MESH).wait_recv()

    gather_c = Gather(me, call.at[me], lambda src, rows: call.at[src, rows, :], C_CHUNK, c_send, c_recv, cs_send, cs_recv)
    gather_c.stage0()
    pltpu.make_async_copy(qt_ref.at[me], in_q.at[me], q_recv.at[me]).start()
    pltpu.make_async_copy(do_ref.at[me], in_do.at[me], do_recv.at[me]).start()
    dk[...] = jnp.zeros_like(dk)
    dv[...] = jnp.zeros_like(dv)
    qz[...] = jnp.zeros_like(qz)
    dwk_own[...] = jnp.zeros_like(dwk_own)
    dwv_own[...] = jnp.zeros_like(dwv_own)
    gather_c.stage1()
    gather_c.stage2()

    def send_q(n, carry):
        other = xor(me, partner(n))
        send(qt_ref.at[other], in_q, n, q_send, q_recv).start()
        send(do_ref.at[other], in_do, n, do_send, do_recv).start()
        return carry

    lax.fori_loop(1, N, send_q, 0)
    for load in loads[:2]:
        load.wait()
    gather_c.stage3()
    gather_c.finish()

    lanes = pl.ds(pl.multiple_of(me * D, D), D)

    def make_kv(jt, carry):
        wcat = jnp.concatenate([wuk[:, lanes], wuv[:, lanes]], axis=1)
        for half in range(2):
            j = jt * 2 + half
            rows = pl.ds(half * T, T)
            kv = nn_dot(call[j, pl.ds(0, T), :], wcat)
            rt = jnp.concatenate([call[j, pl.ds(T, 32), pl.ds(0, T)], call[j, pl.ds(T, 32), pl.ds(T, T)]], axis=0)
            rtz = jnp.concatenate([rt.astype(F32), jnp.zeros((R, T), F32)], axis=0)
            kcat[jt, rows, pl.ds(0, D)] = kv[:, :D].astype(BF16)
            kcat[jt, rows, pl.ds(D, D)] = transpose(rtz).astype(BF16)
            v[jt, rows, :] = kv[:, D:].astype(BF16)
            kvt = transpose(kv).astype(BF16)
            kt[jt, pl.ds(0, D), rows] = kvt[:D]
            kt[jt, pl.ds(D, R), rows] = rt
            vt[jt, :, rows] = kvt[D:]
        return carry

    lax.fori_loop(0, NT, make_kv, 0)

    def first_prob(i):
        half = lax.div(i, 2)
        return (half + lax.rem(i, 2)) * (half + 1)

    def forward(n, carry):
        i = xor(me, partner(n))
        take(qt_ref.at[i], in_q, i, q_send, q_recv)
        take(do_ref.at[i], in_do, i, do_send, do_recv)
        last = lax.div(i, 2)
        base = first_prob(i)
        qz[pl.ds(0, QK), :] = in_q[i]

        def score_tile(jt, top):
            sc = nn_dot(kcat[jt], qz[...])
            sbuf[jt] = sc
            return jnp.maximum(top, fold(sc, jnp.max))

        top = lax.fori_loop(0, last, score_tile, jnp.full((8, T), -1e30, F32))
        sc = nn_dot(kcat[last], qz[...])
        ahead = lax.broadcasted_iota(jnp.int32, sc.shape, 0) - lax.broadcasted_iota(jnp.int32, sc.shape, 1)
        sc = jnp.where(ahead <= i * T - last * TK, sc, -1e30)
        sbuf[last] = sc
        top = jnp.maximum(top, fold(sc, jnp.max))
        top = jnp.max(top, axis=0, keepdims=True) * EXP_C

        ot[...] = jnp.zeros_like(ot)

        def soft_tile(jt, total):
            e = jnp.exp2(sbuf[jt] * EXP_C - top)
            sbuf[jt] = e
            ot[...] += nn_dot(vt[jt], e.astype(BF16))
            return total + fold(e, jnp.sum)

        total = lax.fori_loop(0, last + 1, soft_tile, jnp.zeros((8, T), F32))
        inv = 1.0 / jnp.sum(total, axis=0, keepdims=True)
        o_t = ot[...] * inv
        stage_o[n] = transpose(o_t).astype(BF16)

        @pl.when(n > 0)
        def _():
            send(stage_o.at[n], o_ref, n, o_send, o_recv).start()

        do_t = transpose(in_do[i].astype(F32))
        delta[n] = jnp.broadcast_to(jnp.sum(o_t * do_t, axis=0, keepdims=True), (8, T))

        def value_tile(jt, c):
            p = (sbuf[jt] * inv).astype(BF16)
            prob[base + jt] = p
            dv[jt] += nn_dot(p, in_do[i])
            return c

        lax.fori_loop(0, last + 1, value_tile, 0)
        return carry

    lax.fori_loop(0, N, forward, 0)
    pltpu.make_async_copy(stage_o.at[0], o_ref.at[me], o_recv.at[me]).start()

    def block_rows(i):
        return pl.ds(pl.multiple_of(lax.rem(i, 2) * T, T), T)

    def grad_v(n, carry):
        i = xor(me, partner(n))
        stage_v[n] = transpose(dv[lax.div(i, 2), block_rows(i), :]).astype(BF16)

        @pl.when(n > 0)
        def _():
            send(stage_v.at[n], in_v, n, v_send, v_recv).start()

        return carry

    def weight_grad(stage, own):
        def step(m, acc):
            lhs = jnp.concatenate([stage[4 * m + r, pl.ds(0, D), :] for r in range(4)], axis=1)
            rhs = jnp.concatenate([call[xor(me, partner(4 * m + r)), pl.ds(0, T), :] for r in range(4)], axis=0)
            return acc + nn_dot(lhs, rhs)

        dwt = lax.fori_loop(0, 4, step, jnp.zeros((D, L), F32))
        own[pl.ds(0, L), :] = transpose(dwt)

    lax.fori_loop(0, N, grad_v, 0)
    pltpu.make_async_copy(stage_v.at[0], in_v.at[me], v_recv.at[me]).start()
    weight_grad(stage_v, dwv_own)
    gather_v = Gather(me, dwv_own, lambda src, rows: dwv_ref.at[src, rows, :], W_CHUNK, gv_send, gv_recv, gvs_send, gvs_recv)
    all_rows = pl.ds(0, 3 * W_CHUNK)
    own_v = pltpu.make_async_copy(dwv_own, gather_v.view(me, all_rows), local_sem.at[5])
    own_v.start()
    gather_v.stage0()

    def backward(n, carry):
        i = xor(me, partner(n))
        last = lax.div(i, 2)
        base = first_prob(i)
        qz[pl.ds(0, QK), :] = in_q[i]
        dqt[...] = jnp.zeros_like(dqt)
        row_delta = delta[n, pl.ds(0, 1), :]

        def back_tile(jt, c):
            dp = nt_dot(v[jt], in_do[i])
            ds = (prob[base + jt].astype(F32) * (dp - row_delta)).astype(BF16)
            dk[jt] += nt_dot(ds, qz[...])
            dqt[...] += nn_dot(kt[jt], ds)
            return c

        lax.fori_loop(0, last + 1, back_tile, 0)
        stage_dq[n] = (dqt[...] * SCALE).astype(BF16)

        @pl.when(n > 0)
        def _():
            send(stage_dq.at[n], dq_ref, n, dq_send, dq_recv).start()

        @pl.when(n == 4)
        def _():
            gather_v.stage1()

        @pl.when(n == 8)
        def _():
            gather_v.stage2()

        @pl.when(n == 12)
        def _():
            gather_v.stage3()

        return carry

    lax.fori_loop(0, N, backward, 0)
    pltpu.make_async_copy(stage_dq.at[0], dq_ref.at[me], dq_recv.at[me]).start()

    def grad_k(n, carry):
        i = xor(me, partner(n))
        key = transpose(dk[lax.div(i, 2), block_rows(i), :] * SCALE)
        stage_k[n] = key[:QK].astype(BF16)
        return carry

    lax.fori_loop(0, N, grad_k, 0)
    pltpu.make_async_copy(stage_k.at[0], in_k.at[me], k_recv.at[me]).start()

    def send_k(n, carry):
        send(stage_k.at[n], in_k, n, k_send, k_recv).start()
        return carry

    lax.fori_loop(1, 4, send_k, 0)
    weight_grad(stage_k, dwk_own)
    gather_k = Gather(me, dwk_own, lambda src, rows: dwk_ref.at[src, rows, :], W_CHUNK, gk_send, gk_recv, gks_send, gks_recv)
    own_k = pltpu.make_async_copy(dwk_own, gather_k.view(me, all_rows), local_sem.at[6])
    own_k.start()
    gather_k.stage0()
    lax.fori_loop(4, 8, send_k, 0)

    dct[...] = jnp.zeros_like(dct)

    def latent_from_v(h, carry):
        take(stage_v.at[0], in_v, h, v_send, v_recv)
        cols = pl.ds(pl.multiple_of(h * D, D), D)
        dct[...] += nn_dot(wuv[:, cols], in_v[h])
        return carry

    lax.fori_loop(0, N, latent_from_v, 0)
    gather_k.stage1()
    lax.fori_loop(8, N, send_k, 0)
    gather_k.stage2()

    def latent_from_k(n, acc):
        h = xor(me, partner(n))
        take(stage_k.at[0], in_k, h, k_send, k_recv)
        cols = pl.ds(pl.multiple_of(h * D, D), D)
        dct[...] += nn_dot(wuk[:, cols], in_k[h, pl.ds(0, D), :])
        return acc + in_k[h, pl.ds(D, R), :].astype(F32)

    drt_ref[...] = lax.fori_loop(0, N, latent_from_k, jnp.zeros((R, T), F32)).astype(BF16)
    dc_ref[...] = transpose(dct[...]).astype(BF16)

    gather_k.stage3()
    gather_v.finish()
    gather_k.finish()
    own_v.wait()
    own_k.wait()

    def take_o(h, carry):
        take(stage_o.at[0], o_ref, h, o_send, o_recv)
        take(stage_dq.at[0], dq_ref, h, dq_send, dq_recv)
        return carry

    lax.fori_loop(0, N, take_o, 0)

    def drain(n, carry):
        other = xor(me, partner(n))
        send(qt_ref.at[other], in_q, n, q_send, q_recv).wait_send()
        send(do_ref.at[other], in_do, n, do_send, do_recv).wait_send()
        send(stage_o.at[n], o_ref, n, o_send, o_recv).wait_send()
        send(stage_dq.at[n], dq_ref, n, dq_send, dq_recv).wait_send()
        send(stage_v.at[n], in_v, n, v_send, v_recv).wait_send()
        send(stage_k.at[n], in_k, n, k_send, k_recv).wait_send()
        return carry

    lax.fori_loop(1, N, drain, 0)
    gather_c.drain()
    gather_v.drain()
    gather_k.drain()


def solution(mesh):
    seq_spec = P("cp")

    def local_step(queries, latent, key_rope, w_uk, w_uv, d_out):
        any_spec = pl.BlockSpec(memory_space=pl.ANY)
        vmem_spec = pl.BlockSpec(memory_space=pltpu.VMEM)
        dma = pltpu.SemaphoreType.DMA
        o_all, dq_all, dc, drt, dwk, dwv = pl.pallas_call(
            kernel,
            name="mla_core",
            out_shape=(jax.ShapeDtypeStruct((N, T, D), BF16),
                       jax.ShapeDtypeStruct((N, QK, T), BF16),
                       jax.ShapeDtypeStruct((T, L), BF16),
                       jax.ShapeDtypeStruct((R, T), BF16),
                       jax.ShapeDtypeStruct((N, 3 * W_CHUNK, D), F32),
                       jax.ShapeDtypeStruct((N, 3 * W_CHUNK, D), F32)),
            in_specs=[any_spec] * 6,
            out_specs=(any_spec, any_spec, vmem_spec, vmem_spec, any_spec, any_spec),
            scratch_shapes=[
                pltpu.VMEM((N, QK, T), BF16),
                pltpu.VMEM((N, T, D), BF16),
                pltpu.VMEM((N, T, D), BF16),
                pltpu.VMEM((N, QK, T), BF16),
                pltpu.VMEM((N, D, T), BF16),
                pltpu.VMEM((N, QK, T), BF16),
                pltpu.VMEM((N, D, T), BF16),
                pltpu.VMEM((N, QK, T), BF16),
                pltpu.VMEM((N, 3 * C_CHUNK, L), BF16),
                pltpu.VMEM((NT, TK, 2 * D), BF16),
                pltpu.VMEM((NT, QK, TK), BF16),
                pltpu.VMEM((NT, TK, D), BF16),
                pltpu.VMEM((NT, D, TK), BF16),
                pltpu.VMEM((NT, TK, T), F32),
                pltpu.VMEM((NP, TK, T), BF16),
                pltpu.VMEM((2 * D, T), BF16),
                pltpu.VMEM((NT, TK, 2 * D), F32),
                pltpu.VMEM((NT, TK, D), F32),
                pltpu.VMEM((D, T), F32),
                pltpu.VMEM((QK, T), F32),
                pltpu.VMEM((N, 8, T), F32),
                pltpu.VMEM((L, T), F32),
                pltpu.VMEM((L, N * D), BF16),
                pltpu.VMEM((L, N * D), BF16),
                pltpu.VMEM((3 * W_CHUNK, D), F32),
                pltpu.VMEM((3 * W_CHUNK, D), F32),
            ] + [dma((N,))] * 12 + [dma((7,))] + [dma((24,))] * 12,
            compiler_params=pltpu.CompilerParams(
                collective_id=0, has_side_effects=True, vmem_limit_bytes=67043328),
        )(jnp.transpose(queries, (1, 2, 0)), jnp.transpose(d_out, (1, 0, 2)), latent, jnp.transpose(key_rope, (1, 0)),
          w_uk.reshape(L, N * D), w_uv.reshape(L, N * D))

        return (jnp.transpose(o_all, (1, 0, 2)), jnp.transpose(dq_all, (2, 0, 1)), dc, jnp.transpose(drt, (1, 0)),
                jnp.transpose(dwk[:, :L], (1, 0, 2)), jnp.transpose(dwv[:, :L], (1, 0, 2)))

    return jax.shard_map(local_step, mesh=mesh,
                         in_specs=(seq_spec, seq_spec, seq_spec, P(), P(), seq_spec),
                         out_specs=(seq_spec, seq_spec, seq_spec, seq_spec, P(), P()),
                         check_vma=False)
```

```python
import math
import jax
import jax.numpy as jnp
from jax import lax
from jax.experimental import pallas as pl
from jax.experimental.pallas import tpu as pltpu
from jax.sharding import PartitionSpec as P

MESH = pl.DeviceIdType.MESH
BF16 = jnp.bfloat16
F32 = jnp.float32

N = 16
T = 256
L = 512
D = 128
R = 64
QK = D + R
TK = 512
NT = 8
C_CHUNK = 96
W_CHUNK = 176
NP = 72
ORDER = (0, 7, 3, 4, 5, 2, 6, 1)
TABLE = sum(chip << (3 * n) for n, chip in enumerate(ORDER))
SCALE = 1.0 / math.sqrt(QK)
EXP_C = SCALE * math.log2(math.e)


def nt_dot(a, b):
    return lax.dot_general(a, b, (((1,), (1,)), ((), ())), preferred_element_type=F32)


def nn_dot(a, b):
    return lax.dot_general(a, b, (((1,), (0,)), ((), ())), preferred_element_type=F32)


def flip(x, bit):
    return x + bit * (1 - 2 * lax.rem(lax.div(x, bit), 2))


def xor(x, s):
    for bit in (1, 2, 4, 8):
        on = lax.rem(lax.div(s, bit), 2)
        x = x + on * bit * (1 - 2 * lax.rem(lax.div(x, bit), 2))
    return x


def partner(n):
    k = lax.div(n, 2)
    power = (1 + 7 * lax.rem(k, 2)) * (1 + 63 * lax.rem(lax.div(k, 2), 2)) * (1 + 4095 * lax.div(k, 4))
    return 2 * lax.rem(lax.div(TABLE, power), 8) + lax.rem(n, 2)


def fold(x, reduce):
    return reduce(x.reshape(x.shape[0] // 8, 8, x.shape[1]), axis=0)


def transpose(x):
    return jnp.transpose(x, (1, 0))


class Gather:
    def __init__(self, me, own, buf, chunk, send_sem, recv_sem, sib_send, sib_recv):
        self.me, self.own, self.buf, self.chunk = me, own, buf, chunk
        self.send_sem, self.recv_sem = send_sem, recv_sem
        self.sib_send, self.sib_recv = sib_send, sib_recv

    def view(self, src, rows):
        return self.buf.at[src, rows, :]

    def axes(self, k):
        out = []
        for t in range(3):
            axis = lax.rem(k + t, 3)
            out.append(2 + axis * (axis + 1))
        return out

    def make(self, k, masks, mask, target, send_sem, recv_sem):
        src = self.me
        for bit in masks:
            src = flip(src, bit)
        rows = pl.ds(k * self.chunk, self.chunk)
        slot = k * 8 + lax.div(mask, 2)
        first = self.own.at[rows, :] if not masks else self.view(src, rows)
        recv = recv_sem.at[0] if recv_sem is self.sib_recv else recv_sem.at[slot]
        return pltpu.make_async_remote_copy(
            src_ref=first, dst_ref=self.view(src, rows), send_sem=send_sem.at[0], recv_sem=recv,
            device_id=(target,), device_id_type=MESH)

    def hop(self, k, masks, bit):
        return self.make(k, masks, sum(masks) + bit, flip(self.me, bit), self.send_sem, self.recv_sem)

    def sib(self, k, masks):
        return self.make(k, masks, sum(masks), flip(self.me, 1), self.sib_send, self.sib_recv)

    def arrived(self, k, masks):
        self.make(k, masks, sum(masks), flip(self.me, 1), self.send_sem, self.recv_sem).wait_recv()

    def stage0(self):
        for t in range(3):
            def send(k, carry):
                self.hop(k, (), self.axes(k)[t]).start()
                return carry
            lax.fori_loop(0, 3, send, 0)

        def send_sib(k, carry):
            self.sib(k, ()).start()
            return carry
        lax.fori_loop(0, 3, send_sib, 0)

    def stage1(self):
        def step(k, carry):
            a, b, c = self.axes(k)
            self.arrived(k, (a,))
            self.hop(k, (a,), b).start()
            self.hop(k, (a,), c).start()
            self.sib(k, (a,)).start()
            return carry
        lax.fori_loop(0, 3, step, 0)

    def stage2(self):
        for both in (False, True):
            def step(k, carry):
                a, b, c = self.axes(k)
                masks = (a, b) if both else (b,)
                self.arrived(k, masks)
                self.hop(k, masks, c).start()
                self.sib(k, masks).start()
                return carry
            lax.fori_loop(0, 3, step, 0)

    def stage3(self):
        for extra in range(4):
            def step(k, carry):
                a, b, c = self.axes(k)
                masks = ((c,), (a, c), (b, c), (a, b, c))[extra]
                self.arrived(k, masks)
                self.sib(k, masks).start()
                return carry
            lax.fori_loop(0, 3, step, 0)

    def wait_items(self, items, sem):
        ref = self.buf.at[pl.ds(0, items)]
        pltpu.make_async_copy(ref, ref, sem.at[0]).wait()

    def finish(self):
        self.wait_items(8, self.sib_recv)

    def drain(self):
        self.wait_items(7, self.send_sem)
        self.wait_items(8, self.sib_send)


def wait_bytes(ref, sem):
    pltpu.make_async_copy(ref, ref, sem).wait()


def kernel(qt_ref, do_ref, c_ref, rt_ref, wuk_ref, wuv_ref,
           o_ref, dq_ref, dc_ref, drt_ref, dwk_ref, dwv_ref,
           in_q, in_do, stage_o, stage_dq, stage_v, stage_k, in_v, in_k, call, kcat, kt, v, vt, sbuf, prob, qz, qn, dot, dk, dv,
           ot, dqt, delta, dct, wuk, wuv, dwk_own, dwv_own,
           q_send, q_recv, o_send, o_recv, dq_send, dq_recv, v_send, v_recv, k_send, k_recv, local_sem,
           c_send, c_recv, cs_send, cs_recv, gk_send, gk_recv, gks_send, gks_recv, gv_send, gv_recv, gvs_send, gvs_recv):
    me = lax.axis_index("cp")

    loads = [
        pltpu.make_async_copy(wuk_ref, wuk, local_sem.at[0]),
        pltpu.make_async_copy(wuv_ref, wuv, local_sem.at[1]),
        pltpu.make_async_copy(c_ref, call.at[me, pl.ds(0, T), :], local_sem.at[2]),
        pltpu.make_async_copy(rt_ref.at[pl.ds(0, 32), :], call.at[me, pl.ds(T, 32), pl.ds(0, T)], local_sem.at[3]),
        pltpu.make_async_copy(rt_ref.at[pl.ds(32, 32), :], call.at[me, pl.ds(T, 32), pl.ds(T, T)], local_sem.at[4]),
    ]
    for load in loads[::-1]:
        load.start()

    barrier = pltpu.get_barrier_semaphore()

    def hello(s, carry):
        pl.semaphore_signal(barrier, inc=1, device_id=(xor(me, s),), device_id_type=MESH)
        return carry

    lax.fori_loop(1, N, hello, 0)
    for load in loads[2:]:
        load.wait()
    pl.semaphore_wait(barrier, N - 1)

    def send(src, dst, n, send_sem, recv):
        pltpu.make_async_remote_copy(
            src_ref=src, dst_ref=dst.at[me], send_sem=send_sem.at[0], recv_sem=recv,
            device_id=(xor(me, partner(n)),), device_id_type=MESH).start()

    gather_c = Gather(me, call.at[me], call, C_CHUNK, c_send, c_recv, cs_send, cs_recv)
    gather_c.stage0()
    pltpu.make_async_copy(qt_ref.at[me], in_q.at[me], q_recv.at[me]).start()
    pltpu.make_async_copy(do_ref.at[me], in_do.at[me], q_recv.at[me]).start()
    dk[...] = jnp.zeros_like(dk)
    dv[...] = jnp.zeros_like(dv)
    qz[...] = jnp.zeros_like(qz)
    dwk_own[...] = jnp.zeros_like(dwk_own)
    dwv_own[...] = jnp.zeros_like(dwv_own)
    gather_c.stage1()
    gather_c.stage2()

    def send_q(n, carry):
        other = xor(me, partner(n))
        send(qt_ref.at[other], in_q, n, q_send, q_recv.at[me])
        send(do_ref.at[other], in_do, n, q_send, q_recv.at[me])
        return carry

    lax.fori_loop(1, N, send_q, 0)
    for load in loads[:2]:
        load.wait()
    gather_c.stage3()
    gather_c.finish()

    lanes = pl.ds(pl.multiple_of(me * D, D), D)

    def make_kv(jt, carry):
        wcat = jnp.concatenate([wuk[:, lanes], wuv[:, lanes]], axis=1)
        for half in range(2):
            j = jt * 2 + half
            rows = pl.ds(half * T, T)
            kv = nn_dot(call[j, pl.ds(0, T), :], wcat)
            rt = jnp.concatenate([call[j, pl.ds(T, 32), pl.ds(0, T)], call[j, pl.ds(T, 32), pl.ds(T, T)]], axis=0)
            rtz = jnp.concatenate([rt.astype(F32), jnp.zeros((R, T), F32)], axis=0)
            kcat[jt, rows, pl.ds(0, D)] = kv[:, :D].astype(BF16)
            kcat[jt, rows, pl.ds(D, D)] = transpose(rtz).astype(BF16)
            v[jt, rows, :] = kv[:, D:].astype(BF16)
            kvt = transpose(kv).astype(BF16)
            kt[jt, pl.ds(0, D), rows] = kvt[:D]
            kt[jt, pl.ds(D, R), rows] = rt
            vt[jt, :, rows] = kvt[D:]
        return carry

    lax.fori_loop(0, NT, make_kv, 0)

    def first_prob(i):
        half = lax.div(i, 2)
        return (half + lax.rem(i, 2)) * (half + 1)

    def forward(n, carry):
        i = xor(me, partner(n))
        wait_bytes(call.at[0, pl.ds(0, 160), :], q_recv.at[i])
        last = lax.div(i, 2)
        base = first_prob(i)
        qz[pl.ds(0, QK), :] = in_q[i]

        def score_tile(jt, top):
            sc = nn_dot(kcat[jt], qz[...])
            sbuf[jt] = sc
            return jnp.maximum(top, fold(sc, jnp.max))

        top = lax.fori_loop(0, last, score_tile, jnp.full((8, T), -1e30, F32))
        sc = nn_dot(kcat[last], qz[...])
        ahead = lax.broadcasted_iota(jnp.int32, sc.shape, 0) - lax.broadcasted_iota(jnp.int32, sc.shape, 1)
        sc = jnp.where(ahead <= i * T - last * TK, sc, -1e30)
        sbuf[last] = sc
        top = jnp.maximum(top, fold(sc, jnp.max))
        top = jnp.max(top, axis=0, keepdims=True) * EXP_C

        ot[...] = jnp.zeros_like(ot)

        def soft_tile(jt, total):
            e = jnp.exp2(sbuf[jt] * EXP_C - top)
            sbuf[jt] = e
            ot[...] += nn_dot(vt[jt], e.astype(BF16))
            return total + fold(e, jnp.sum)

        total = lax.fori_loop(0, last + 1, soft_tile, jnp.zeros((8, T), F32))
        inv = 1.0 / jnp.sum(total, axis=0, keepdims=True)
        o_t = ot[...] * inv
        stage_o[n] = transpose(o_t).astype(BF16)

        @pl.when(n > 0)
        def _():
            send(stage_o.at[n], o_ref, n, o_send, o_recv.at[0])

        do_t = transpose(in_do[i].astype(F32))
        dot[n] = do_t.astype(BF16)
        delta[n] = jnp.broadcast_to(jnp.sum(o_t * do_t, axis=0, keepdims=True), (8, T))

        def value_tile(jt, c):
            p = (sbuf[jt] * inv).astype(BF16)
            prob[base + jt] = p
            dv[jt] += nn_dot(p, in_do[i])
            return c

        lax.fori_loop(0, last + 1, value_tile, 0)
        return carry

    lax.fori_loop(0, N, forward, 0)
    pltpu.make_async_copy(stage_o.at[0], o_ref.at[me], o_recv.at[0]).start()

    def block_rows(i):
        return pl.ds(pl.multiple_of(lax.rem(i, 2) * T, T), T)

    def grad_v(n, carry):
        i = xor(me, partner(n))
        stage_v[n] = transpose(dv[lax.div(i, 2), block_rows(i), :]).astype(BF16)
        return carry

    def weight_grad(stage, own):
        def step(m, acc):
            lhs = jnp.concatenate([stage[4 * m + r, pl.ds(0, D), :] for r in range(4)], axis=1)
            rhs = jnp.concatenate([call[xor(me, partner(4 * m + r)), pl.ds(0, T), :] for r in range(4)], axis=0)
            return acc + nn_dot(lhs, rhs)

        dwt = lax.fori_loop(0, 4, step, jnp.zeros((D, L), F32))
        own[pl.ds(0, L), :] = transpose(dwt)

    lax.fori_loop(0, N, grad_v, 0)
    pltpu.make_async_copy(stage_v.at[0], in_v.at[me], v_recv.at[0]).start()
    weight_grad(stage_v, dwv_own)
    gather_v = Gather(me, dwv_own, dwv_ref, W_CHUNK, gv_send, gv_recv, gvs_send, gvs_recv)
    all_rows = pl.ds(0, 3 * W_CHUNK)
    own_v = pltpu.make_async_copy(dwv_own, gather_v.view(me, all_rows), local_sem.at[5])
    own_v.start()
    gather_v.stage0()

    def backward(n, carry):
        i = xor(me, partner(n))
        last = lax.div(i, 2)
        base = first_prob(i)
        qz[pl.ds(0, QK), :] = in_q[i]
        qn[...] = transpose(qz[...].astype(F32)).astype(BF16)
        dqt[...] = jnp.zeros_like(dqt)
        row_delta = delta[n, pl.ds(0, 1), :]

        sbuf[0] = nn_dot(v[0], dot[n])

        def back_tile(jt, c):
            ds = (prob[base + jt].astype(F32) * (sbuf[jt] - row_delta)).astype(BF16)
            dp = nn_dot(v[lax.rem(jt + 1, NT)], dot[n])
            dk[jt] += nn_dot(ds, qn[...])
            dqt[...] += nn_dot(kt[jt], ds)
            sbuf[jt + 1] = dp
            return c

        lax.fori_loop(0, last + 1, back_tile, 0)
        stage_dq[n] = (dqt[...] * SCALE).astype(BF16)

        @pl.when(n > 0)
        def _():
            send(stage_dq.at[n], dq_ref, n, dq_send, dq_recv.at[0])
            send(stage_v.at[n], in_v, n, v_send, v_recv.at[0])

        @pl.when(n == 3)
        def _():
            gather_v.stage1()

        @pl.when(n == 7)
        def _():
            gather_v.stage2()

        @pl.when(n == 11)
        def _():
            gather_v.stage3()

        return carry

    lax.fori_loop(0, N, backward, 0)
    pltpu.make_async_copy(stage_dq.at[0], dq_ref.at[me], dq_recv.at[0]).start()

    def grad_k(n, carry):
        i = xor(me, partner(n))
        key = transpose(dk[lax.div(i, 2), block_rows(i), :] * SCALE)
        stage_k[n] = key[:QK].astype(BF16)
        return carry

    lax.fori_loop(0, N, grad_k, 0)
    pltpu.make_async_copy(stage_k.at[0], in_k.at[me], k_recv.at[0]).start()

    def send_k(n, carry):
        send(stage_k.at[n], in_k, n, k_send, k_recv.at[0])
        return carry

    lax.fori_loop(1, 4, send_k, 0)
    weight_grad(stage_k, dwk_own)
    gather_k = Gather(me, dwk_own, dwk_ref, W_CHUNK, gk_send, gk_recv, gks_send, gks_recv)
    own_k = pltpu.make_async_copy(dwk_own, gather_k.view(me, all_rows), local_sem.at[6])
    own_k.start()
    gather_k.stage0()
    lax.fori_loop(4, 8, send_k, 0)

    dct[...] = jnp.zeros_like(dct)

    wait_bytes(in_v, v_recv.at[0])

    def latent_from_v(h, carry):
        cols = pl.ds(pl.multiple_of(h * D, D), D)
        dct[...] += nn_dot(wuv[:, cols], in_v[h])
        return carry

    lax.fori_loop(0, N, latent_from_v, 0)
    gather_k.stage1()
    lax.fori_loop(8, N, send_k, 0)
    gather_k.stage2()

    wait_bytes(in_k, k_recv.at[0])

    def latent_from_k(h, acc):
        cols = pl.ds(pl.multiple_of(h * D, D), D)
        dct[...] += nn_dot(wuk[:, cols], in_k[h, pl.ds(0, D), :])
        return acc + in_k[h, pl.ds(D, R), :].astype(F32)

    drt_ref[...] = lax.fori_loop(0, N, latent_from_k, jnp.zeros((R, T), F32)).astype(BF16)
    dc_ref[...] = transpose(dct[...]).astype(BF16)

    gather_k.stage3()
    gather_v.finish()
    gather_k.finish()
    own_v.wait()
    own_k.wait()

    wait_bytes(o_ref, o_recv.at[0])
    wait_bytes(dq_ref, dq_recv.at[0])
    others = pl.ds(0, N - 1)
    wait_bytes(qt_ref.at[others], q_send.at[0])
    wait_bytes(do_ref.at[others], q_send.at[0])
    wait_bytes(stage_o.at[others], o_send.at[0])
    wait_bytes(stage_dq.at[others], dq_send.at[0])
    wait_bytes(stage_v.at[others], v_send.at[0])
    wait_bytes(stage_k.at[others], k_send.at[0])
    gather_c.drain()
    gather_v.drain()
    gather_k.drain()


def solution(mesh):
    seq_spec = P("cp")

    def local_step(queries, latent, key_rope, w_uk, w_uv, d_out):
        any_spec = pl.BlockSpec(memory_space=pl.ANY)
        vmem_spec = pl.BlockSpec(memory_space=pltpu.VMEM)
        dma = pltpu.SemaphoreType.DMA
        o_all, dq_all, dc, drt, dwk, dwv = pl.pallas_call(
            kernel,
            name="mla_core",
            out_shape=(jax.ShapeDtypeStruct((N, T, D), BF16),
                       jax.ShapeDtypeStruct((N, QK, T), BF16),
                       jax.ShapeDtypeStruct((T, L), BF16),
                       jax.ShapeDtypeStruct((R, T), BF16),
                       jax.ShapeDtypeStruct((N, 3 * W_CHUNK, D), F32),
                       jax.ShapeDtypeStruct((N, 3 * W_CHUNK, D), F32)),
            in_specs=[any_spec] * 6,
            out_specs=(any_spec, any_spec, vmem_spec, vmem_spec, any_spec, any_spec),
            scratch_shapes=[
                pltpu.VMEM((N, QK, T), BF16),
                pltpu.VMEM((N, T, D), BF16),
                pltpu.VMEM((N, T, D), BF16),
                pltpu.VMEM((N, QK, T), BF16),
                pltpu.VMEM((N, D, T), BF16),
                pltpu.VMEM((N, QK, T), BF16),
                pltpu.VMEM((N, D, T), BF16),
                pltpu.VMEM((N, QK, T), BF16),
                pltpu.VMEM((N, 3 * C_CHUNK, L), BF16),
                pltpu.VMEM((NT, TK, 2 * D), BF16),
                pltpu.VMEM((NT, QK, TK), BF16),
                pltpu.VMEM((NT, TK, D), BF16),
                pltpu.VMEM((NT, D, TK), BF16),
                pltpu.VMEM((NT + 1, TK, T), F32),
                pltpu.VMEM((NP, TK, T), BF16),
                pltpu.VMEM((2 * D, T), BF16),
                pltpu.VMEM((T, 2 * D), BF16),
                pltpu.VMEM((N, D, T), BF16),
                pltpu.VMEM((NT, TK, 2 * D), F32),
                pltpu.VMEM((NT, TK, D), F32),
                pltpu.VMEM((D, T), F32),
                pltpu.VMEM((QK, T), F32),
                pltpu.VMEM((N, 8, T), F32),
                pltpu.VMEM((L, T), F32),
                pltpu.VMEM((L, N * D), BF16),
                pltpu.VMEM((L, N * D), BF16),
                pltpu.VMEM((3 * W_CHUNK, D), F32),
                pltpu.VMEM((3 * W_CHUNK, D), F32),
            ] + [dma((1,)), dma((N,))] + [dma((1,))] * 8 + [dma((7,))] + [dma((1,)), dma((24,)), dma((1,)), dma((1,))] * 3,
            compiler_params=pltpu.CompilerParams(
                collective_id=0, has_side_effects=True, vmem_limit_bytes=67043328),
        )(jnp.transpose(queries, (1, 2, 0)), jnp.transpose(d_out, (1, 0, 2)), latent, jnp.transpose(key_rope, (1, 0)),
          w_uk.reshape(L, N * D), w_uv.reshape(L, N * D))

        return (jnp.transpose(o_all, (1, 0, 2)), jnp.transpose(dq_all, (2, 0, 1)), dc, jnp.transpose(drt, (1, 0)),
                jnp.transpose(dwk[:, :L], (1, 0, 2)), jnp.transpose(dwv[:, :L], (1, 0, 2)))

    return jax.shard_map(local_step, mesh=mesh,
                         in_specs=(seq_spec, seq_spec, seq_spec, P(), P(), seq_spec),
                         out_specs=(seq_spec, seq_spec, seq_spec, seq_spec, P(), P()),
                         check_vma=False)
```

```python
import math
import jax
import jax.numpy as jnp
from jax import lax
from jax.experimental import pallas as pl
from jax.experimental.pallas import tpu as pltpu
from jax.sharding import PartitionSpec as P

MESH = pl.DeviceIdType.MESH
BF16 = jnp.bfloat16
F32 = jnp.float32

N = 16
T = 256
L = 512
D = 128
R = 64
QK = D + R
TK = 512
NT = 8
C_CHUNK = 96
W_CHUNK = 176
TILES = 9
ORDER = (0, 7, 3, 4, 5, 2, 6, 1)
TABLE = sum(chip << (3 * n) for n, chip in enumerate(ORDER))
SCALE = 1.0 / math.sqrt(QK)
EXP_C = SCALE * math.log2(math.e)


def nt_dot(a, b):
    return lax.dot_general(a, b, (((1,), (1,)), ((), ())), preferred_element_type=F32)


def nn_dot(a, b):
    return lax.dot_general(a, b, (((1,), (0,)), ((), ())), preferred_element_type=F32)


def flip(x, bit):
    return x + bit * (1 - 2 * lax.rem(lax.div(x, bit), 2))


def xor(x, s):
    for bit in (1, 2, 4, 8):
        on = lax.rem(lax.div(s, bit), 2)
        x = x + on * bit * (1 - 2 * lax.rem(lax.div(x, bit), 2))
    return x


def partner(n):
    k = lax.div(n, 2)
    power = (1 + 7 * lax.rem(k, 2)) * (1 + 63 * lax.rem(lax.div(k, 2), 2)) * (1 + 4095 * lax.div(k, 4))
    return 2 * lax.rem(lax.div(TABLE, power), 8) + lax.rem(n, 2)


def fold(x, reduce):
    return reduce(x.reshape(x.shape[0] // 8, 8, x.shape[1]), axis=0)


def transpose(x):
    return jnp.transpose(x, (1, 0))


class Gather:
    def __init__(self, me, own, buf, chunk, send_sem, recv_sem, sib_send, sib_recv):
        self.me, self.own, self.buf, self.chunk = me, own, buf, chunk
        self.send_sem, self.recv_sem = send_sem, recv_sem
        self.sib_send, self.sib_recv = sib_send, sib_recv

    def view(self, src, rows):
        return self.buf.at[src, rows, :]

    def axes(self, k):
        out = []
        for t in range(3):
            axis = lax.rem(k + t, 3)
            out.append(2 + axis * (axis + 1))
        return out

    def make(self, k, masks, mask, target, send_sem, recv_sem):
        src = self.me
        for bit in masks:
            src = flip(src, bit)
        rows = pl.ds(k * self.chunk, self.chunk)
        slot = k * 8 + lax.div(mask, 2)
        first = self.own.at[rows, :] if not masks else self.view(src, rows)
        recv = recv_sem.at[0] if recv_sem is self.sib_recv else recv_sem.at[slot]
        return pltpu.make_async_remote_copy(
            src_ref=first, dst_ref=self.view(src, rows), send_sem=send_sem.at[0], recv_sem=recv,
            device_id=(target,), device_id_type=MESH)

    def hop(self, k, masks, bit):
        return self.make(k, masks, sum(masks) + bit, flip(self.me, bit), self.send_sem, self.recv_sem)

    def sib(self, k, masks):
        return self.make(k, masks, sum(masks), flip(self.me, 1), self.sib_send, self.sib_recv)

    def arrived(self, k, masks):
        self.make(k, masks, sum(masks), flip(self.me, 1), self.send_sem, self.recv_sem).wait_recv()

    def stage0(self):
        for t in range(3):
            def send(k, carry):
                self.hop(k, (), self.axes(k)[t]).start()
                return carry
            lax.fori_loop(0, 3, send, 0)

        def send_sib(k, carry):
            self.sib(k, ()).start()
            return carry
        lax.fori_loop(0, 3, send_sib, 0)

    def stage1(self):
        def step(k, carry):
            a, b, c = self.axes(k)
            self.arrived(k, (a,))
            self.hop(k, (a,), b).start()
            self.hop(k, (a,), c).start()
            self.sib(k, (a,)).start()
            return carry
        lax.fori_loop(0, 3, step, 0)

    def stage2(self):
        for both in (False, True):
            def step(k, carry):
                a, b, c = self.axes(k)
                masks = (a, b) if both else (b,)
                self.arrived(k, masks)
                self.hop(k, masks, c).start()
                self.sib(k, masks).start()
                return carry
            lax.fori_loop(0, 3, step, 0)

    def stage3(self):
        for extra in range(4):
            def step(k, carry):
                a, b, c = self.axes(k)
                masks = ((c,), (a, c), (b, c), (a, b, c))[extra]
                self.arrived(k, masks)
                self.sib(k, masks).start()
                return carry
            lax.fori_loop(0, 3, step, 0)

    def wait_items(self, items, sem):
        ref = self.buf.at[pl.ds(0, items)]
        pltpu.make_async_copy(ref, ref, sem.at[0]).wait()

    def finish(self):
        self.wait_items(8, self.sib_recv)

    def drain(self):
        self.wait_items(7, self.send_sem)
        self.wait_items(8, self.sib_send)


def wait_bytes(ref, sem):
    pltpu.make_async_copy(ref, ref, sem).wait()


def kernel(qt_ref, do_ref, c_ref, rt_ref, wuk_ref, wuv_ref,
           o_ref, dq_ref, dc_ref, drt_ref, dwk_ref, dwv_ref,
           in_q, in_do, stage_o, stage_dq, stage_v, stage_k, in_v, in_k, call, kcat, kt, v, vt, sbuf, prob, qz, qn, dot, own_do, dk, dv,
           ot, dqt, delta, dct, wuk, wuv, dwk_own, dwv_own,
           q_send, q_recv, o_send, o_recv, dq_send, dq_recv, v_send, v_recv, k_send, k_recv, local_sem,
           c_send, c_recv, cs_send, cs_recv, gk_send, gk_recv, gks_send, gks_recv, gv_send, gv_recv, gvs_send, gvs_recv):
    me = lax.axis_index("cp")

    loads = [
        pltpu.make_async_copy(wuk_ref, wuk, local_sem.at[0]),
        pltpu.make_async_copy(wuv_ref, wuv, local_sem.at[1]),
        pltpu.make_async_copy(c_ref, call.at[me, pl.ds(0, T), :], local_sem.at[2]),
        pltpu.make_async_copy(rt_ref.at[pl.ds(0, 32), :], call.at[me, pl.ds(T, 32), pl.ds(0, T)], local_sem.at[3]),
        pltpu.make_async_copy(rt_ref.at[pl.ds(32, 32), :], call.at[me, pl.ds(T, 32), pl.ds(T, T)], local_sem.at[4]),
    ]
    for load in loads[::-1]:
        load.start()

    barrier = pltpu.get_barrier_semaphore()

    def hello(s, carry):
        pl.semaphore_signal(barrier, inc=1, device_id=(xor(me, s),), device_id_type=MESH)
        return carry

    lax.fori_loop(1, N, hello, 0)
    for load in loads[2:]:
        load.wait()
    pl.semaphore_wait(barrier, N - 1)

    def send(src, dst, n, send_sem, recv):
        pltpu.make_async_remote_copy(
            src_ref=src, dst_ref=dst.at[me], send_sem=send_sem.at[0], recv_sem=recv,
            device_id=(xor(me, partner(n)),), device_id_type=MESH).start()

    gather_c = Gather(me, call.at[me], call, C_CHUNK, c_send, c_recv, cs_send, cs_recv)
    gather_c.stage0()
    pltpu.make_async_copy(qt_ref.at[me], in_q.at[me], q_recv.at[me]).start()
    pltpu.make_async_copy(do_ref.at[me], in_do.at[me], q_recv.at[me]).start()
    dk[...] = jnp.zeros_like(dk)
    dv[...] = jnp.zeros_like(dv)
    qz[...] = jnp.zeros_like(qz)
    dwk_own[...] = jnp.zeros_like(dwk_own)
    dwv_own[...] = jnp.zeros_like(dwv_own)
    gather_c.stage1()
    gather_c.stage2()

    def send_q(n, carry):
        other = xor(me, partner(n))
        send(qt_ref.at[other], in_q, n, q_send, q_recv.at[me])
        send(do_ref.at[other], in_do, n, q_send, q_recv.at[me])
        return carry

    lax.fori_loop(1, N, send_q, 0)
    for load in loads[:2]:
        load.wait()
    gather_c.stage3()
    gather_c.finish()

    lanes = pl.ds(pl.multiple_of(me * D, D), D)

    def make_kv(jt, carry):
        wcat = jnp.concatenate([wuk[:, lanes], wuv[:, lanes]], axis=1)
        for half in range(2):
            j = jt * 2 + half
            rows = pl.ds(half * T, T)
            kv = nn_dot(call[j, pl.ds(0, T), :], wcat)
            rt = jnp.concatenate([call[j, pl.ds(T, 32), pl.ds(0, T)], call[j, pl.ds(T, 32), pl.ds(T, T)]], axis=0)
            rtz = jnp.concatenate([rt.astype(F32), jnp.zeros((R, T), F32)], axis=0)
            kcat[jt, rows, pl.ds(0, D)] = kv[:, :D].astype(BF16)
            kcat[jt, rows, pl.ds(D, D)] = transpose(rtz).astype(BF16)
            v[jt, rows, :] = kv[:, D:].astype(BF16)
            kvt = transpose(kv).astype(BF16)
            kt[jt, pl.ds(0, D), rows] = kvt[:D]
            kt[jt, pl.ds(D, R), rows] = rt
            vt[jt, :, rows] = kvt[D:]
        return carry

    lax.fori_loop(0, NT, make_kv, 0)

    def pair(p):
        na = 4 * lax.div(p, 2) + lax.rem(p, 2)
        nb = 4 * lax.div(p, 2) + 3 - lax.rem(p, 2)
        ia, ib = xor(me, partner(na)), xor(me, partner(nb))
        split = lax.div(ia, 2) + 1
        which = [jnp.minimum(lax.div(t, split), 1) for t in range(TILES)]
        tile = [t - w * split for t, w in enumerate(which)]
        return (na, nb), (ia, ib), which, tile

    def pick(w, rows):
        return jnp.where(w == 1, rows[1], rows[0])

    def forward(p, carry):
        steps, blocks, which, tile = pair(p)
        for b, i in enumerate(blocks):
            wait_bytes(call.at[0, pl.ds(0, 160), :], q_recv.at[i])
            qz[b, pl.ds(0, QK), :] = in_q[i]
            own_do[b] = in_do[i]

        tops = [jnp.full((8, T), -1e30, F32)] * 2
        for t in range(TILES):
            w, jt = which[t], tile[t]
            sc = nn_dot(kcat[jt], qz[w])
            ahead = lax.broadcasted_iota(jnp.int32, sc.shape, 0) - lax.broadcasted_iota(jnp.int32, sc.shape, 1)
            i = blocks[0] + w * (blocks[1] - blocks[0])
            sc = jnp.where(ahead <= i * T - jt * TK, sc, -1e30)
            sbuf[t] = sc
            top = fold(sc, jnp.max)
            tops = [jnp.where(w == b, jnp.maximum(tops[b], top), tops[b]) for b in range(2)]
        tops = [jnp.max(x, axis=0, keepdims=True) * EXP_C for x in tops]

        ot[...] = jnp.zeros_like(ot)
        totals = [jnp.zeros((8, T), F32)] * 2
        for t in range(TILES):
            w, jt = which[t], tile[t]
            e = jnp.exp2(sbuf[t] * EXP_C - pick(w, tops))
            sbuf[t] = e
            ot[w] += nn_dot(vt[jt], e.astype(BF16))
            total = fold(e, jnp.sum)
            totals = [jnp.where(w == b, totals[b] + total, totals[b]) for b in range(2)]
        invs = [1.0 / jnp.sum(x, axis=0, keepdims=True) for x in totals]

        for t in range(TILES):
            w, jt = which[t], tile[t]
            prob_t = (sbuf[t] * pick(w, invs)).astype(BF16)
            prob[p * TILES + t] = prob_t
            dv[jt] += nn_dot(prob_t, own_do[w])

        for b, n in enumerate(steps):
            o_t = ot[b] * invs[b]
            stage_o[n] = transpose(o_t).astype(BF16)
            do_t = transpose(own_do[b].astype(F32))
            dot[p * 2 + b] = do_t.astype(BF16)
            delta[p * 2 + b] = jnp.broadcast_to(jnp.sum(o_t * do_t, axis=0, keepdims=True), (8, T))

            @pl.when(n > 0)
            def _():
                send(stage_o.at[n], o_ref, n, o_send, o_recv.at[0])

        return carry

    lax.fori_loop(0, N // 2, forward, 0)
    pltpu.make_async_copy(stage_o.at[0], o_ref.at[me], o_recv.at[0]).start()

    def block_rows(i):
        return pl.ds(pl.multiple_of(lax.rem(i, 2) * T, T), T)

    def grad_v(n, carry):
        i = xor(me, partner(n))
        stage_v[n] = transpose(dv[lax.div(i, 2), block_rows(i), :]).astype(BF16)
        return carry

    def weight_grad(stage, own):
        def step(m, acc):
            lhs = jnp.concatenate([stage[4 * m + r, pl.ds(0, D), :] for r in range(4)], axis=1)
            rhs = jnp.concatenate([call[xor(me, partner(4 * m + r)), pl.ds(0, T), :] for r in range(4)], axis=0)
            return acc + nn_dot(lhs, rhs)

        dwt = lax.fori_loop(0, 4, step, jnp.zeros((D, L), F32))
        own[pl.ds(0, L), :] = transpose(dwt)

    lax.fori_loop(0, N, grad_v, 0)
    pltpu.make_async_copy(stage_v.at[0], in_v.at[me], v_recv.at[0]).start()
    weight_grad(stage_v, dwv_own)
    gather_v = Gather(me, dwv_own, dwv_ref, W_CHUNK, gv_send, gv_recv, gvs_send, gvs_recv)
    all_rows = pl.ds(0, 3 * W_CHUNK)
    own_v = pltpu.make_async_copy(dwv_own, gather_v.view(me, all_rows), local_sem.at[5])
    own_v.start()
    gather_v.stage0()

    def backward(p, carry):
        steps, blocks, which, tile = pair(p)
        for b, i in enumerate(blocks):
            qz[b, pl.ds(0, QK), :] = in_q[i]
            qn[b] = transpose(qz[b].astype(F32)).astype(BF16)
        dqt[...] = jnp.zeros_like(dqt)
        deltas = [delta[p * 2 + b, pl.ds(0, 1), :] for b in range(2)]
        for t in range(TILES):
            w, jt = which[t], tile[t]
            dp = nn_dot(v[jt], dot[p * 2 + w])
            ds = (prob[p * TILES + t].astype(F32) * (dp - pick(w, deltas))).astype(BF16)
            dk[jt] += nn_dot(ds, qn[w])
            dqt[w] += nn_dot(kt[jt], ds)

        for b, n in enumerate(steps):
            stage_dq[n] = (dqt[b] * SCALE).astype(BF16)

            @pl.when(n > 0)
            def _():
                send(stage_dq.at[n], dq_ref, n, dq_send, dq_recv.at[0])
                send(stage_v.at[n], in_v, n, v_send, v_recv.at[0])

        @pl.when(p == 2)
        def _():
            gather_v.stage1()

        @pl.when(p == 4)
        def _():
            gather_v.stage2()

        @pl.when(p == 6)
        def _():
            gather_v.stage3()

        return carry

    lax.fori_loop(0, N // 2, backward, 0)
    pltpu.make_async_copy(stage_dq.at[0], dq_ref.at[me], dq_recv.at[0]).start()

    def grad_k(n, carry):
        i = xor(me, partner(n))
        key = transpose(dk[lax.div(i, 2), block_rows(i), :] * SCALE)
        stage_k[n] = key[:QK].astype(BF16)
        return carry

    lax.fori_loop(0, N, grad_k, 0)
    pltpu.make_async_copy(stage_k.at[0], in_k.at[me], k_recv.at[0]).start()

    def send_k(n, carry):
        send(stage_k.at[n], in_k, n, k_send, k_recv.at[0])
        return carry

    lax.fori_loop(1, 4, send_k, 0)
    weight_grad(stage_k, dwk_own)
    gather_k = Gather(me, dwk_own, dwk_ref, W_CHUNK, gk_send, gk_recv, gks_send, gks_recv)
    own_k = pltpu.make_async_copy(dwk_own, gather_k.view(me, all_rows), local_sem.at[6])
    own_k.start()
    gather_k.stage0()
    lax.fori_loop(4, 8, send_k, 0)

    dct[...] = jnp.zeros_like(dct)

    wait_bytes(in_v, v_recv.at[0])

    def latent_from_v(h, carry):
        cols = pl.ds(pl.multiple_of(h * D, D), D)
        dct[...] += nn_dot(wuv[:, cols], in_v[h])
        return carry

    lax.fori_loop(0, N, latent_from_v, 0)
    gather_k.stage1()
    lax.fori_loop(8, N, send_k, 0)
    gather_k.stage2()

    wait_bytes(in_k, k_recv.at[0])

    def latent_from_k(h, acc):
        cols = pl.ds(pl.multiple_of(h * D, D), D)
        dct[...] += nn_dot(wuk[:, cols], in_k[h, pl.ds(0, D), :])
        return acc + in_k[h, pl.ds(D, R), :].astype(F32)

    drt_ref[...] = lax.fori_loop(0, N, latent_from_k, jnp.zeros((R, T), F32)).astype(BF16)
    dc_ref[...] = transpose(dct[...]).astype(BF16)

    gather_k.stage3()
    gather_v.finish()
    gather_k.finish()
    own_v.wait()
    own_k.wait()

    wait_bytes(o_ref, o_recv.at[0])
    wait_bytes(dq_ref, dq_recv.at[0])
    others = pl.ds(0, N - 1)
    wait_bytes(qt_ref.at[others], q_send.at[0])
    wait_bytes(do_ref.at[others], q_send.at[0])
    wait_bytes(stage_o.at[others], o_send.at[0])
    wait_bytes(stage_dq.at[others], dq_send.at[0])
    wait_bytes(stage_v.at[others], v_send.at[0])
    wait_bytes(stage_k.at[others], k_send.at[0])
    gather_c.drain()
    gather_v.drain()
    gather_k.drain()


def solution(mesh):
    seq_spec = P("cp")

    def local_step(queries, latent, key_rope, w_uk, w_uv, d_out):
        any_spec = pl.BlockSpec(memory_space=pl.ANY)
        vmem_spec = pl.BlockSpec(memory_space=pltpu.VMEM)
        dma = pltpu.SemaphoreType.DMA
        o_all, dq_all, dc, drt, dwk, dwv = pl.pallas_call(
            kernel,
            name="mla_core",
            out_shape=(jax.ShapeDtypeStruct((N, T, D), BF16),
                       jax.ShapeDtypeStruct((N, QK, T), BF16),
                       jax.ShapeDtypeStruct((T, L), BF16),
                       jax.ShapeDtypeStruct((R, T), BF16),
                       jax.ShapeDtypeStruct((N, 3 * W_CHUNK, D), F32),
                       jax.ShapeDtypeStruct((N, 3 * W_CHUNK, D), F32)),
            in_specs=[any_spec] * 6,
            out_specs=(any_spec, any_spec, vmem_spec, vmem_spec, any_spec, any_spec),
            scratch_shapes=[
                pltpu.VMEM((N, QK, T), BF16),
                pltpu.VMEM((N, T, D), BF16),
                pltpu.VMEM((N, T, D), BF16),
                pltpu.VMEM((N, QK, T), BF16),
                pltpu.VMEM((N, D, T), BF16),
                pltpu.VMEM((N, QK, T), BF16),
                pltpu.VMEM((N, D, T), BF16),
                pltpu.VMEM((N, QK, T), BF16),
                pltpu.VMEM((N, 3 * C_CHUNK, L), BF16),
                pltpu.VMEM((NT, TK, 2 * D), BF16),
                pltpu.VMEM((NT, QK, TK), BF16),
                pltpu.VMEM((NT, TK, D), BF16),
                pltpu.VMEM((NT, D, TK), BF16),
                pltpu.VMEM((TILES, TK, T), F32),
                pltpu.VMEM((N // 2 * TILES, TK, T), BF16),
                pltpu.VMEM((2, 2 * D, T), BF16),
                pltpu.VMEM((2, T, 2 * D), BF16),
                pltpu.VMEM((N, D, T), BF16),
                pltpu.VMEM((2, T, D), BF16),
                pltpu.VMEM((NT, TK, 2 * D), F32),
                pltpu.VMEM((NT, TK, D), F32),
                pltpu.VMEM((2, D, T), F32),
                pltpu.VMEM((2, QK, T), F32),
                pltpu.VMEM((N, 8, T), F32),
                pltpu.VMEM((L, T), F32),
                pltpu.VMEM((L, N * D), BF16),
                pltpu.VMEM((L, N * D), BF16),
                pltpu.VMEM((3 * W_CHUNK, D), F32),
                pltpu.VMEM((3 * W_CHUNK, D), F32),
            ] + [dma((1,)), dma((N,))] + [dma((1,))] * 8 + [dma((7,))] + [dma((1,)), dma((24,)), dma((1,)), dma((1,))] * 3,
            compiler_params=pltpu.CompilerParams(
                collective_id=0, has_side_effects=True, vmem_limit_bytes=67043328),
        )(jnp.transpose(queries, (1, 2, 0)), jnp.transpose(d_out, (1, 0, 2)), latent, jnp.transpose(key_rope, (1, 0)),
          w_uk.reshape(L, N * D), w_uv.reshape(L, N * D))

        return (jnp.transpose(o_all, (1, 0, 2)), jnp.transpose(dq_all, (2, 0, 1)), dc, jnp.transpose(drt, (1, 0)),
                jnp.transpose(dwk[:, :L], (1, 0, 2)), jnp.transpose(dwv[:, :L], (1, 0, 2)))

    return jax.shard_map(local_step, mesh=mesh,
                         in_specs=(seq_spec, seq_spec, seq_spec, P(), P(), seq_spec),
                         out_specs=(seq_spec, seq_spec, seq_spec, seq_spec, P(), P()),
                         check_vma=False)
```

```python
import math
import jax
import jax.numpy as jnp
from jax import lax
from jax.experimental import pallas as pl
from jax.experimental.pallas import tpu as pltpu
from jax.sharding import PartitionSpec as P

MESH = pl.DeviceIdType.MESH
BF16 = jnp.bfloat16
F32 = jnp.float32

N = 16
T = 256
L = 512
D = 128
R = 64
QK = D + R
TK = 512
NT = 8
C_CHUNK = 96
W_CHUNK = 176
TILES = 9
ORDER = (0, 7, 3, 4, 5, 2, 6, 1)
TABLE = sum(chip << (3 * n) for n, chip in enumerate(ORDER))
SCALE = 1.0 / math.sqrt(QK)
EXP_C = SCALE * math.log2(math.e)


def nt_dot(a, b):
    return lax.dot_general(a, b, (((1,), (1,)), ((), ())), preferred_element_type=F32)


def nn_dot(a, b):
    return lax.dot_general(a, b, (((1,), (0,)), ((), ())), preferred_element_type=F32)


def flip(x, bit):
    return x + bit * (1 - 2 * lax.rem(lax.div(x, bit), 2))


def xor(x, s):
    for bit in (1, 2, 4, 8):
        on = lax.rem(lax.div(s, bit), 2)
        x = x + on * bit * (1 - 2 * lax.rem(lax.div(x, bit), 2))
    return x


def partner(n):
    k = lax.div(n, 2)
    power = (1 + 7 * lax.rem(k, 2)) * (1 + 63 * lax.rem(lax.div(k, 2), 2)) * (1 + 4095 * lax.div(k, 4))
    return 2 * lax.rem(lax.div(TABLE, power), 8) + lax.rem(n, 2)


def fold(x, reduce):
    return reduce(x.reshape(x.shape[0] // 8, 8, x.shape[1]), axis=0)


def transpose(x):
    return jnp.transpose(x, (1, 0))


class Gather:
    def __init__(self, me, own, buf, by_row, chunk, send_sem, recv_sem, sib_send, sib_recv):
        self.me, self.own, self.buf, self.by_row, self.chunk = me, own, buf, by_row, chunk
        self.send_sem, self.recv_sem = send_sem, recv_sem
        self.sib_send, self.sib_recv = sib_send, sib_recv

    def view(self, src, rows):
        return self.buf.at[rows, src, 0, :] if self.by_row else self.buf.at[src, rows, :]

    def axes(self, k):
        out = []
        for t in range(3):
            axis = lax.rem(k + t, 3)
            out.append(2 + axis * (axis + 1))
        return out

    def make(self, k, masks, mask, target, send_sem, recv_sem):
        src = self.me
        for bit in masks:
            src = flip(src, bit)
        rows = pl.ds(k * self.chunk, self.chunk)
        slot = k * 8 + lax.div(mask, 2)
        first = self.own.at[rows, :] if not masks else self.view(src, rows)
        recv = recv_sem.at[0] if recv_sem is self.sib_recv else recv_sem.at[slot]
        return pltpu.make_async_remote_copy(
            src_ref=first, dst_ref=self.view(src, rows), send_sem=send_sem.at[0], recv_sem=recv,
            device_id=(target,), device_id_type=MESH)

    def hop(self, k, masks, bit):
        return self.make(k, masks, sum(masks) + bit, flip(self.me, bit), self.send_sem, self.recv_sem)

    def sib(self, k, masks):
        return self.make(k, masks, sum(masks), flip(self.me, 1), self.sib_send, self.sib_recv)

    def arrived(self, k, masks):
        self.make(k, masks, sum(masks), flip(self.me, 1), self.send_sem, self.recv_sem).wait_recv()

    def stage0(self):
        for t in range(3):
            def send(k, carry):
                self.hop(k, (), self.axes(k)[t]).start()
                return carry
            lax.fori_loop(0, 3, send, 0)

        def send_sib(k, carry):
            self.sib(k, ()).start()
            return carry
        lax.fori_loop(0, 3, send_sib, 0)

    def stage1(self):
        def step(k, carry):
            a, b, c = self.axes(k)
            self.arrived(k, (a,))
            self.hop(k, (a,), b).start()
            self.hop(k, (a,), c).start()
            self.sib(k, (a,)).start()
            return carry
        lax.fori_loop(0, 3, step, 0)

    def stage2(self):
        for both in (False, True):
            def step(k, carry):
                a, b, c = self.axes(k)
                masks = (a, b) if both else (b,)
                self.arrived(k, masks)
                self.hop(k, masks, c).start()
                self.sib(k, masks).start()
                return carry
            lax.fori_loop(0, 3, step, 0)

    def stage3(self):
        for extra in range(4):
            def step(k, carry):
                a, b, c = self.axes(k)
                masks = ((c,), (a, c), (b, c), (a, b, c))[extra]
                self.arrived(k, masks)
                self.sib(k, masks).start()
                return carry
            lax.fori_loop(0, 3, step, 0)

    def wait_items(self, items, sem):
        ref = self.buf.at[:, pl.ds(0, items)] if self.by_row else self.buf.at[pl.ds(0, items)]
        pltpu.make_async_copy(ref, ref, sem.at[0]).wait()

    def finish(self):
        self.wait_items(8, self.sib_recv)

    def drain(self):
        self.wait_items(7, self.send_sem)
        self.wait_items(8, self.sib_send)


def wait_bytes(ref, sem):
    pltpu.make_async_copy(ref, ref, sem).wait()


def kernel(qt_ref, do_ref, c_ref, rt_ref, wuk_ref, wuv_ref,
           o_ref, dq_ref, dc_ref, drt_ref, dwk_ref, dwv_ref,
           in_q, in_do, stage_o, stage_dq, stage_v, stage_k, in_v, in_k, call, kcat, kt, v, vt, sbuf, prob, qz, qn, dot, own_do, dk, dv,
           ot, dqt, delta, dct, raw_w, raw_do, do_heads, wuk, wuv, dwk_own, dwv_own,
           q_send, q_recv, o_send, o_recv, dq_send, dq_recv, v_send, v_recv, k_send, k_recv, local_sem,
           c_send, c_recv, cs_send, cs_recv, gk_send, gk_recv, gks_send, gks_recv, gv_send, gv_recv, gvs_send, gvs_recv):
    me = lax.axis_index("cp")

    loads = [
        pltpu.make_async_copy(wuk_ref, raw_w.at[0], local_sem.at[0]),
        pltpu.make_async_copy(wuv_ref, raw_w.at[1], local_sem.at[1]),
        pltpu.make_async_copy(do_ref, raw_do, local_sem.at[7]),
        pltpu.make_async_copy(c_ref, call.at[me, pl.ds(0, T), :], local_sem.at[2]),
        pltpu.make_async_copy(rt_ref.at[pl.ds(0, 32), :], call.at[me, pl.ds(T, 32), pl.ds(0, T)], local_sem.at[3]),
        pltpu.make_async_copy(rt_ref.at[pl.ds(32, 32), :], call.at[me, pl.ds(T, 32), pl.ds(T, T)], local_sem.at[4]),
    ]
    for load in loads[::-1]:
        load.start()

    barrier = pltpu.get_barrier_semaphore()

    def hello(s, carry):
        pl.semaphore_signal(barrier, inc=1, device_id=(xor(me, s),), device_id_type=MESH)
        return carry

    lax.fori_loop(1, N, hello, 0)
    for load in loads[3:]:
        load.wait()
    pl.semaphore_wait(barrier, N - 1)

    def send(src, dst, n, send_sem, recv):
        pltpu.make_async_remote_copy(
            src_ref=src, dst_ref=dst.at[me], send_sem=send_sem.at[0], recv_sem=recv,
            device_id=(xor(me, partner(n)),), device_id_type=MESH).start()

    gather_c = Gather(me, call.at[me], call, False, C_CHUNK, c_send, c_recv, cs_send, cs_recv)
    gather_c.stage0()
    pltpu.make_async_copy(qt_ref.at[me], in_q.at[me], q_recv.at[me]).start()
    dk[...] = jnp.zeros_like(dk)
    qz[...] = jnp.zeros_like(qz)
    dwk_own[...] = jnp.zeros_like(dwk_own)
    dwv_own[...] = jnp.zeros_like(dwv_own)

    def by_head(raw, put):
        def spread(g, carry):
            dv[g] = raw[pl.ds(pl.multiple_of(g * 32, 32), 32)].astype(F32).reshape(TK, D)
            return carry

        lax.fori_loop(0, NT, spread, 0)

        def head(h, carry):
            put(h, jnp.concatenate([dv[g, pl.ds(h, 32, stride=N), :] for g in range(NT)], axis=0).astype(BF16))
            return carry

        lax.fori_loop(0, N, head, 0)

    def put_do(h, x):
        do_heads[h] = x

    loads[2].wait()
    by_head(raw_do, put_do)
    pltpu.make_async_copy(do_heads.at[me], in_do.at[me], q_recv.at[me]).start()
    gather_c.stage1()
    gather_c.stage2()

    def send_q(n, carry):
        other = xor(me, partner(n))
        send(qt_ref.at[other], in_q, n, q_send, q_recv.at[me])
        send(do_heads.at[other], in_do, n, q_send, q_recv.at[me])
        return carry

    lax.fori_loop(1, N, send_q, 0)
    for load, raw, out in ((loads[0], raw_w.at[0], wuk), (loads[1], raw_w.at[1], wuv)):
        load.wait()
        for half in range(2):
            def put_w(h, x):
                out[pl.ds(half * T, T), pl.ds(pl.multiple_of(h * D, D), D)] = x

            by_head(raw.at[pl.ds(half * T, T)], put_w)
    dv[...] = jnp.zeros_like(dv)
    gather_c.stage3()
    gather_c.finish()

    lanes = pl.ds(pl.multiple_of(me * D, D), D)

    def make_kv(jt, carry):
        wcat = jnp.concatenate([wuk[:, lanes], wuv[:, lanes]], axis=1)
        for half in range(2):
            j = jt * 2 + half
            rows = pl.ds(half * T, T)
            kv = nn_dot(call[j, pl.ds(0, T), :], wcat)
            rt = jnp.concatenate([call[j, pl.ds(T, 32), pl.ds(0, T)], call[j, pl.ds(T, 32), pl.ds(T, T)]], axis=0)
            rtz = jnp.concatenate([rt.astype(F32), jnp.zeros((R, T), F32)], axis=0)
            kcat[jt, rows, pl.ds(0, D)] = kv[:, :D].astype(BF16)
            kcat[jt, rows, pl.ds(D, D)] = transpose(rtz).astype(BF16)
            v[jt, rows, :] = kv[:, D:].astype(BF16)
            kvt = transpose(kv).astype(BF16)
            kt[jt, pl.ds(0, D), rows] = kvt[:D]
            kt[jt, pl.ds(D, R), rows] = rt
            vt[jt, :, rows] = kvt[D:]
        return carry

    lax.fori_loop(0, NT, make_kv, 0)

    def pair(p):
        na = 4 * lax.div(p, 2) + lax.rem(p, 2)
        nb = 4 * lax.div(p, 2) + 3 - lax.rem(p, 2)
        ia, ib = xor(me, partner(na)), xor(me, partner(nb))
        split = lax.div(ia, 2) + 1
        which = [jnp.minimum(lax.div(t, split), 1) for t in range(TILES)]
        tile = [t - w * split for t, w in enumerate(which)]
        return (na, nb), (ia, ib), which, tile

    def pick(w, rows):
        return jnp.where(w == 1, rows[1], rows[0])

    def forward(p, carry):
        steps, blocks, which, tile = pair(p)
        for b, i in enumerate(blocks):
            wait_bytes(call.at[0, pl.ds(0, 160), :], q_recv.at[i])
            qz[b, pl.ds(0, QK), :] = in_q[i]
            own_do[b] = in_do[i]

        tops = [jnp.full((8, T), -1e30, F32)] * 2
        for t in range(TILES):
            w, jt = which[t], tile[t]
            sc = nn_dot(kcat[jt], qz[w])
            ahead = lax.broadcasted_iota(jnp.int32, sc.shape, 0) - lax.broadcasted_iota(jnp.int32, sc.shape, 1)
            i = blocks[0] + w * (blocks[1] - blocks[0])
            sc = jnp.where(ahead <= i * T - jt * TK, sc, -1e30)
            sbuf[t] = sc
            top = fold(sc, jnp.max)
            tops = [jnp.where(w == b, jnp.maximum(tops[b], top), tops[b]) for b in range(2)]
        tops = [jnp.max(x, axis=0, keepdims=True) * EXP_C for x in tops]

        ot[...] = jnp.zeros_like(ot)
        totals = [jnp.zeros((8, T), F32)] * 2
        for t in range(TILES):
            w, jt = which[t], tile[t]
            e = jnp.exp2(sbuf[t] * EXP_C - pick(w, tops))
            sbuf[t] = e
            ot[w] += nn_dot(vt[jt], e.astype(BF16))
            total = fold(e, jnp.sum)
            totals = [jnp.where(w == b, totals[b] + total, totals[b]) for b in range(2)]
        invs = [1.0 / jnp.sum(x, axis=0, keepdims=True) for x in totals]

        for t in range(TILES):
            w, jt = which[t], tile[t]
            prob_t = (sbuf[t] * pick(w, invs)).astype(BF16)
            prob[p * TILES + t] = prob_t
            dv[jt] += nn_dot(prob_t, own_do[w])

        for b, n in enumerate(steps):
            o_t = ot[b] * invs[b]
            stage_o[n] = transpose(o_t).astype(BF16)
            do_t = transpose(own_do[b].astype(F32))
            dot[p * 2 + b] = do_t.astype(BF16)
            delta[p * 2 + b] = jnp.broadcast_to(jnp.sum(o_t * do_t, axis=0, keepdims=True), (8, T))

            @pl.when(n > 0)
            def _():
                send(stage_o.at[n], o_ref, n, o_send, o_recv.at[0])

        return carry

    lax.fori_loop(0, N // 2, forward, 0)
    pltpu.make_async_copy(stage_o.at[0], o_ref.at[me], o_recv.at[0]).start()

    def block_rows(i):
        return pl.ds(pl.multiple_of(lax.rem(i, 2) * T, T), T)

    def grad_v(n, carry):
        i = xor(me, partner(n))
        stage_v[n] = transpose(dv[lax.div(i, 2), block_rows(i), :]).astype(BF16)
        return carry

    def weight_grad(stage, own):
        def step(m, acc):
            lhs = jnp.concatenate([stage[4 * m + r, pl.ds(0, D), :] for r in range(4)], axis=1)
            rhs = jnp.concatenate([call[xor(me, partner(4 * m + r)), pl.ds(0, T), :] for r in range(4)], axis=0)
            return acc + nn_dot(lhs, rhs)

        dwt = lax.fori_loop(0, 4, step, jnp.zeros((D, L), F32))
        own[pl.ds(0, L), :] = transpose(dwt)

    lax.fori_loop(0, N, grad_v, 0)
    pltpu.make_async_copy(stage_v.at[0], in_v.at[me], v_recv.at[0]).start()
    weight_grad(stage_v, dwv_own)
    gather_v = Gather(me, dwv_own, dwv_ref, True, W_CHUNK, gv_send, gv_recv, gvs_send, gvs_recv)
    all_rows = pl.ds(0, 3 * W_CHUNK)
    own_v = pltpu.make_async_copy(dwv_own, gather_v.view(me, all_rows), local_sem.at[5])
    own_v.start()
    gather_v.stage0()

    def backward(p, carry):
        steps, blocks, which, tile = pair(p)
        for b, i in enumerate(blocks):
            qz[b, pl.ds(0, QK), :] = in_q[i]
            qn[b] = transpose(qz[b].astype(F32)).astype(BF16)
        dqt[...] = jnp.zeros_like(dqt)
        deltas = [delta[p * 2 + b, pl.ds(0, 1), :] for b in range(2)]
        for t in range(TILES):
            w, jt = which[t], tile[t]
            dp = nn_dot(v[jt], dot[p * 2 + w])
            ds = (prob[p * TILES + t].astype(F32) * (dp - pick(w, deltas))).astype(BF16)
            dk[jt] += nn_dot(ds, qn[w])
            dqt[w] += nn_dot(kt[jt], ds)

        for b, n in enumerate(steps):
            stage_dq[n] = (dqt[b] * SCALE).astype(BF16)

            @pl.when(n > 0)
            def _():
                send(stage_dq.at[n], dq_ref, n, dq_send, dq_recv.at[0])
                send(stage_v.at[n], in_v, n, v_send, v_recv.at[0])

        @pl.when(p == 2)
        def _():
            gather_v.stage1()

        @pl.when(p == 4)
        def _():
            gather_v.stage2()

        @pl.when(p == 6)
        def _():
            gather_v.stage3()

        return carry

    lax.fori_loop(0, N // 2, backward, 0)
    pltpu.make_async_copy(stage_dq.at[0], dq_ref.at[me], dq_recv.at[0]).start()

    def grad_k(n, carry):
        i = xor(me, partner(n))
        key = transpose(dk[lax.div(i, 2), block_rows(i), :] * SCALE)
        stage_k[n] = key[:QK].astype(BF16)
        return carry

    lax.fori_loop(0, N, grad_k, 0)
    pltpu.make_async_copy(stage_k.at[0], in_k.at[me], k_recv.at[0]).start()

    def send_k(n, carry):
        send(stage_k.at[n], in_k, n, k_send, k_recv.at[0])
        return carry

    lax.fori_loop(1, 4, send_k, 0)
    weight_grad(stage_k, dwk_own)
    gather_k = Gather(me, dwk_own, dwk_ref, True, W_CHUNK, gk_send, gk_recv, gks_send, gks_recv)
    own_k = pltpu.make_async_copy(dwk_own, gather_k.view(me, all_rows), local_sem.at[6])
    own_k.start()
    gather_k.stage0()
    lax.fori_loop(4, 8, send_k, 0)

    dct[...] = jnp.zeros_like(dct)

    wait_bytes(in_v, v_recv.at[0])

    def latent_from_v(h, carry):
        cols = pl.ds(pl.multiple_of(h * D, D), D)
        dct[...] += nn_dot(wuv[:, cols], in_v[h])
        return carry

    lax.fori_loop(0, N, latent_from_v, 0)
    gather_k.stage1()
    lax.fori_loop(8, N, send_k, 0)
    gather_k.stage2()

    wait_bytes(in_k, k_recv.at[0])

    def latent_from_k(h, acc):
        cols = pl.ds(pl.multiple_of(h * D, D), D)
        dct[...] += nn_dot(wuk[:, cols], in_k[h, pl.ds(0, D), :])
        return acc + in_k[h, pl.ds(D, R), :].astype(F32)

    drt_ref[...] = lax.fori_loop(0, N, latent_from_k, jnp.zeros((R, T), F32)).astype(BF16)
    dc_ref[...] = transpose(dct[...]).astype(BF16)

    gather_k.stage3()
    gather_v.finish()
    gather_k.finish()
    own_v.wait()
    own_k.wait()

    wait_bytes(o_ref, o_recv.at[0])
    wait_bytes(dq_ref, dq_recv.at[0])
    others = pl.ds(0, N - 1)
    wait_bytes(qt_ref.at[others], q_send.at[0])
    wait_bytes(do_heads.at[others], q_send.at[0])
    wait_bytes(stage_o.at[others], o_send.at[0])
    wait_bytes(stage_dq.at[others], dq_send.at[0])
    wait_bytes(stage_v.at[others], v_send.at[0])
    wait_bytes(stage_k.at[others], k_send.at[0])
    gather_c.drain()
    gather_v.drain()
    gather_k.drain()


def copy_kernel(a_ref, b_ref, c_ref, d_ref):
    c_ref[...] = a_ref[...]
    d_ref[...] = b_ref[...]


def final_rows(a, b):
    spec = pl.BlockSpec((64, N, D), lambda r: (r, 0, 0))
    shape = jax.ShapeDtypeStruct((L, N, D), F32)
    return pl.pallas_call(copy_kernel, name="final_rows", grid=(L // 64,), in_specs=[spec, spec], out_specs=(spec, spec),
                          out_shape=(shape, shape))(a, b)


def solution(mesh):
    seq_spec = P("cp")

    def local_step(queries, latent, key_rope, w_uk, w_uv, d_out):
        any_spec = pl.BlockSpec(memory_space=pl.ANY)
        vmem_spec = pl.BlockSpec(memory_space=pltpu.VMEM)
        dma = pltpu.SemaphoreType.DMA
        o_all, dq_all, dc, drt, dwk, dwv = pl.pallas_call(
            kernel,
            name="mla_core",
            out_shape=(jax.ShapeDtypeStruct((N, T, D), BF16),
                       jax.ShapeDtypeStruct((N, QK, T), BF16),
                       jax.ShapeDtypeStruct((T, L), BF16),
                       jax.ShapeDtypeStruct((R, T), BF16),
                       jax.ShapeDtypeStruct((3 * W_CHUNK, N, 1, D), F32),
                       jax.ShapeDtypeStruct((3 * W_CHUNK, N, 1, D), F32)),
            in_specs=[any_spec] * 6,
            out_specs=(any_spec, any_spec, vmem_spec, vmem_spec, any_spec, any_spec),
            scratch_shapes=[
                pltpu.VMEM((N, QK, T), BF16),
                pltpu.VMEM((N, T, D), BF16),
                pltpu.VMEM((N, T, D), BF16),
                pltpu.VMEM((N, QK, T), BF16),
                pltpu.VMEM((N, D, T), BF16),
                pltpu.VMEM((N, QK, T), BF16),
                pltpu.VMEM((N, D, T), BF16),
                pltpu.VMEM((N, QK, T), BF16),
                pltpu.VMEM((N, 3 * C_CHUNK, L), BF16),
                pltpu.VMEM((NT, TK, 2 * D), BF16),
                pltpu.VMEM((NT, QK, TK), BF16),
                pltpu.VMEM((NT, TK, D), BF16),
                pltpu.VMEM((NT, D, TK), BF16),
                pltpu.VMEM((TILES, TK, T), F32),
                pltpu.VMEM((N // 2 * TILES, TK, T), BF16),
                pltpu.VMEM((2, 2 * D, T), BF16),
                pltpu.VMEM((2, T, 2 * D), BF16),
                pltpu.VMEM((N, D, T), BF16),
                pltpu.VMEM((2, T, D), BF16),
                pltpu.VMEM((NT, TK, 2 * D), F32),
                pltpu.VMEM((NT, TK, D), F32),
                pltpu.VMEM((2, D, T), F32),
                pltpu.VMEM((2, QK, T), F32),
                pltpu.VMEM((N, 8, T), F32),
                pltpu.VMEM((L, T), F32),
                pltpu.VMEM((2, L, N, D), BF16),
                pltpu.VMEM((T, N, D), BF16),
                pltpu.VMEM((N, T, D), BF16),
                pltpu.VMEM((L, N * D), BF16),
                pltpu.VMEM((L, N * D), BF16),
                pltpu.VMEM((3 * W_CHUNK, D), F32),
                pltpu.VMEM((3 * W_CHUNK, D), F32),
            ] + [dma((1,)), dma((N,))] + [dma((1,))] * 8 + [dma((8,))] + [dma((1,)), dma((24,)), dma((1,)), dma((1,))] * 3,
            compiler_params=pltpu.CompilerParams(
                collective_id=0, has_side_effects=True, vmem_limit_bytes=67043328),
        )(jnp.transpose(queries, (1, 2, 0)), d_out, latent, jnp.transpose(key_rope, (1, 0)),
          w_uk, w_uv)

        return (jnp.transpose(o_all, (1, 0, 2)), jnp.transpose(dq_all, (2, 0, 1)), dc, jnp.transpose(drt, (1, 0)),
                *final_rows(dwk.reshape(3 * W_CHUNK, N, D), dwv.reshape(3 * W_CHUNK, N, D)))

    return jax.shard_map(local_step, mesh=mesh,
                         in_specs=(seq_spec, seq_spec, seq_spec, P(), P(), seq_spec),
                         out_specs=(seq_spec, seq_spec, seq_spec, seq_spec, P(), P()),
                         check_vma=False)
```

```python
import math
import jax
import jax.numpy as jnp
from jax import lax
from jax.experimental import pallas as pl
from jax.experimental.pallas import tpu as pltpu
from jax.sharding import PartitionSpec as P

MESH = pl.DeviceIdType.MESH
BF16 = jnp.bfloat16
F32 = jnp.float32

N = 16
T = 256
L = 512
D = 128
R = 64
QK = D + R
TK = 512
NT = 8
C_CHUNK = 96
W_CHUNK = 176
TILES = 9
ORDER = (0, 7, 3, 4, 5, 2, 6, 1)
TABLE = sum(chip << (3 * n) for n, chip in enumerate(ORDER))
SCALE = 1.0 / math.sqrt(QK)
EXP_C = SCALE * math.log2(math.e)


def nt_dot(a, b):
    return lax.dot_general(a, b, (((1,), (1,)), ((), ())), preferred_element_type=F32)


def nn_dot(a, b):
    return lax.dot_general(a, b, (((1,), (0,)), ((), ())), preferred_element_type=F32)


def flip(x, bit):
    return x + bit * (1 - 2 * lax.rem(lax.div(x, bit), 2))


def xor(x, s):
    for bit in (1, 2, 4, 8):
        on = lax.rem(lax.div(s, bit), 2)
        x = x + on * bit * (1 - 2 * lax.rem(lax.div(x, bit), 2))
    return x


def partner(n):
    k = lax.div(n, 2)
    power = (1 + 7 * lax.rem(k, 2)) * (1 + 63 * lax.rem(lax.div(k, 2), 2)) * (1 + 4095 * lax.div(k, 4))
    return 2 * lax.rem(lax.div(TABLE, power), 8) + lax.rem(n, 2)


def fold(x, reduce):
    return reduce(x.reshape(x.shape[0] // 8, 8, x.shape[1]), axis=0)


def transpose(x):
    return jnp.transpose(x, (1, 0))


class Gather:
    def __init__(self, me, own, buf, by_row, chunk, send_sem, recv_sem, sib_send, sib_recv):
        self.me, self.own, self.buf, self.by_row, self.chunk = me, own, buf, by_row, chunk
        self.send_sem, self.recv_sem = send_sem, recv_sem
        self.sib_send, self.sib_recv = sib_send, sib_recv

    def view(self, src, rows):
        return self.buf.at[rows, src, 0, :] if self.by_row else self.buf.at[src, rows, :]

    def axes(self, k):
        out = []
        for t in range(3):
            axis = lax.rem(k + t, 3)
            out.append(2 + axis * (axis + 1))
        return out

    def make(self, k, masks, mask, target, send_sem, recv_sem):
        src = self.me
        for bit in masks:
            src = flip(src, bit)
        rows = pl.ds(k * self.chunk, self.chunk)
        slot = k * 8 + lax.div(mask, 2)
        first = self.own.at[rows, :] if not masks else self.view(src, rows)
        recv = recv_sem.at[0] if recv_sem is self.sib_recv else recv_sem.at[slot]
        return pltpu.make_async_remote_copy(
            src_ref=first, dst_ref=self.view(src, rows), send_sem=send_sem.at[0], recv_sem=recv,
            device_id=(target,), device_id_type=MESH)

    def hop(self, k, masks, bit):
        return self.make(k, masks, sum(masks) + bit, flip(self.me, bit), self.send_sem, self.recv_sem)

    def sib(self, k, masks):
        return self.make(k, masks, sum(masks), flip(self.me, 1), self.sib_send, self.sib_recv)

    def arrived(self, k, masks):
        self.make(k, masks, sum(masks), flip(self.me, 1), self.send_sem, self.recv_sem).wait_recv()

    def stage0(self):
        for t in range(3):
            def send(k, carry):
                self.hop(k, (), self.axes(k)[t]).start()
                return carry
            lax.fori_loop(0, 3, send, 0)

        def send_sib(k, carry):
            self.sib(k, ()).start()
            return carry
        lax.fori_loop(0, 3, send_sib, 0)

    def stage1(self):
        def step(k, carry):
            a, b, c = self.axes(k)
            self.arrived(k, (a,))
            self.hop(k, (a,), b).start()
            self.hop(k, (a,), c).start()
            self.sib(k, (a,)).start()
            return carry
        lax.fori_loop(0, 3, step, 0)

    def stage2(self):
        for both in (False, True):
            def step(k, carry):
                a, b, c = self.axes(k)
                masks = (a, b) if both else (b,)
                self.arrived(k, masks)
                self.hop(k, masks, c).start()
                self.sib(k, masks).start()
                return carry
            lax.fori_loop(0, 3, step, 0)

    def stage3(self):
        for extra in range(4):
            def step(k, carry):
                a, b, c = self.axes(k)
                masks = ((c,), (a, c), (b, c), (a, b, c))[extra]
                self.arrived(k, masks)
                self.sib(k, masks).start()
                return carry
            lax.fori_loop(0, 3, step, 0)

    def wait_items(self, items, sem):
        ref = self.buf.at[:, pl.ds(0, items)] if self.by_row else self.buf.at[pl.ds(0, items)]
        pltpu.make_async_copy(ref, ref, sem.at[0]).wait()

    def finish(self):
        self.wait_items(8, self.sib_recv)

    def drain(self):
        self.wait_items(7, self.send_sem)
        self.wait_items(8, self.sib_send)


def wait_bytes(ref, sem):
    pltpu.make_async_copy(ref, ref, sem).wait()


def kernel(qt_ref, do_ref, c_ref, rt_ref, wuk_ref, wuv_ref,
           o_ref, dq_ref, dc_ref, drt_ref, dwk_ref, dwv_ref,
           in_q, in_do, stage_o, stage_dq, stage_v, stage_k, in_v, in_k, call, kcat, kt, v, vt, sbuf, prob, qz, qn, dot, own_do, dk, dv,
           ot, dqt, delta, dct, raw_w, raw_do, do_heads, wuk, wuv, dwk_own, dwv_own,
           q_send, q_recv, o_send, o_recv, dq_send, dq_recv, v_send, v_recv, k_send, k_recv, local_sem,
           c_send, c_recv, cs_send, cs_recv, gk_send, gk_recv, gks_send, gks_recv, gv_send, gv_recv, gvs_send, gvs_recv):
    me = lax.axis_index("cp")

    loads = [
        pltpu.make_async_copy(wuk_ref, raw_w.at[0], local_sem.at[0]),
        pltpu.make_async_copy(wuv_ref, raw_w.at[1], local_sem.at[1]),
        pltpu.make_async_copy(do_ref, raw_do, local_sem.at[7]),
        pltpu.make_async_copy(c_ref, call.at[me, pl.ds(0, T), :], local_sem.at[2]),
        pltpu.make_async_copy(rt_ref.at[pl.ds(0, 32), :], call.at[me, pl.ds(T, 32), pl.ds(0, T)], local_sem.at[3]),
        pltpu.make_async_copy(rt_ref.at[pl.ds(32, 32), :], call.at[me, pl.ds(T, 32), pl.ds(T, T)], local_sem.at[4]),
    ]
    for load in loads[::-1]:
        load.start()

    barrier = pltpu.get_barrier_semaphore()

    def hello(s, carry):
        pl.semaphore_signal(barrier, inc=1, device_id=(xor(me, s),), device_id_type=MESH)
        return carry

    lax.fori_loop(1, N, hello, 0)
    for load in loads[3:]:
        load.wait()
    pl.semaphore_wait(barrier, N - 1)

    def send(src, dst, n, send_sem, recv):
        pltpu.make_async_remote_copy(
            src_ref=src, dst_ref=dst.at[me], send_sem=send_sem.at[0], recv_sem=recv,
            device_id=(xor(me, partner(n)),), device_id_type=MESH).start()

    gather_c = Gather(me, call.at[me], call, False, C_CHUNK, c_send, c_recv, cs_send, cs_recv)
    gather_c.stage0()
    pltpu.make_async_copy(qt_ref.at[me], in_q.at[me], q_recv.at[me]).start()
    dk[...] = jnp.zeros_like(dk)
    qz[...] = jnp.zeros_like(qz)
    dwk_own[...] = jnp.zeros_like(dwk_own)
    dwv_own[...] = jnp.zeros_like(dwv_own)

    def by_head(raw, put):
        def spread(g, carry):
            dv[g] = raw[pl.ds(pl.multiple_of(g * 32, 32), 32)].astype(F32).reshape(TK, D)
            return carry

        lax.fori_loop(0, NT, spread, 0)

        def head(h, carry):
            put(h, jnp.concatenate([dv[g, pl.ds(h, 32, stride=N), :] for g in range(NT)], axis=0).astype(BF16))
            return carry

        lax.fori_loop(0, N, head, 0)

    def put_do(h, x):
        do_heads[h] = x

    def send_q(n, carry):
        send(qt_ref.at[xor(me, partner(n))], in_q, n, q_send, q_recv.at[me])
        return carry

    def send_do(n, carry):
        send(do_heads.at[xor(me, partner(n))], in_do, n, q_send, q_recv.at[me])
        return carry

    def send_both(n, carry):
        return send_do(n, send_q(n, carry))

    lax.fori_loop(1, 4, send_q, 0)
    loads[2].wait()
    by_head(raw_do, put_do)
    pltpu.make_async_copy(do_heads.at[me], in_do.at[me], q_recv.at[me]).start()
    gather_c.stage1()
    gather_c.stage2()

    lax.fori_loop(1, 4, send_do, 0)
    lax.fori_loop(4, N, send_both, 0)
    for load, raw, out in ((loads[0], raw_w.at[0], wuk), (loads[1], raw_w.at[1], wuv)):
        load.wait()
        for half in range(2):
            def put_w(h, x):
                out[pl.ds(half * T, T), pl.ds(pl.multiple_of(h * D, D), D)] = x

            by_head(raw.at[pl.ds(half * T, T)], put_w)
    dv[...] = jnp.zeros_like(dv)
    gather_c.stage3()
    gather_c.finish()

    lanes = pl.ds(pl.multiple_of(me * D, D), D)

    def make_kv(jt, carry):
        wcat = jnp.concatenate([wuk[:, lanes], wuv[:, lanes]], axis=1)
        for half in range(2):
            j = jt * 2 + half
            rows = pl.ds(half * T, T)
            kv = nn_dot(call[j, pl.ds(0, T), :], wcat)
            rt = jnp.concatenate([call[j, pl.ds(T, 32), pl.ds(0, T)], call[j, pl.ds(T, 32), pl.ds(T, T)]], axis=0)
            rtz = jnp.concatenate([rt.astype(F32), jnp.zeros((R, T), F32)], axis=0)
            kcat[jt, rows, pl.ds(0, D)] = kv[:, :D].astype(BF16)
            kcat[jt, rows, pl.ds(D, D)] = transpose(rtz).astype(BF16)
            v[jt, rows, :] = kv[:, D:].astype(BF16)
            kvt = transpose(kv).astype(BF16)
            kt[jt, pl.ds(0, D), rows] = kvt[:D]
            kt[jt, pl.ds(D, R), rows] = rt
            vt[jt, :, rows] = kvt[D:]
        return carry

    lax.fori_loop(0, NT, make_kv, 0)

    def pair(p):
        na = 4 * lax.div(p, 2) + lax.rem(p, 2)
        nb = 4 * lax.div(p, 2) + 3 - lax.rem(p, 2)
        ia, ib = xor(me, partner(na)), xor(me, partner(nb))
        split = lax.div(ia, 2) + 1
        which = [jnp.minimum(lax.div(t, split), 1) for t in range(TILES)]
        tile = [t - w * split for t, w in enumerate(which)]
        return (na, nb), (ia, ib), which, tile

    def pick(w, rows):
        return jnp.where(w == 1, rows[1], rows[0])

    def forward(p, carry):
        steps, blocks, which, tile = pair(p)
        for b, i in enumerate(blocks):
            wait_bytes(call.at[0, pl.ds(0, 160), :], q_recv.at[i])
            qz[b, pl.ds(0, QK), :] = in_q[i]
            own_do[b] = in_do[i]

        tops = [jnp.full((8, T), -1e30, F32)] * 2
        for t in range(TILES):
            w, jt = which[t], tile[t]
            sc = nn_dot(kcat[jt], qz[w])
            ahead = lax.broadcasted_iota(jnp.int32, sc.shape, 0) - lax.broadcasted_iota(jnp.int32, sc.shape, 1)
            i = blocks[0] + w * (blocks[1] - blocks[0])
            sc = jnp.where(ahead <= i * T - jt * TK, sc, -1e30)
            sbuf[t] = sc
            top = fold(sc, jnp.max)
            tops = [jnp.where(w == b, jnp.maximum(tops[b], top), tops[b]) for b in range(2)]
        tops = [jnp.max(x, axis=0, keepdims=True) * EXP_C for x in tops]

        ot[...] = jnp.zeros_like(ot)
        totals = [jnp.zeros((8, T), F32)] * 2
        for t in range(TILES):
            w, jt = which[t], tile[t]
            e = jnp.exp2(sbuf[t] * EXP_C - pick(w, tops))
            sbuf[t] = e
            ot[w] += nn_dot(vt[jt], e.astype(BF16))
            total = fold(e, jnp.sum)
            totals = [jnp.where(w == b, totals[b] + total, totals[b]) for b in range(2)]
        invs = [1.0 / jnp.sum(x, axis=0, keepdims=True) for x in totals]

        for t in range(TILES):
            w, jt = which[t], tile[t]
            prob_t = (sbuf[t] * pick(w, invs)).astype(BF16)
            prob[p * TILES + t] = prob_t
            dv[jt] += nn_dot(prob_t, own_do[w])

        for b, n in enumerate(steps):
            o_t = ot[b] * invs[b]
            stage_o[n] = transpose(o_t).astype(BF16)
            do_t = transpose(own_do[b].astype(F32))
            dot[p * 2 + b] = do_t.astype(BF16)
            delta[p * 2 + b] = jnp.broadcast_to(jnp.sum(o_t * do_t, axis=0, keepdims=True), (8, T))

            @pl.when(n > 0)
            def _():
                send(stage_o.at[n], o_ref, n, o_send, o_recv.at[0])

        return carry

    lax.fori_loop(0, N // 2, forward, 0)
    pltpu.make_async_copy(stage_o.at[0], o_ref.at[me], o_recv.at[0]).start()

    def block_rows(i):
        return pl.ds(pl.multiple_of(lax.rem(i, 2) * T, T), T)

    def grad_v(n, carry):
        i = xor(me, partner(n))
        stage_v[n] = transpose(dv[lax.div(i, 2), block_rows(i), :]).astype(BF16)
        return carry

    def weight_grad(stage, own):
        def step(m, acc):
            lhs = jnp.concatenate([stage[4 * m + r, pl.ds(0, D), :] for r in range(4)], axis=1)
            rhs = jnp.concatenate([call[xor(me, partner(4 * m + r)), pl.ds(0, T), :] for r in range(4)], axis=0)
            return acc + nn_dot(lhs, rhs)

        dwt = lax.fori_loop(0, 4, step, jnp.zeros((D, L), F32))
        own[pl.ds(0, L), :] = transpose(dwt)

    lax.fori_loop(0, N, grad_v, 0)
    pltpu.make_async_copy(stage_v.at[0], in_v.at[me], v_recv.at[0]).start()
    weight_grad(stage_v, dwv_own)
    gather_v = Gather(me, dwv_own, dwv_ref, True, W_CHUNK, gv_send, gv_recv, gvs_send, gvs_recv)
    all_rows = pl.ds(0, 3 * W_CHUNK)
    own_v = pltpu.make_async_copy(dwv_own, gather_v.view(me, all_rows), local_sem.at[5])
    own_v.start()
    gather_v.stage0()

    def send_v(n, carry):
        send(stage_v.at[n], in_v, n, v_send, v_recv.at[0])
        return carry

    lax.fori_loop(1, 8, send_v, 0)

    def backward(p, carry):
        steps, blocks, which, tile = pair(p)
        for b, i in enumerate(blocks):
            qz[b, pl.ds(0, QK), :] = in_q[i]
            qn[b] = transpose(qz[b].astype(F32)).astype(BF16)
        dqt[...] = jnp.zeros_like(dqt)
        deltas = [delta[p * 2 + b, pl.ds(0, 1), :] for b in range(2)]
        for t in range(TILES):
            w, jt = which[t], tile[t]
            dp = nn_dot(v[jt], dot[p * 2 + w])
            ds = (prob[p * TILES + t].astype(F32) * (dp - pick(w, deltas))).astype(BF16)
            dk[jt] += nn_dot(ds, qn[w])
            dqt[w] += nn_dot(kt[jt], ds)

        for b, n in enumerate(steps):
            stage_dq[n] = (dqt[b] * SCALE).astype(BF16)

            @pl.when(n > 0)
            def _():
                send(stage_dq.at[n], dq_ref, n, dq_send, dq_recv.at[0])

        @pl.when(p < 4)
        def _():
            send_v(8 + 2 * p, 0)
            send_v(9 + 2 * p, 0)

        @pl.when(p == 2)
        def _():
            gather_v.stage1()

        @pl.when(p == 5)
        def _():
            gather_v.stage2()

        @pl.when(p == 7)
        def _():
            gather_v.stage3()

        return carry

    lax.fori_loop(0, N // 2, backward, 0)
    pltpu.make_async_copy(stage_dq.at[0], dq_ref.at[me], dq_recv.at[0]).start()

    def grad_k(n, carry):
        i = xor(me, partner(n))
        key = transpose(dk[lax.div(i, 2), block_rows(i), :] * SCALE)
        stage_k[n] = key[:QK].astype(BF16)
        return carry

    lax.fori_loop(0, N, grad_k, 0)
    pltpu.make_async_copy(stage_k.at[0], in_k.at[me], k_recv.at[me]).start()

    def send_k(n, carry):
        send(stage_k.at[n], in_k, n, k_send, k_recv.at[me])
        return carry

    lax.fori_loop(1, 4, send_k, 0)
    weight_grad(stage_k, dwk_own)
    gather_k = Gather(me, dwk_own, dwk_ref, True, W_CHUNK, gk_send, gk_recv, gks_send, gks_recv)
    own_k = pltpu.make_async_copy(dwk_own, gather_k.view(me, all_rows), local_sem.at[6])
    own_k.start()
    gather_k.stage0()
    lax.fori_loop(4, 6, send_k, 0)
    wait_bytes(in_v, v_recv.at[0])
    dct[...] = jnp.zeros_like(dct)
    gather_k.stage1()
    lax.fori_loop(6, 10, send_k, 0)

    def latent_from_v(g, carry):
        cols = pl.ds(pl.multiple_of(g * 4 * D, 4 * D), 4 * D)
        dct[...] += nn_dot(wuv[:, cols], in_v[pl.ds(4 * g, 4)].reshape(4 * D, T))
        return carry

    lax.fori_loop(0, 4, latent_from_v, 0)
    gather_k.stage2()
    lax.fori_loop(10, N, send_k, 0)
    gather_v.finish()
    gather_k.stage3()

    def latent_from_k(g, acc):
        parts = []
        for r in range(4):
            h = xor(me, partner(4 * g + r))
            wait_bytes(in_k.at[h], k_recv.at[h])
            parts.append(h)
        weights = jnp.concatenate([wuk[:, pl.ds(pl.multiple_of(h * D, D), D)] for h in parts], axis=1)
        grads = jnp.concatenate([in_k[h, pl.ds(0, D), :] for h in parts], axis=0)
        dct[...] += nn_dot(weights, grads)
        for h in parts:
            acc = acc + in_k[h, pl.ds(D, R), :].astype(F32)
        return acc

    drt_ref[...] = lax.fori_loop(0, 4, latent_from_k, jnp.zeros((R, T), F32)).astype(BF16)
    dc_ref[...] = transpose(dct[...]).astype(BF16)
    gather_k.finish()
    own_v.wait()
    own_k.wait()

    wait_bytes(o_ref, o_recv.at[0])
    wait_bytes(dq_ref, dq_recv.at[0])
    others = pl.ds(0, N - 1)
    wait_bytes(qt_ref.at[others], q_send.at[0])
    wait_bytes(do_heads.at[others], q_send.at[0])
    wait_bytes(stage_o.at[others], o_send.at[0])
    wait_bytes(stage_dq.at[others], dq_send.at[0])
    wait_bytes(stage_v.at[others], v_send.at[0])
    wait_bytes(stage_k.at[others], k_send.at[0])
    gather_c.drain()
    gather_v.drain()
    gather_k.drain()


def close_kernel(o_ref, dq_ref, dwk_ref, dwv_ref, o_out, dq_out, dwk_out, dwv_out,
                 o_in, o_rows, o_back, dq_buf, dwk_buf, dwv_buf, sem_in, sem_out):
    moves = []
    for r in range(8):
        for src, dst, buf in ((dwk_ref, dwk_out, dwk_buf), (dwv_ref, dwv_out, dwv_buf)):
            moves.append((src, dst, buf, pl.ds(r * 64, 64)))
    for r in range(4):
        moves.append((dq_ref, dq_out, dq_buf, pl.ds(r * 4, 4)))
    first = pltpu.make_async_copy(o_ref, o_in, sem_in.at[len(moves)])
    first.start()
    ins = [pltpu.make_async_copy(src.at[rows], buf.at[rows], sem_in.at[m]) for m, (src, dst, buf, rows) in enumerate(moves)]
    outs = [pltpu.make_async_copy(buf.at[rows], dst.at[rows], sem_out.at[m]) for m, (src, dst, buf, rows) in enumerate(moves)]
    for copy in ins:
        copy.start()
    first.wait()

    def head(h, carry):
        x = o_in[h].astype(F32)
        for g in range(NT):
            o_rows[g, pl.ds(h, 32, stride=N), :] = x[g * 32:(g + 1) * 32]
        return carry

    lax.fori_loop(0, N, head, 0)
    for g in range(NT):
        o_back[pl.ds(g * 32, 32)] = o_rows[g].reshape(32, N, D).astype(BF16)
    last = pltpu.make_async_copy(o_back, o_out, sem_out.at[len(moves)])
    last.start()
    for copy, out in zip(ins, outs):
        copy.wait()
        out.start()
    for out in outs:
        out.wait()
    last.wait()


def close(o, dq, dwk, dwv):
    any_spec = pl.BlockSpec(memory_space=pl.ANY)
    dw = (L, N, D)
    return pl.pallas_call(
        close_kernel, name="close", in_specs=[any_spec] * 4, out_specs=(any_spec,) * 4,
        out_shape=(jax.ShapeDtypeStruct((T, N, D), BF16), jax.ShapeDtypeStruct((N, QK, T), BF16),
                   jax.ShapeDtypeStruct(dw, F32), jax.ShapeDtypeStruct(dw, F32)),
        scratch_shapes=[pltpu.VMEM((N, T, D), BF16), pltpu.VMEM((NT, TK, D), F32), pltpu.VMEM((T, N, D), BF16),
                        pltpu.VMEM((N, QK, T), BF16), pltpu.VMEM(dw, F32), pltpu.VMEM(dw, F32),
                        pltpu.SemaphoreType.DMA((21,)), pltpu.SemaphoreType.DMA((21,))],
        compiler_params=pltpu.CompilerParams(vmem_limit_bytes=60 << 20))(o, dq, dwk, dwv)


def solution(mesh):
    seq_spec = P("cp")

    def local_step(queries, latent, key_rope, w_uk, w_uv, d_out):
        any_spec = pl.BlockSpec(memory_space=pl.ANY)
        vmem_spec = pl.BlockSpec(memory_space=pltpu.VMEM)
        dma = pltpu.SemaphoreType.DMA
        o_all, dq_all, dc, drt, dwk, dwv = pl.pallas_call(
            kernel,
            name="mla_core",
            out_shape=(jax.ShapeDtypeStruct((N, T, D), BF16),
                       jax.ShapeDtypeStruct((N, QK, T), BF16),
                       jax.ShapeDtypeStruct((T, L), BF16),
                       jax.ShapeDtypeStruct((R, T), BF16),
                       jax.ShapeDtypeStruct((3 * W_CHUNK, N, 1, D), F32),
                       jax.ShapeDtypeStruct((3 * W_CHUNK, N, 1, D), F32)),
            in_specs=[any_spec] * 6,
            out_specs=(any_spec, any_spec, vmem_spec, vmem_spec, any_spec, any_spec),
            scratch_shapes=[
                pltpu.VMEM((N, QK, T), BF16),
                pltpu.VMEM((N, T, D), BF16),
                pltpu.VMEM((N, T, D), BF16),
                pltpu.VMEM((N, QK, T), BF16),
                pltpu.VMEM((N, D, T), BF16),
                pltpu.VMEM((N, QK, T), BF16),
                pltpu.VMEM((N, D, T), BF16),
                pltpu.VMEM((N, QK, T), BF16),
                pltpu.VMEM((N, 3 * C_CHUNK, L), BF16),
                pltpu.VMEM((NT, TK, 2 * D), BF16),
                pltpu.VMEM((NT, QK, TK), BF16),
                pltpu.VMEM((NT, TK, D), BF16),
                pltpu.VMEM((NT, D, TK), BF16),
                pltpu.VMEM((TILES, TK, T), F32),
                pltpu.VMEM((N // 2 * TILES, TK, T), BF16),
                pltpu.VMEM((2, 2 * D, T), BF16),
                pltpu.VMEM((2, T, 2 * D), BF16),
                pltpu.VMEM((N, D, T), BF16),
                pltpu.VMEM((2, T, D), BF16),
                pltpu.VMEM((NT, TK, 2 * D), F32),
                pltpu.VMEM((NT, TK, D), F32),
                pltpu.VMEM((2, D, T), F32),
                pltpu.VMEM((2, QK, T), F32),
                pltpu.VMEM((N, 8, T), F32),
                pltpu.VMEM((L, T), F32),
                pltpu.VMEM((2, L, N, D), BF16),
                pltpu.VMEM((T, N, D), BF16),
                pltpu.VMEM((N, T, D), BF16),
                pltpu.VMEM((L, N * D), BF16),
                pltpu.VMEM((L, N * D), BF16),
                pltpu.VMEM((3 * W_CHUNK, D), F32),
                pltpu.VMEM((3 * W_CHUNK, D), F32),
            ] + [dma((1,)), dma((N,))] + [dma((1,))] * 7 + [dma((N,)), dma((8,))] + [dma((1,)), dma((24,)), dma((1,)), dma((1,))] * 3,
            compiler_params=pltpu.CompilerParams(
                collective_id=0, has_side_effects=True, vmem_limit_bytes=67043328),
        )(jnp.transpose(queries, (1, 2, 0)), d_out, latent, jnp.transpose(key_rope, (1, 0)),
          w_uk, w_uv)

        o, dq, dwk, dwv = close(o_all, dq_all, dwk.reshape(3 * W_CHUNK, N, D), dwv.reshape(3 * W_CHUNK, N, D))
        return o, jnp.transpose(dq, (2, 0, 1)), dc, jnp.transpose(drt, (1, 0)), dwk, dwv

    return jax.shard_map(local_step, mesh=mesh,
                         in_specs=(seq_spec, seq_spec, seq_spec, P(), P(), seq_spec),
                         out_specs=(seq_spec, seq_spec, seq_spec, seq_spec, P(), P()),
                         check_vma=False)
```

```python
import math
import jax
import jax.numpy as jnp
from jax import lax
from jax.experimental import pallas as pl
from jax.experimental.pallas import tpu as pltpu
from jax.sharding import PartitionSpec as P

MESH = pl.DeviceIdType.MESH
BF16 = jnp.bfloat16
F32 = jnp.float32

N = 16
T = 256
L = 512
D = 128
R = 64
QK = D + R
TK = 512
NT = 8
C_CHUNK = 96
W_CHUNK = 176
TILES = 9
ORDER = (0, 7, 3, 4, 5, 2, 6, 1)
TABLE = sum(chip << (3 * n) for n, chip in enumerate(ORDER))
SCALE = 1.0 / math.sqrt(QK)
EXP_C = SCALE * math.log2(math.e)


def nt_dot(a, b):
    return lax.dot_general(a, b, (((1,), (1,)), ((), ())), preferred_element_type=F32)


def nn_dot(a, b):
    return lax.dot_general(a, b, (((1,), (0,)), ((), ())), preferred_element_type=F32)


def flip(x, bit):
    return x + bit * (1 - 2 * lax.rem(lax.div(x, bit), 2))


def xor(x, s):
    for bit in (1, 2, 4, 8):
        on = lax.rem(lax.div(s, bit), 2)
        x = x + on * bit * (1 - 2 * lax.rem(lax.div(x, bit), 2))
    return x


def partner(n):
    k = lax.div(n, 2)
    power = (1 + 7 * lax.rem(k, 2)) * (1 + 63 * lax.rem(lax.div(k, 2), 2)) * (1 + 4095 * lax.div(k, 4))
    return 2 * lax.rem(lax.div(TABLE, power), 8) + lax.rem(n, 2)


def fold(x, reduce):
    return reduce(x.reshape(x.shape[0] // 8, 8, x.shape[1]), axis=0)


def transpose(x):
    return jnp.transpose(x, (1, 0))


class Gather:
    def __init__(self, me, own, buf, by_row, chunk, send_sem, recv_sem, sib_send, sib_recv):
        self.me, self.own, self.buf, self.by_row, self.chunk = me, own, buf, by_row, chunk
        self.send_sem, self.recv_sem = send_sem, recv_sem
        self.sib_send, self.sib_recv = sib_send, sib_recv

    def view(self, src, rows):
        return self.buf.at[rows, src, 0, :] if self.by_row else self.buf.at[src, rows, :]

    def axes(self, k):
        out = []
        for t in range(3):
            axis = lax.rem(k + t, 3)
            out.append(2 + axis * (axis + 1))
        return out

    def make(self, k, masks, mask, target, send_sem, recv_sem):
        src = self.me
        for bit in masks:
            src = flip(src, bit)
        rows = pl.ds(k * self.chunk, self.chunk)
        slot = k * 8 + lax.div(mask, 2)
        first = self.own.at[rows, :] if not masks else self.view(src, rows)
        recv = recv_sem.at[0] if recv_sem is self.sib_recv else recv_sem.at[slot]
        return pltpu.make_async_remote_copy(
            src_ref=first, dst_ref=self.view(src, rows), send_sem=send_sem.at[0], recv_sem=recv,
            device_id=(target,), device_id_type=MESH)

    def hop(self, k, masks, bit):
        return self.make(k, masks, sum(masks) + bit, flip(self.me, bit), self.send_sem, self.recv_sem)

    def sib(self, k, masks):
        return self.make(k, masks, sum(masks), flip(self.me, 1), self.sib_send, self.sib_recv)

    def arrived(self, k, masks):
        self.make(k, masks, sum(masks), flip(self.me, 1), self.send_sem, self.recv_sem).wait_recv()

    def stage0(self):
        for t in range(3):
            def send(k, carry):
                self.hop(k, (), self.axes(k)[t]).start()
                return carry
            lax.fori_loop(0, 3, send, 0)

        def send_sib(k, carry):
            self.sib(k, ()).start()
            return carry
        lax.fori_loop(0, 3, send_sib, 0)

    def stage1(self):
        def step(k, carry):
            a, b, c = self.axes(k)
            self.arrived(k, (a,))
            self.hop(k, (a,), b).start()
            self.hop(k, (a,), c).start()
            self.sib(k, (a,)).start()
            return carry
        lax.fori_loop(0, 3, step, 0)

    def stage2(self):
        for both in (False, True):
            def step(k, carry):
                a, b, c = self.axes(k)
                masks = (a, b) if both else (b,)
                self.arrived(k, masks)
                self.hop(k, masks, c).start()
                self.sib(k, masks).start()
                return carry
            lax.fori_loop(0, 3, step, 0)

    def stage3(self):
        for extra in range(4):
            def step(k, carry):
                a, b, c = self.axes(k)
                masks = ((c,), (a, c), (b, c), (a, b, c))[extra]
                self.arrived(k, masks)
                self.sib(k, masks).start()
                return carry
            lax.fori_loop(0, 3, step, 0)

    def wait_items(self, items, sem):
        ref = self.buf.at[:, pl.ds(0, items)] if self.by_row else self.buf.at[pl.ds(0, items)]
        pltpu.make_async_copy(ref, ref, sem.at[0]).wait()

    def finish(self):
        self.wait_items(8, self.sib_recv)

    def drain(self):
        self.wait_items(7, self.send_sem)
        self.wait_items(8, self.sib_send)


def wait_bytes(ref, sem):
    pltpu.make_async_copy(ref, ref, sem).wait()


def kernel(qt_ref, do_ref, c_ref, rt_ref, wuk_ref, wuv_ref,
           o_ref, dq_ref, dc_ref, drt_ref, dwk_ref, dwv_ref,
           in_q, in_do, stage_o, stage_dq, stage_v, stage_k, in_v, in_k, dr_part, dr_sib, dr_sum, in_dr, call, kcat, kt, v, vt, sbuf, prob, qz, qn, dot, own_do, dk, dv,
           ot, dqt, delta, dct, raw_w, raw_do, do_heads, wuk, wuv, dwk_own, dwv_own,
           q_send, q_recv, o_send, o_recv, dq_send, dq_recv, v_send, v_recv, k_send, k_recv, drs_send, drs_recv, dr_send, dr_recv, local_sem,
           c_send, c_recv, cs_send, cs_recv, gk_send, gk_recv, gks_send, gks_recv, gv_send, gv_recv, gvs_send, gvs_recv):
    me = lax.axis_index("cp")

    loads = [
        pltpu.make_async_copy(wuk_ref, raw_w.at[0], local_sem.at[0]),
        pltpu.make_async_copy(wuv_ref, raw_w.at[1], local_sem.at[1]),
        pltpu.make_async_copy(do_ref, raw_do, local_sem.at[7]),
        pltpu.make_async_copy(c_ref, call.at[me, pl.ds(0, T), :], local_sem.at[2]),
        pltpu.make_async_copy(rt_ref.at[pl.ds(0, 32), :], call.at[me, pl.ds(T, 32), pl.ds(0, T)], local_sem.at[3]),
        pltpu.make_async_copy(rt_ref.at[pl.ds(32, 32), :], call.at[me, pl.ds(T, 32), pl.ds(T, T)], local_sem.at[4]),
    ]
    for load in loads[::-1]:
        load.start()

    barrier = pltpu.get_barrier_semaphore()

    def hello(s, carry):
        pl.semaphore_signal(barrier, inc=1, device_id=(xor(me, s),), device_id_type=MESH)
        return carry

    lax.fori_loop(1, N, hello, 0)
    for load in loads[3:]:
        load.wait()
    pl.semaphore_wait(barrier, N - 1)

    def send(src, dst, n, send_sem, recv):
        pltpu.make_async_remote_copy(
            src_ref=src, dst_ref=dst.at[me], send_sem=send_sem.at[0], recv_sem=recv,
            device_id=(xor(me, partner(n)),), device_id_type=MESH).start()

    gather_c = Gather(me, call.at[me], call, False, C_CHUNK, c_send, c_recv, cs_send, cs_recv)
    gather_c.stage0()
    pltpu.make_async_copy(qt_ref.at[me], in_q.at[me], q_recv.at[me]).start()
    dk[...] = jnp.zeros_like(dk)
    qz[...] = jnp.zeros_like(qz)
    dwk_own[...] = jnp.zeros_like(dwk_own)
    dwv_own[...] = jnp.zeros_like(dwv_own)

    def by_head(raw, put):
        def spread(g, carry):
            dv[g] = raw[pl.ds(pl.multiple_of(g * 32, 32), 32)].astype(F32).reshape(TK, D)
            return carry

        lax.fori_loop(0, NT, spread, 0)

        def head(h, carry):
            put(h, jnp.concatenate([dv[g, pl.ds(h, 32, stride=N), :] for g in range(NT)], axis=0).astype(BF16))
            return carry

        lax.fori_loop(0, N, head, 0)

    def put_do(h, x):
        do_heads[h] = x

    def send_q(n, carry):
        send(qt_ref.at[xor(me, partner(n))], in_q, n, q_send, q_recv.at[me])
        return carry

    def send_do(n, carry):
        send(do_heads.at[xor(me, partner(n))], in_do, n, q_send, q_recv.at[me])
        return carry

    lax.fori_loop(1, 8, send_q, 0)
    loads[2].wait()
    by_head(raw_do, put_do)
    pltpu.make_async_copy(do_heads.at[me], in_do.at[me], q_recv.at[me]).start()
    gather_c.stage1()
    lax.fori_loop(1, 8, send_do, 0)
    gather_c.stage2()

    lax.fori_loop(8, N, send_q, 0)
    lax.fori_loop(8, N, send_do, 0)
    for load, raw, out in ((loads[0], raw_w.at[0], wuk), (loads[1], raw_w.at[1], wuv)):
        load.wait()
        for half in range(2):
            def put_w(h, x):
                out[pl.ds(half * T, T), pl.ds(pl.multiple_of(h * D, D), D)] = x

            by_head(raw.at[pl.ds(half * T, T)], put_w)
    dv[...] = jnp.zeros_like(dv)
    gather_c.stage3()
    gather_c.finish()

    lanes = pl.ds(pl.multiple_of(me * D, D), D)

    def make_kv(jt, carry):
        wcat = jnp.concatenate([wuk[:, lanes], wuv[:, lanes]], axis=1)
        for half in range(2):
            j = jt * 2 + half
            rows = pl.ds(half * T, T)
            kv = nn_dot(call[j, pl.ds(0, T), :], wcat)
            rt = jnp.concatenate([call[j, pl.ds(T, 32), pl.ds(0, T)], call[j, pl.ds(T, 32), pl.ds(T, T)]], axis=0)
            rtz = jnp.concatenate([rt.astype(F32), jnp.zeros((R, T), F32)], axis=0)
            kcat[jt, rows, pl.ds(0, D)] = kv[:, :D].astype(BF16)
            kcat[jt, rows, pl.ds(D, D)] = transpose(rtz).astype(BF16)
            v[jt, rows, :] = kv[:, D:].astype(BF16)
            kvt = transpose(kv).astype(BF16)
            kt[jt, pl.ds(0, D), rows] = kvt[:D]
            kt[jt, pl.ds(D, R), rows] = rt
            vt[jt, :, rows] = kvt[D:]
        return carry

    lax.fori_loop(0, NT, make_kv, 0)

    def pair(p):
        na = 4 * lax.div(p, 2) + lax.rem(p, 2)
        nb = 4 * lax.div(p, 2) + 3 - lax.rem(p, 2)
        ia, ib = xor(me, partner(na)), xor(me, partner(nb))
        split = lax.div(ia, 2) + 1
        which = [jnp.minimum(lax.div(t, split), 1) for t in range(TILES)]
        tile = [t - w * split for t, w in enumerate(which)]
        return (na, nb), (ia, ib), which, tile

    def pick(w, rows):
        return jnp.where(w == 1, rows[1], rows[0])

    def forward(p, carry):
        steps, blocks, which, tile = pair(p)
        for b, i in enumerate(blocks):
            wait_bytes(call.at[0, pl.ds(0, 160), :], q_recv.at[i])
            qz[b, pl.ds(0, QK), :] = in_q[i]
            own_do[b] = in_do[i]

        tops = [jnp.full((8, T), -1e30, F32)] * 2
        for t in range(TILES):
            w, jt = which[t], tile[t]
            sc = nn_dot(kcat[jt], qz[w])
            ahead = lax.broadcasted_iota(jnp.int32, sc.shape, 0) - lax.broadcasted_iota(jnp.int32, sc.shape, 1)
            i = blocks[0] + w * (blocks[1] - blocks[0])
            sc = jnp.where(ahead <= i * T - jt * TK, sc, -1e30)
            sbuf[t] = sc
            top = fold(sc, jnp.max)
            tops = [jnp.where(w == b, jnp.maximum(tops[b], top), tops[b]) for b in range(2)]
        tops = [jnp.max(x, axis=0, keepdims=True) * EXP_C for x in tops]

        ot[...] = jnp.zeros_like(ot)
        totals = [jnp.zeros((8, T), F32)] * 2
        for t in range(TILES):
            w, jt = which[t], tile[t]
            e = jnp.exp2(sbuf[t] * EXP_C - pick(w, tops))
            sbuf[t] = e
            ot[w] += nn_dot(vt[jt], e.astype(BF16))
            total = fold(e, jnp.sum)
            totals = [jnp.where(w == b, totals[b] + total, totals[b]) for b in range(2)]
        invs = [1.0 / jnp.sum(x, axis=0, keepdims=True) for x in totals]

        for t in range(TILES):
            w, jt = which[t], tile[t]
            prob_t = (sbuf[t] * pick(w, invs)).astype(BF16)
            prob[p * TILES + t] = prob_t
            dv[jt] += nn_dot(prob_t, own_do[w])

        for b, n in enumerate(steps):
            o_t = ot[b] * invs[b]
            stage_o[n] = transpose(o_t).astype(BF16)
            do_t = transpose(own_do[b].astype(F32))
            dot[p * 2 + b] = do_t.astype(BF16)
            delta[p * 2 + b] = jnp.broadcast_to(jnp.sum(o_t * do_t, axis=0, keepdims=True), (8, T))

            @pl.when(n > 0)
            def _():
                send(stage_o.at[n], o_ref, n, o_send, o_recv.at[0])

        return carry

    lax.fori_loop(0, N // 2, forward, 0)
    pltpu.make_async_copy(stage_o.at[0], o_ref.at[me], o_recv.at[0]).start()

    def block_rows(i):
        return pl.ds(pl.multiple_of(lax.rem(i, 2) * T, T), T)

    def grad_v(n, carry):
        i = xor(me, partner(n))
        stage_v[n] = transpose(dv[lax.div(i, 2), block_rows(i), :]).astype(BF16)
        return carry

    def weight_grad(stage, own):
        def step(m, acc):
            lhs = jnp.concatenate([stage[4 * m + r, pl.ds(0, D), :] for r in range(4)], axis=1)
            rhs = jnp.concatenate([call[xor(me, partner(4 * m + r)), pl.ds(0, T), :] for r in range(4)], axis=0)
            return acc + nn_dot(lhs, rhs)

        dwt = lax.fori_loop(0, 4, step, jnp.zeros((D, L), F32))
        own[pl.ds(0, L), :] = transpose(dwt)

    lax.fori_loop(0, N, grad_v, 0)
    pltpu.make_async_copy(stage_v.at[0], in_v.at[me], v_recv.at[0]).start()
    weight_grad(stage_v, dwv_own)
    gather_v = Gather(me, dwv_own, dwv_ref, True, W_CHUNK, gv_send, gv_recv, gvs_send, gvs_recv)
    all_rows = pl.ds(0, 3 * W_CHUNK)
    own_v = pltpu.make_async_copy(dwv_own, gather_v.view(me, all_rows), local_sem.at[5])
    own_v.start()
    gather_v.stage0()

    def send_v(n, carry):
        send(stage_v.at[n], in_v, n, v_send, v_recv.at[0])
        return carry

    lax.fori_loop(1, 8, send_v, 0)

    def backward(p, carry):
        steps, blocks, which, tile = pair(p)
        for b, i in enumerate(blocks):
            qz[b, pl.ds(0, QK), :] = in_q[i]
            qn[b] = transpose(qz[b].astype(F32)).astype(BF16)
        dqt[...] = jnp.zeros_like(dqt)
        deltas = [delta[p * 2 + b, pl.ds(0, 1), :] for b in range(2)]
        for t in range(TILES):
            w, jt = which[t], tile[t]
            dp = nn_dot(v[jt], dot[p * 2 + w])
            ds = (prob[p * TILES + t].astype(F32) * (dp - pick(w, deltas))).astype(BF16)
            dk[jt] += nn_dot(ds, qn[w])
            dqt[w] += nn_dot(kt[jt], ds)

        for b, n in enumerate(steps):
            stage_dq[n] = (dqt[b] * SCALE).astype(BF16)

            @pl.when(n > 0)
            def _():
                send(stage_dq.at[n], dq_ref, n, dq_send, dq_recv.at[0])

        @pl.when(p < 4)
        def _():
            send_v(8 + 2 * p, 0)
            send_v(9 + 2 * p, 0)

        @pl.when(p == 2)
        def _():
            gather_v.stage1()

        @pl.when(p == 5)
        def _():
            gather_v.stage2()

        @pl.when(p == 7)
        def _():
            gather_v.stage3()

        return carry

    lax.fori_loop(0, N // 2, backward, 0)
    pltpu.make_async_copy(stage_dq.at[0], dq_ref.at[me], dq_recv.at[0]).start()

    def grad_k(n, carry):
        i = xor(me, partner(n))
        key = transpose(dk[lax.div(i, 2), block_rows(i), :] * SCALE)
        stage_k[n] = key[:D].astype(BF16)
        dr_part[lax.rem(n, 2), lax.div(n, 2)] = key[D:QK].astype(BF16)
        return carry

    lax.fori_loop(0, N, grad_k, 0)
    pltpu.make_async_copy(stage_k.at[0], in_k.at[me], k_recv.at[me]).start()

    def send_k(n, carry):
        send(stage_k.at[n], in_k, n, k_send, k_recv.at[me])
        return carry

    give = pltpu.make_async_remote_copy(
        src_ref=dr_part.at[1], dst_ref=dr_sib, send_sem=drs_send.at[0], recv_sem=drs_recv.at[0],
        device_id=(flip(me, 1),), device_id_type=MESH)
    give.start()
    lax.fori_loop(1, 4, send_k, 0)
    weight_grad(stage_k, dwk_own)
    gather_k = Gather(me, dwk_own, dwk_ref, True, W_CHUNK, gk_send, gk_recv, gks_send, gks_recv)
    own_k = pltpu.make_async_copy(dwk_own, gather_k.view(me, all_rows), local_sem.at[6])
    own_k.start()
    gather_k.stage0()
    lax.fori_loop(4, 6, send_k, 0)
    give.wait_recv()
    dr_sum[...] = (dr_part[0].astype(F32) + dr_sib[...].astype(F32)).astype(BF16)
    chip = lax.div(me, 2)
    pltpu.make_async_copy(dr_sum.at[0], in_dr.at[chip], dr_recv.at[0]).start()

    def send_dr(k, carry):
        pltpu.make_async_remote_copy(
            src_ref=dr_sum.at[k], dst_ref=in_dr.at[chip], send_sem=dr_send.at[0], recv_sem=dr_recv.at[0],
            device_id=(xor(me, partner(2 * k)),), device_id_type=MESH).start()
        return carry

    lax.fori_loop(1, N // 2, send_dr, 0)
    wait_bytes(in_v, v_recv.at[0])
    dct[...] = jnp.zeros_like(dct)
    gather_k.stage1()
    lax.fori_loop(6, 10, send_k, 0)

    def latent_from_v(g, carry):
        cols = pl.ds(pl.multiple_of(g * 4 * D, 4 * D), 4 * D)
        dct[...] += nn_dot(wuv[:, cols], in_v[pl.ds(4 * g, 4)].reshape(4 * D, T))
        return carry

    lax.fori_loop(0, 4, latent_from_v, 0)
    gather_k.stage2()
    lax.fori_loop(10, N, send_k, 0)
    gather_v.finish()
    gather_k.stage3()

    wait_bytes(in_dr, dr_recv.at[0])
    drt_ref[...] = jnp.sum(in_dr[...].astype(F32), axis=0).astype(BF16)

    def latent_from_k(g, carry):
        parts = []
        for r in range(4):
            h = xor(me, partner(4 * g + r))
            wait_bytes(in_k.at[h], k_recv.at[h])
            parts.append(h)
        weights = jnp.concatenate([wuk[:, pl.ds(pl.multiple_of(h * D, D), D)] for h in parts], axis=1)
        grads = jnp.concatenate([in_k[h] for h in parts], axis=0)
        dct[...] += nn_dot(weights, grads)
        return carry

    lax.fori_loop(0, 4, latent_from_k, 0)
    dc_ref[...] = transpose(dct[...]).astype(BF16)
    gather_k.finish()
    own_v.wait()
    own_k.wait()

    wait_bytes(o_ref, o_recv.at[0])
    wait_bytes(dq_ref, dq_recv.at[0])
    others = pl.ds(0, N - 1)
    wait_bytes(qt_ref.at[others], q_send.at[0])
    wait_bytes(do_heads.at[others], q_send.at[0])
    wait_bytes(stage_o.at[others], o_send.at[0])
    wait_bytes(stage_dq.at[others], dq_send.at[0])
    wait_bytes(stage_v.at[others], v_send.at[0])
    wait_bytes(stage_k.at[others], k_send.at[0])
    give.wait_send()
    wait_bytes(dr_sum.at[pl.ds(0, N // 2 - 1)], dr_send.at[0])
    gather_c.drain()
    gather_v.drain()
    gather_k.drain()


def close_kernel(o_ref, dq_ref, dwk_ref, dwv_ref, dc_ref, dr_ref, o_out, dq_out, dwk_out, dwv_out, dc_out, dr_out,
                 o_in, o_rows, o_back, dq_buf, dwk_buf, dwv_buf, dc_buf, dr_buf, sem_in, sem_out):
    moves = []
    for r in range(8):
        for src, dst, buf in ((dwk_ref, dwk_out, dwk_buf), (dwv_ref, dwv_out, dwv_buf)):
            moves.append((src, dst, buf, pl.ds(r * 64, 64)))
    for r in range(4):
        moves.append((dq_ref, dq_out, dq_buf, pl.ds(r * 4, 4)))
    moves.append((dc_ref, dc_out, dc_buf, pl.ds(0, T)))
    moves.append((dr_ref, dr_out, dr_buf, pl.ds(0, R)))
    first = pltpu.make_async_copy(o_ref, o_in, sem_in.at[len(moves)])
    first.start()
    ins = [pltpu.make_async_copy(src.at[rows], buf.at[rows], sem_in.at[m]) for m, (src, dst, buf, rows) in enumerate(moves)]
    outs = [pltpu.make_async_copy(buf.at[rows], dst.at[rows], sem_out.at[m]) for m, (src, dst, buf, rows) in enumerate(moves)]
    for copy in ins:
        copy.start()
    first.wait()

    def head(h, carry):
        x = o_in[h].astype(F32)
        for g in range(NT):
            o_rows[g, pl.ds(h, 32, stride=N), :] = x[g * 32:(g + 1) * 32]
        return carry

    lax.fori_loop(0, N, head, 0)
    for g in range(NT):
        o_back[pl.ds(g * 32, 32)] = o_rows[g].reshape(32, N, D).astype(BF16)
    last = pltpu.make_async_copy(o_back, o_out, sem_out.at[len(moves)])
    last.start()
    for copy, out in zip(ins, outs):
        copy.wait()
        out.start()
    for out in outs:
        out.wait()
    last.wait()


def close(*arrays):
    any_spec = pl.BlockSpec(memory_space=pl.ANY)
    dw = (L, N, D)
    return pl.pallas_call(
        close_kernel, name="close", in_specs=[any_spec] * 6, out_specs=(any_spec,) * 6,
        out_shape=(jax.ShapeDtypeStruct((T, N, D), BF16), jax.ShapeDtypeStruct((N, QK, T), BF16),
                   jax.ShapeDtypeStruct(dw, F32), jax.ShapeDtypeStruct(dw, F32),
                   jax.ShapeDtypeStruct((T, L), BF16), jax.ShapeDtypeStruct((R, T), BF16)),
        scratch_shapes=[pltpu.VMEM((N, T, D), BF16), pltpu.VMEM((NT, TK, D), F32), pltpu.VMEM((T, N, D), BF16),
                        pltpu.VMEM((N, QK, T), BF16), pltpu.VMEM(dw, F32), pltpu.VMEM(dw, F32),
                        pltpu.VMEM((T, L), BF16), pltpu.VMEM((R, T), BF16),
                        pltpu.SemaphoreType.DMA((23,)), pltpu.SemaphoreType.DMA((23,))],
        compiler_params=pltpu.CompilerParams(vmem_limit_bytes=60 << 20))(*arrays)


def solution(mesh):
    seq_spec = P("cp")

    def local_step(queries, latent, key_rope, w_uk, w_uv, d_out):
        any_spec = pl.BlockSpec(memory_space=pl.ANY)
        vmem_spec = pl.BlockSpec(memory_space=pltpu.VMEM)
        dma = pltpu.SemaphoreType.DMA
        o_all, dq_all, dc, drt, dwk, dwv = pl.pallas_call(
            kernel,
            name="mla_core",
            out_shape=(jax.ShapeDtypeStruct((N, T, D), BF16),
                       jax.ShapeDtypeStruct((N, QK, T), BF16),
                       jax.ShapeDtypeStruct((T, L), BF16),
                       jax.ShapeDtypeStruct((R, T), BF16),
                       jax.ShapeDtypeStruct((3 * W_CHUNK, N, 1, D), F32),
                       jax.ShapeDtypeStruct((3 * W_CHUNK, N, 1, D), F32)),
            in_specs=[any_spec] * 6,
            out_specs=(any_spec, any_spec, vmem_spec, vmem_spec, any_spec, any_spec),
            scratch_shapes=[
                pltpu.VMEM((N, QK, T), BF16),
                pltpu.VMEM((N, T, D), BF16),
                pltpu.VMEM((N, T, D), BF16),
                pltpu.VMEM((N, QK, T), BF16),
                pltpu.VMEM((N, D, T), BF16),
                pltpu.VMEM((N, D, T), BF16),
                pltpu.VMEM((N, D, T), BF16),
                pltpu.VMEM((N, D, T), BF16),
                pltpu.VMEM((2, N // 2, R, T), BF16),
                pltpu.VMEM((N // 2, R, T), BF16),
                pltpu.VMEM((N // 2, R, T), BF16),
                pltpu.VMEM((N // 2, R, T), BF16),
                pltpu.VMEM((N, 3 * C_CHUNK, L), BF16),
                pltpu.VMEM((NT, TK, 2 * D), BF16),
                pltpu.VMEM((NT, QK, TK), BF16),
                pltpu.VMEM((NT, TK, D), BF16),
                pltpu.VMEM((NT, D, TK), BF16),
                pltpu.VMEM((TILES, TK, T), F32),
                pltpu.VMEM((N // 2 * TILES, TK, T), BF16),
                pltpu.VMEM((2, 2 * D, T), BF16),
                pltpu.VMEM((2, T, 2 * D), BF16),
                pltpu.VMEM((N, D, T), BF16),
                pltpu.VMEM((2, T, D), BF16),
                pltpu.VMEM((NT, TK, 2 * D), F32),
                pltpu.VMEM((NT, TK, D), F32),
                pltpu.VMEM((2, D, T), F32),
                pltpu.VMEM((2, QK, T), F32),
                pltpu.VMEM((N, 8, T), F32),
                pltpu.VMEM((L, T), F32),
                pltpu.VMEM((2, L, N, D), BF16),
                pltpu.VMEM((T, N, D), BF16),
                pltpu.VMEM((N, T, D), BF16),
                pltpu.VMEM((L, N * D), BF16),
                pltpu.VMEM((L, N * D), BF16),
                pltpu.VMEM((3 * W_CHUNK, D), F32),
                pltpu.VMEM((3 * W_CHUNK, D), F32),
            ] + [dma((1,)), dma((N,))] + [dma((1,))] * 7 + [dma((N,))] + [dma((1,))] * 4 + [dma((8,))] + [dma((1,)), dma((24,)), dma((1,)), dma((1,))] * 3,
            compiler_params=pltpu.CompilerParams(
                collective_id=0, has_side_effects=True, vmem_limit_bytes=67043328),
        )(jnp.transpose(queries, (1, 2, 0)), d_out, latent, jnp.transpose(key_rope, (1, 0)),
          w_uk, w_uv)

        o, dq, dwk, dwv, dc, drt = close(
            o_all, dq_all, dwk.reshape(3 * W_CHUNK, N, D), dwv.reshape(3 * W_CHUNK, N, D), dc, drt)
        return o, jnp.transpose(dq, (2, 0, 1)), dc, jnp.transpose(drt, (1, 0)), dwk, dwv

    return jax.shard_map(local_step, mesh=mesh,
                         in_specs=(seq_spec, seq_spec, seq_spec, P(), P(), seq_spec),
                         out_specs=(seq_spec, seq_spec, seq_spec, seq_spec, P(), P()),
                         check_vma=False)
```

```python
import math
import jax
import jax.numpy as jnp
from jax import lax
from jax.experimental import pallas as pl
from jax.experimental.pallas import tpu as pltpu
from jax.sharding import PartitionSpec as P

MESH = pl.DeviceIdType.MESH
BF16 = jnp.bfloat16
F32 = jnp.float32

N = 16
T = 256
L = 512
D = 128
R = 64
QK = D + R
TK = 512
NT = 8
C_CHUNK = 96
W_CHUNK = 176
TILES = 9
ORDER = (0, 7, 3, 4, 5, 2, 6, 1)
TABLE = sum(chip << (3 * n) for n, chip in enumerate(ORDER))
SCALE = 1.0 / math.sqrt(QK)
EXP_C = SCALE * math.log2(math.e)


def nt_dot(a, b):
    return lax.dot_general(a, b, (((1,), (1,)), ((), ())), preferred_element_type=F32)


def nn_dot(a, b):
    return lax.dot_general(a, b, (((1,), (0,)), ((), ())), preferred_element_type=F32)


def flip(x, bit):
    return x + bit * (1 - 2 * lax.rem(lax.div(x, bit), 2))


def xor(x, s):
    for bit in (1, 2, 4, 8):
        on = lax.rem(lax.div(s, bit), 2)
        x = x + on * bit * (1 - 2 * lax.rem(lax.div(x, bit), 2))
    return x


def partner(n):
    k = lax.div(n, 2)
    power = (1 + 7 * lax.rem(k, 2)) * (1 + 63 * lax.rem(lax.div(k, 2), 2)) * (1 + 4095 * lax.div(k, 4))
    return 2 * lax.rem(lax.div(TABLE, power), 8) + lax.rem(n, 2)


def fold(x, reduce):
    return reduce(x.reshape(x.shape[0] // 8, 8, x.shape[1]), axis=0)


def transpose(x):
    return jnp.transpose(x, (1, 0))


class Gather:
    def __init__(self, me, own, buf, by_row, chunk, send_sem, recv_sem, sib_send, sib_recv):
        self.me, self.own, self.buf, self.by_row, self.chunk = me, own, buf, by_row, chunk
        self.send_sem, self.recv_sem = send_sem, recv_sem
        self.sib_send, self.sib_recv = sib_send, sib_recv

    def view(self, src, rows):
        return self.buf.at[rows, src, 0, :] if self.by_row else self.buf.at[src, rows, :]

    def axes(self, k):
        out = []
        for t in range(3):
            axis = lax.rem(k + t, 3)
            out.append(2 + axis * (axis + 1))
        return out

    def make(self, k, masks, mask, target, send_sem, recv_sem):
        src = self.me
        for bit in masks:
            src = flip(src, bit)
        rows = pl.ds(k * self.chunk, self.chunk)
        slot = k * 8 + lax.div(mask, 2)
        first = self.own.at[rows, :] if not masks else self.view(src, rows)
        recv = recv_sem.at[0] if recv_sem is self.sib_recv else recv_sem.at[slot]
        return pltpu.make_async_remote_copy(
            src_ref=first, dst_ref=self.view(src, rows), send_sem=send_sem.at[0], recv_sem=recv,
            device_id=(target,), device_id_type=MESH)

    def hop(self, k, masks, bit):
        return self.make(k, masks, sum(masks) + bit, flip(self.me, bit), self.send_sem, self.recv_sem)

    def sib(self, k, masks):
        return self.make(k, masks, sum(masks), flip(self.me, 1), self.sib_send, self.sib_recv)

    def arrived(self, k, masks):
        self.make(k, masks, sum(masks), flip(self.me, 1), self.send_sem, self.recv_sem).wait_recv()

    def stage0(self):
        for t in range(3):
            def send(k, carry):
                self.hop(k, (), self.axes(k)[t]).start()
                return carry
            lax.fori_loop(0, 3, send, 0)

        def send_sib(k, carry):
            self.sib(k, ()).start()
            return carry
        lax.fori_loop(0, 3, send_sib, 0)

    def stage1(self):
        def step(k, carry):
            a, b, c = self.axes(k)
            self.arrived(k, (a,))
            self.hop(k, (a,), b).start()
            self.hop(k, (a,), c).start()
            self.sib(k, (a,)).start()
            return carry
        lax.fori_loop(0, 3, step, 0)

    def stage2(self):
        for both in (False, True):
            def step(k, carry):
                a, b, c = self.axes(k)
                masks = (a, b) if both else (b,)
                self.arrived(k, masks)
                self.hop(k, masks, c).start()
                self.sib(k, masks).start()
                return carry
            lax.fori_loop(0, 3, step, 0)

    def stage3(self):
        for extra in range(4):
            def step(k, carry):
                a, b, c = self.axes(k)
                masks = ((c,), (a, c), (b, c), (a, b, c))[extra]
                self.arrived(k, masks)
                self.sib(k, masks).start()
                return carry
            lax.fori_loop(0, 3, step, 0)

    def wait_items(self, items, sem):
        ref = self.buf.at[:, pl.ds(0, items)] if self.by_row else self.buf.at[pl.ds(0, items)]
        pltpu.make_async_copy(ref, ref, sem.at[0]).wait()

    def finish(self):
        self.wait_items(8, self.sib_recv)

    def drain(self):
        self.wait_items(7, self.send_sem)
        self.wait_items(8, self.sib_send)


def wait_bytes(ref, sem):
    pltpu.make_async_copy(ref, ref, sem).wait()


def kernel(qt_ref, do_ref, c_ref, rt_ref, wuk_ref, wuv_ref,
           o_ref, dq_ref, dc_ref, drt_ref, dwk_ref, dwv_ref,
           in_q, in_do, stage_o, stage_dq, stage_v, stage_k, in_v, in_k, dr_part, dr_sib, dr_sum, in_dr, call, kcat, kt, v, vt, sbuf, prob, qz, qn, dot, own_do, dk, dv,
           ot, dqt, delta, dct, raw_w, raw_do, do_heads, wuk, wuv, dwk_own, dwv_own,
           q_send, q_recv, o_send, o_recv, dq_send, dq_recv, v_send, v_recv, k_send, k_recv, drs_send, drs_recv, dr_send, dr_recv, local_sem,
           c_send, c_recv, cs_send, cs_recv, gk_send, gk_recv, gks_send, gks_recv, gv_send, gv_recv, gvs_send, gvs_recv):
    me = lax.axis_index("cp")

    loads = [
        pltpu.make_async_copy(wuk_ref, raw_w.at[0], local_sem.at[0]),
        pltpu.make_async_copy(wuv_ref, raw_w.at[1], local_sem.at[1]),
        pltpu.make_async_copy(do_ref, raw_do, local_sem.at[7]),
        pltpu.make_async_copy(c_ref, call.at[me, pl.ds(0, T), :], local_sem.at[2]),
        pltpu.make_async_copy(rt_ref.at[pl.ds(0, 32), :], call.at[me, pl.ds(T, 32), pl.ds(0, T)], local_sem.at[3]),
        pltpu.make_async_copy(rt_ref.at[pl.ds(32, 32), :], call.at[me, pl.ds(T, 32), pl.ds(T, T)], local_sem.at[4]),
    ]
    for load in loads[::-1]:
        load.start()

    barrier = pltpu.get_barrier_semaphore()

    def hello(s, carry):
        pl.semaphore_signal(barrier, inc=1, device_id=(xor(me, s),), device_id_type=MESH)
        return carry

    lax.fori_loop(1, N, hello, 0)
    for load in loads[3:]:
        load.wait()
    pl.semaphore_wait(barrier, N - 1)

    def send(src, dst, n, send_sem, recv):
        pltpu.make_async_remote_copy(
            src_ref=src, dst_ref=dst.at[me], send_sem=send_sem.at[0], recv_sem=recv,
            device_id=(xor(me, partner(n)),), device_id_type=MESH).start()

    gather_c = Gather(me, call.at[me], call, False, C_CHUNK, c_send, c_recv, cs_send, cs_recv)
    gather_c.stage0()
    pltpu.make_async_copy(qt_ref.at[me], in_q.at[me], q_recv.at[me]).start()
    dk[...] = jnp.zeros_like(dk)
    qz[...] = jnp.zeros_like(qz)
    dwk_own[...] = jnp.zeros_like(dwk_own)
    dwv_own[...] = jnp.zeros_like(dwv_own)

    def by_head(raw, put):
        def spread(g, carry):
            dv[g] = raw[pl.ds(pl.multiple_of(g * 32, 32), 32)].astype(F32).reshape(TK, D)
            return carry

        lax.fori_loop(0, NT, spread, 0)

        def head(h, carry):
            put(h, jnp.concatenate([dv[g, pl.ds(h, 32, stride=N), :] for g in range(NT)], axis=0).astype(BF16))
            return carry

        lax.fori_loop(0, N, head, 0)

    def put_do(h, x):
        do_heads[h] = x

    def send_q(n, carry):
        send(qt_ref.at[xor(me, partner(n))], in_q, n, q_send, q_recv.at[me])
        return carry

    def send_do(n, carry):
        send(do_heads.at[xor(me, partner(n))], in_do, n, q_send, q_recv.at[me])
        return carry

    lax.fori_loop(1, 4, send_q, 0)
    loads[2].wait()
    by_head(raw_do, put_do)
    pltpu.make_async_copy(do_heads.at[me], in_do.at[me], q_recv.at[me]).start()
    gather_c.stage1()
    gather_c.stage2()

    def send_both(n, carry):
        return send_do(n, send_q(n, carry))

    lax.fori_loop(1, 4, send_do, 0)
    lax.fori_loop(4, N, send_both, 0)
    for load, raw, out in ((loads[0], raw_w.at[0], wuk), (loads[1], raw_w.at[1], wuv)):
        load.wait()
        for half in range(2):
            def put_w(h, x):
                out[pl.ds(half * T, T), pl.ds(pl.multiple_of(h * D, D), D)] = x

            by_head(raw.at[pl.ds(half * T, T)], put_w)
    dv[...] = jnp.zeros_like(dv)
    gather_c.stage3()
    gather_c.finish()

    lanes = pl.ds(pl.multiple_of(me * D, D), D)

    def make_kv(jt, carry):
        wcat = jnp.concatenate([wuk[:, lanes], wuv[:, lanes]], axis=1)
        for half in range(2):
            j = jt * 2 + half
            rows = pl.ds(half * T, T)
            kv = nn_dot(call[j, pl.ds(0, T), :], wcat)
            rt = jnp.concatenate([call[j, pl.ds(T, 32), pl.ds(0, T)], call[j, pl.ds(T, 32), pl.ds(T, T)]], axis=0)
            rtz = jnp.concatenate([rt.astype(F32), jnp.zeros((R, T), F32)], axis=0)
            kcat[jt, rows, pl.ds(0, D)] = kv[:, :D].astype(BF16)
            kcat[jt, rows, pl.ds(D, D)] = transpose(rtz).astype(BF16)
            v[jt, rows, :] = kv[:, D:].astype(BF16)
            kvt = transpose(kv).astype(BF16)
            kt[jt, pl.ds(0, D), rows] = kvt[:D]
            kt[jt, pl.ds(D, R), rows] = rt
            vt[jt, :, rows] = kvt[D:]
        return carry

    lax.fori_loop(0, NT, make_kv, 0)

    def pair(p):
        na = 4 * lax.div(p, 2) + lax.rem(p, 2)
        nb = 4 * lax.div(p, 2) + 3 - lax.rem(p, 2)
        ia, ib = xor(me, partner(na)), xor(me, partner(nb))
        split = lax.div(ia, 2) + 1
        which = [jnp.minimum(lax.div(t, split), 1) for t in range(TILES)]
        tile = [split - 1] + [t - w * split - (1 - w) for t, w in enumerate(which) if t > 0]
        return (na, nb), (ia, ib), which, tile

    def pick(w, rows):
        return jnp.where(w == 1, rows[1], rows[0])

    def forward(p, carry):
        steps, blocks, which, tile = pair(p)
        for b, i in enumerate(blocks):
            wait_bytes(call.at[0, pl.ds(0, 160), :], q_recv.at[i])
            qz[b, pl.ds(0, QK), :] = in_q[i]
            own_do[b] = in_do[i]

        tops = [jnp.full((8, T), -1e30, F32)] * 2
        for t in range(TILES):
            w, jt = which[t], tile[t]
            sc = nn_dot(kcat[jt], qz[w])
            if t in (0, TILES - 1):
                ahead = lax.broadcasted_iota(jnp.int32, sc.shape, 0) - lax.broadcasted_iota(jnp.int32, sc.shape, 1)
                sc = jnp.where(ahead <= blocks[t > 0] * T - jt * TK, sc, -1e30)
            sbuf[t] = sc
            top = fold(sc, jnp.max)
            tops = [jnp.where(w == b, jnp.maximum(tops[b], top), tops[b]) for b in range(2)]
        tops = [jnp.max(x, axis=0, keepdims=True) * EXP_C for x in tops]

        ot[...] = jnp.zeros_like(ot)
        totals = [jnp.zeros((8, T), F32)] * 2
        for t in range(TILES):
            w, jt = which[t], tile[t]
            e = jnp.exp2(sbuf[t] * EXP_C - pick(w, tops))
            sbuf[t] = e
            ot[w] += nn_dot(vt[jt], e.astype(BF16))
            total = fold(e, jnp.sum)
            totals = [jnp.where(w == b, totals[b] + total, totals[b]) for b in range(2)]
        invs = [1.0 / jnp.sum(x, axis=0, keepdims=True) for x in totals]

        for t in range(TILES):
            w, jt = which[t], tile[t]
            prob_t = (sbuf[t] * pick(w, invs)).astype(BF16)
            prob[p * TILES + t] = prob_t
            dv[jt] += nn_dot(prob_t, own_do[w])

        for b, n in enumerate(steps):
            o_t = ot[b] * invs[b]
            stage_o[n] = transpose(o_t).astype(BF16)
            do_t = transpose(own_do[b].astype(F32))
            dot[p * 2 + b] = do_t.astype(BF16)
            delta[p * 2 + b] = jnp.broadcast_to(jnp.sum(o_t * do_t, axis=0, keepdims=True), (8, T))

            @pl.when(n > 0)
            def _():
                send(stage_o.at[n], o_ref, n, o_send, o_recv.at[0])

        return carry

    lax.fori_loop(0, N // 2, forward, 0)
    pltpu.make_async_copy(stage_o.at[0], o_ref.at[me], o_recv.at[0]).start()

    def block_rows(i):
        return pl.ds(pl.multiple_of(lax.rem(i, 2) * T, T), T)

    def grad_v(n, carry):
        i = xor(me, partner(n))
        stage_v[n] = transpose(dv[lax.div(i, 2), block_rows(i), :]).astype(BF16)
        return carry

    def weight_grad(stage, own):
        def step(m, acc):
            lhs = jnp.concatenate([stage[4 * m + r, pl.ds(0, D), :] for r in range(4)], axis=1)
            rhs = jnp.concatenate([call[xor(me, partner(4 * m + r)), pl.ds(0, T), :] for r in range(4)], axis=0)
            return acc + nn_dot(lhs, rhs)

        dwt = lax.fori_loop(0, 4, step, jnp.zeros((D, L), F32))
        own[pl.ds(0, L), :] = transpose(dwt)

    lax.fori_loop(0, N, grad_v, 0)
    pltpu.make_async_copy(stage_v.at[0], in_v.at[me], v_recv.at[0]).start()
    weight_grad(stage_v, dwv_own)
    gather_v = Gather(me, dwv_own, dwv_ref, True, W_CHUNK, gv_send, gv_recv, gvs_send, gvs_recv)
    all_rows = pl.ds(0, 3 * W_CHUNK)
    own_v = pltpu.make_async_copy(dwv_own, gather_v.view(me, all_rows), local_sem.at[5])
    own_v.start()
    gather_v.stage0()

    def send_v(n, carry):
        send(stage_v.at[n], in_v, n, v_send, v_recv.at[0])
        return carry

    lax.fori_loop(1, 8, send_v, 0)

    def backward(p, carry):
        steps, blocks, which, tile = pair(p)
        for b, i in enumerate(blocks):
            qz[b, pl.ds(0, QK), :] = in_q[i]
            qn[b] = transpose(qz[b].astype(F32)).astype(BF16)
        dqt[...] = jnp.zeros_like(dqt)
        deltas = [delta[p * 2 + b, pl.ds(0, 1), :] for b in range(2)]
        for t in range(TILES):
            w, jt = which[t], tile[t]
            dp = nn_dot(v[jt], dot[p * 2 + w])
            ds = (prob[p * TILES + t].astype(F32) * (dp - pick(w, deltas))).astype(BF16)
            dk[jt] += nn_dot(ds, qn[w])
            dqt[w] += nn_dot(kt[jt], ds)

        for b, n in enumerate(steps):
            stage_dq[n] = (dqt[b] * SCALE).astype(BF16)

            @pl.when(n > 0)
            def _():
                send(stage_dq.at[n], dq_ref, n, dq_send, dq_recv.at[0])

        @pl.when(p < 4)
        def _():
            send_v(8 + 2 * p, 0)
            send_v(9 + 2 * p, 0)

        @pl.when(p == 2)
        def _():
            gather_v.stage1()

        @pl.when(p == 5)
        def _():
            gather_v.stage2()

        @pl.when(p == 7)
        def _():
            gather_v.stage3()

        return carry

    lax.fori_loop(0, N // 2, backward, 0)
    pltpu.make_async_copy(stage_dq.at[0], dq_ref.at[me], dq_recv.at[0]).start()

    def grad_k(n, carry):
        i = xor(me, partner(n))
        key = transpose(dk[lax.div(i, 2), block_rows(i), :] * SCALE)
        stage_k[n] = key[:D].astype(BF16)
        dr_part[lax.rem(n, 2), lax.div(n, 2)] = key[D:QK].astype(BF16)
        return carry

    lax.fori_loop(0, N, grad_k, 0)
    pltpu.make_async_copy(stage_k.at[0], in_k.at[me], k_recv.at[me]).start()

    def send_k(n, carry):
        send(stage_k.at[n], in_k, n, k_send, k_recv.at[me])
        return carry

    give = pltpu.make_async_remote_copy(
        src_ref=dr_part.at[1], dst_ref=dr_sib, send_sem=drs_send.at[0], recv_sem=drs_recv.at[0],
        device_id=(flip(me, 1),), device_id_type=MESH)
    give.start()
    lax.fori_loop(1, 4, send_k, 0)
    weight_grad(stage_k, dwk_own)
    gather_k = Gather(me, dwk_own, dwk_ref, True, W_CHUNK, gk_send, gk_recv, gks_send, gks_recv)
    own_k = pltpu.make_async_copy(dwk_own, gather_k.view(me, all_rows), local_sem.at[6])
    own_k.start()
    gather_k.stage0()
    lax.fori_loop(4, 6, send_k, 0)
    give.wait_recv()
    dr_sum[...] = (dr_part[0].astype(F32) + dr_sib[...].astype(F32)).astype(BF16)
    chip = lax.div(me, 2)
    pltpu.make_async_copy(dr_sum.at[0], in_dr.at[chip], dr_recv.at[0]).start()

    def send_dr(k, carry):
        pltpu.make_async_remote_copy(
            src_ref=dr_sum.at[k], dst_ref=in_dr.at[chip], send_sem=dr_send.at[0], recv_sem=dr_recv.at[0],
            device_id=(xor(me, partner(2 * k)),), device_id_type=MESH).start()
        return carry

    lax.fori_loop(1, N // 2, send_dr, 0)
    wait_bytes(in_v, v_recv.at[0])
    dct[...] = jnp.zeros_like(dct)
    gather_k.stage1()
    lax.fori_loop(6, 10, send_k, 0)

    def latent_from_v(g, carry):
        cols = pl.ds(pl.multiple_of(g * 4 * D, 4 * D), 4 * D)
        dct[...] += nn_dot(wuv[:, cols], in_v[pl.ds(4 * g, 4)].reshape(4 * D, T))
        return carry

    lax.fori_loop(0, 4, latent_from_v, 0)
    gather_k.stage2()
    lax.fori_loop(10, N, send_k, 0)
    gather_v.finish()
    gather_k.stage3()

    wait_bytes(in_dr, dr_recv.at[0])
    drt_ref[...] = jnp.sum(in_dr[...].astype(F32), axis=0).astype(BF16)

    def latent_from_k(g, carry):
        parts = []
        for r in range(4):
            h = xor(me, partner(4 * g + r))
            wait_bytes(in_k.at[h], k_recv.at[h])
            parts.append(h)
        weights = jnp.concatenate([wuk[:, pl.ds(pl.multiple_of(h * D, D), D)] for h in parts], axis=1)
        grads = jnp.concatenate([in_k[h] for h in parts], axis=0)
        dct[...] += nn_dot(weights, grads)
        return carry

    lax.fori_loop(0, 4, latent_from_k, 0)
    dc_ref[...] = transpose(dct[...]).astype(BF16)
    gather_k.finish()
    own_v.wait()
    own_k.wait()

    wait_bytes(o_ref, o_recv.at[0])
    wait_bytes(dq_ref, dq_recv.at[0])
    others = pl.ds(0, N - 1)
    wait_bytes(qt_ref.at[others], q_send.at[0])
    wait_bytes(do_heads.at[others], q_send.at[0])
    wait_bytes(stage_o.at[others], o_send.at[0])
    wait_bytes(stage_dq.at[others], dq_send.at[0])
    wait_bytes(stage_v.at[others], v_send.at[0])
    wait_bytes(stage_k.at[others], k_send.at[0])
    give.wait_send()
    wait_bytes(dr_sum.at[pl.ds(0, N // 2 - 1)], dr_send.at[0])
    gather_c.drain()
    gather_v.drain()
    gather_k.drain()


def close_kernel(o_ref, dq_ref, dwk_ref, dwv_ref, dc_ref, dr_ref, o_out, dq_out, dwk_out, dwv_out, dc_out, dr_out,
                 o_in, o_rows, o_back, dq_buf, dwk_buf, dwv_buf, dc_buf, dr_buf, sem_in, sem_out):
    moves = []
    for r in range(8):
        for src, dst, buf in ((dwk_ref, dwk_out, dwk_buf), (dwv_ref, dwv_out, dwv_buf)):
            moves.append((src, dst, buf, pl.ds(r * 64, 64)))
    for r in range(4):
        moves.append((dq_ref, dq_out, dq_buf, pl.ds(r * 4, 4)))
    moves.append((dc_ref, dc_out, dc_buf, pl.ds(0, T)))
    moves.append((dr_ref, dr_out, dr_buf, pl.ds(0, R)))
    first = pltpu.make_async_copy(o_ref, o_in, sem_in.at[len(moves)])
    first.start()
    ins = [pltpu.make_async_copy(src.at[rows], buf.at[rows], sem_in.at[m]) for m, (src, dst, buf, rows) in enumerate(moves)]
    outs = [pltpu.make_async_copy(buf.at[rows], dst.at[rows], sem_out.at[m]) for m, (src, dst, buf, rows) in enumerate(moves)]
    for copy in ins:
        copy.start()
    first.wait()

    def head(h, carry):
        x = o_in[h].astype(F32)
        for g in range(NT):
            o_rows[g, pl.ds(h, 32, stride=N), :] = x[g * 32:(g + 1) * 32]
        return carry

    lax.fori_loop(0, N, head, 0)
    for g in range(NT):
        o_back[pl.ds(g * 32, 32)] = o_rows[g].reshape(32, N, D).astype(BF16)
    last = pltpu.make_async_copy(o_back, o_out, sem_out.at[len(moves)])
    last.start()
    for copy, out in zip(ins, outs):
        copy.wait()
        out.start()
    for out in outs:
        out.wait()
    last.wait()


def close(*arrays):
    any_spec = pl.BlockSpec(memory_space=pl.ANY)
    dw = (L, N, D)
    return pl.pallas_call(
        close_kernel, name="close", in_specs=[any_spec] * 6, out_specs=(any_spec,) * 6,
        out_shape=(jax.ShapeDtypeStruct((T, N, D), BF16), jax.ShapeDtypeStruct((N, QK, T), BF16),
                   jax.ShapeDtypeStruct(dw, F32), jax.ShapeDtypeStruct(dw, F32),
                   jax.ShapeDtypeStruct((T, L), BF16), jax.ShapeDtypeStruct((R, T), BF16)),
        scratch_shapes=[pltpu.VMEM((N, T, D), BF16), pltpu.VMEM((NT, TK, D), F32), pltpu.VMEM((T, N, D), BF16),
                        pltpu.VMEM((N, QK, T), BF16), pltpu.VMEM(dw, F32), pltpu.VMEM(dw, F32),
                        pltpu.VMEM((T, L), BF16), pltpu.VMEM((R, T), BF16),
                        pltpu.SemaphoreType.DMA((23,)), pltpu.SemaphoreType.DMA((23,))],
        compiler_params=pltpu.CompilerParams(vmem_limit_bytes=60 << 20))(*arrays)


def solution(mesh):
    seq_spec = P("cp")

    def local_step(queries, latent, key_rope, w_uk, w_uv, d_out):
        any_spec = pl.BlockSpec(memory_space=pl.ANY)
        vmem_spec = pl.BlockSpec(memory_space=pltpu.VMEM)
        dma = pltpu.SemaphoreType.DMA
        o_all, dq_all, dc, drt, dwk, dwv = pl.pallas_call(
            kernel,
            name="mla_core",
            out_shape=(jax.ShapeDtypeStruct((N, T, D), BF16),
                       jax.ShapeDtypeStruct((N, QK, T), BF16),
                       jax.ShapeDtypeStruct((T, L), BF16),
                       jax.ShapeDtypeStruct((R, T), BF16),
                       jax.ShapeDtypeStruct((3 * W_CHUNK, N, 1, D), F32),
                       jax.ShapeDtypeStruct((3 * W_CHUNK, N, 1, D), F32)),
            in_specs=[any_spec] * 6,
            out_specs=(any_spec, any_spec, vmem_spec, vmem_spec, any_spec, any_spec),
            scratch_shapes=[
                pltpu.VMEM((N, QK, T), BF16),
                pltpu.VMEM((N, T, D), BF16),
                pltpu.VMEM((N, T, D), BF16),
                pltpu.VMEM((N, QK, T), BF16),
                pltpu.VMEM((N, D, T), BF16),
                pltpu.VMEM((N, D, T), BF16),
                pltpu.VMEM((N, D, T), BF16),
                pltpu.VMEM((N, D, T), BF16),
                pltpu.VMEM((2, N // 2, R, T), BF16),
                pltpu.VMEM((N // 2, R, T), BF16),
                pltpu.VMEM((N // 2, R, T), BF16),
                pltpu.VMEM((N // 2, R, T), BF16),
                pltpu.VMEM((N, 3 * C_CHUNK, L), BF16),
                pltpu.VMEM((NT, TK, 2 * D), BF16),
                pltpu.VMEM((NT, QK, TK), BF16),
                pltpu.VMEM((NT, TK, D), BF16),
                pltpu.VMEM((NT, D, TK), BF16),
                pltpu.VMEM((TILES, TK, T), F32),
                pltpu.VMEM((N // 2 * TILES, TK, T), BF16),
                pltpu.VMEM((2, 2 * D, T), BF16),
                pltpu.VMEM((2, T, 2 * D), BF16),
                pltpu.VMEM((N, D, T), BF16),
                pltpu.VMEM((2, T, D), BF16),
                pltpu.VMEM((NT, TK, 2 * D), F32),
                pltpu.VMEM((NT, TK, D), F32),
                pltpu.VMEM((2, D, T), F32),
                pltpu.VMEM((2, QK, T), F32),
                pltpu.VMEM((N, 8, T), F32),
                pltpu.VMEM((L, T), F32),
                pltpu.VMEM((2, L, N, D), BF16),
                pltpu.VMEM((T, N, D), BF16),
                pltpu.VMEM((N, T, D), BF16),
                pltpu.VMEM((L, N * D), BF16),
                pltpu.VMEM((L, N * D), BF16),
                pltpu.VMEM((3 * W_CHUNK, D), F32),
                pltpu.VMEM((3 * W_CHUNK, D), F32),
            ] + [dma((1,)), dma((N,))] + [dma((1,))] * 7 + [dma((N,))] + [dma((1,))] * 4 + [dma((8,))] + [dma((1,)), dma((24,)), dma((1,)), dma((1,))] * 3,
            compiler_params=pltpu.CompilerParams(
                collective_id=0, has_side_effects=True, vmem_limit_bytes=67043328),
        )(jnp.transpose(queries, (1, 2, 0)), d_out, latent, jnp.transpose(key_rope, (1, 0)),
          w_uk, w_uv)

        o, dq, dwk, dwv, dc, drt = close(
            o_all, dq_all, dwk.reshape(3 * W_CHUNK, N, D), dwv.reshape(3 * W_CHUNK, N, D), dc, drt)
        return o, jnp.transpose(dq, (2, 0, 1)), dc, jnp.transpose(drt, (1, 0)), dwk, dwv

    return jax.shard_map(local_step, mesh=mesh,
                         in_specs=(seq_spec, seq_spec, seq_spec, P(), P(), seq_spec),
                         out_specs=(seq_spec, seq_spec, seq_spec, seq_spec, P(), P()),
                         check_vma=False)
```

```python
import math
import jax
import jax.numpy as jnp
from jax import lax
from jax.experimental import pallas as pl
from jax.experimental.pallas import tpu as pltpu
from jax.sharding import PartitionSpec as P

MESH = pl.DeviceIdType.MESH
BF16 = jnp.bfloat16
F32 = jnp.float32

N = 16
T = 256
L = 512
D = 128
R = 64
QK = D + R
TK = 512
NT = 8
C_CHUNK = 96
W_CHUNK = 176
TILES = 9
ORDER = (0, 7, 3, 4, 5, 2, 6, 1)
TABLE = sum(chip << (3 * n) for n, chip in enumerate(ORDER))
SCALE = 1.0 / math.sqrt(QK)
EXP_C = SCALE * math.log2(math.e)


def nt_dot(a, b):
    return lax.dot_general(a, b, (((1,), (1,)), ((), ())), preferred_element_type=F32)


def nn_dot(a, b):
    return lax.dot_general(a, b, (((1,), (0,)), ((), ())), preferred_element_type=F32)


def flip(x, bit):
    return x + bit * (1 - 2 * lax.rem(lax.div(x, bit), 2))


def xor(x, s):
    for bit in (1, 2, 4, 8):
        on = lax.rem(lax.div(s, bit), 2)
        x = x + on * bit * (1 - 2 * lax.rem(lax.div(x, bit), 2))
    return x


def partner(n):
    k = lax.div(n, 2)
    power = (1 + 7 * lax.rem(k, 2)) * (1 + 63 * lax.rem(lax.div(k, 2), 2)) * (1 + 4095 * lax.div(k, 4))
    return 2 * lax.rem(lax.div(TABLE, power), 8) + lax.rem(n, 2)


def fold(x, reduce):
    return reduce(x.reshape(x.shape[0] // 8, 8, x.shape[1]), axis=0)


def transpose(x):
    return jnp.transpose(x, (1, 0))


class Gather:
    def __init__(self, me, own, buf, by_row, chunk, send_sem, recv_sem, sib_send, sib_recv):
        self.me, self.own, self.buf, self.by_row, self.chunk = me, own, buf, by_row, chunk
        self.send_sem, self.recv_sem = send_sem, recv_sem
        self.sib_send, self.sib_recv = sib_send, sib_recv

    def view(self, src, rows):
        return self.buf.at[rows, src, 0, :] if self.by_row else self.buf.at[src, rows, :]

    def axes(self, k):
        out = []
        for t in range(3):
            axis = lax.rem(k + t, 3)
            out.append(2 + axis * (axis + 1))
        return out

    def make(self, k, masks, mask, target, send_sem, recv_sem):
        src = self.me
        for bit in masks:
            src = flip(src, bit)
        rows = pl.ds(k * self.chunk, self.chunk)
        slot = k * 8 + lax.div(mask, 2)
        first = self.own.at[rows, :] if not masks else self.view(src, rows)
        recv = recv_sem.at[0] if recv_sem is self.sib_recv else recv_sem.at[slot]
        return pltpu.make_async_remote_copy(
            src_ref=first, dst_ref=self.view(src, rows), send_sem=send_sem.at[0], recv_sem=recv,
            device_id=(target,), device_id_type=MESH)

    def hop(self, k, masks, bit):
        return self.make(k, masks, sum(masks) + bit, flip(self.me, bit), self.send_sem, self.recv_sem)

    def sib(self, k, masks):
        return self.make(k, masks, sum(masks), flip(self.me, 1), self.sib_send, self.sib_recv)

    def arrived(self, k, masks):
        self.make(k, masks, sum(masks), flip(self.me, 1), self.send_sem, self.recv_sem).wait_recv()

    def stage0(self):
        for t in range(3):
            def send(k, carry):
                self.hop(k, (), self.axes(k)[t]).start()
                return carry
            lax.fori_loop(0, 3, send, 0)

        def send_sib(k, carry):
            self.sib(k, ()).start()
            return carry
        lax.fori_loop(0, 3, send_sib, 0)

    def stage1(self):
        def step(k, carry):
            a, b, c = self.axes(k)
            self.arrived(k, (a,))
            self.hop(k, (a,), b).start()
            self.hop(k, (a,), c).start()
            self.sib(k, (a,)).start()
            return carry
        lax.fori_loop(0, 3, step, 0)

    def stage2(self):
        for both in (False, True):
            def step(k, carry):
                a, b, c = self.axes(k)
                masks = (a, b) if both else (b,)
                self.arrived(k, masks)
                self.hop(k, masks, c).start()
                self.sib(k, masks).start()
                return carry
            lax.fori_loop(0, 3, step, 0)

    def stage3(self):
        for extra in range(4):
            def step(k, carry):
                a, b, c = self.axes(k)
                masks = ((c,), (a, c), (b, c), (a, b, c))[extra]
                self.arrived(k, masks)
                self.sib(k, masks).start()
                return carry
            lax.fori_loop(0, 3, step, 0)

    def wait_items(self, items, sem):
        ref = self.buf.at[:, pl.ds(0, items)] if self.by_row else self.buf.at[pl.ds(0, items)]
        pltpu.make_async_copy(ref, ref, sem.at[0]).wait()

    def finish(self):
        self.wait_items(8, self.sib_recv)

    def drain(self):
        self.wait_items(7, self.send_sem)
        self.wait_items(8, self.sib_send)


def wait_bytes(ref, sem):
    pltpu.make_async_copy(ref, ref, sem).wait()


def kernel(qt_ref, do_ref, c_ref, rt_ref, wuk_ref, wuv_ref,
           o_ref, dq_ref, dc_ref, drt_ref, dwk_ref, dwv_ref,
           in_q, in_do, stage_o, stage_dq, stage_v, stage_k, in_v, in_k, dr_part, dr_sib, dr_sum, in_dr, call, kcat, kt, v, vt, sbuf, prob, qz, qn, dot, own_do, dk, dv,
           ot, dqt, delta, dct, raw_w, raw_do, do_heads, wuk, wuv, dwk_own, dwv_own,
           q_send, q_recv, o_send, o_recv, dq_send, dq_recv, v_send, v_recv, k_send, k_recv, drs_send, drs_recv, dr_send, dr_recv, local_sem,
           c_send, c_recv, cs_send, cs_recv, gk_send, gk_recv, gks_send, gks_recv, gv_send, gv_recv, gvs_send, gvs_recv):
    me = lax.axis_index("cp")

    loads = [
        pltpu.make_async_copy(wuk_ref, raw_w.at[0], local_sem.at[0]),
        pltpu.make_async_copy(wuv_ref, raw_w.at[1], local_sem.at[1]),
        pltpu.make_async_copy(do_ref, raw_do, local_sem.at[7]),
        pltpu.make_async_copy(c_ref, call.at[me, pl.ds(0, T), :], local_sem.at[2]),
        pltpu.make_async_copy(rt_ref.at[pl.ds(0, 32), :], call.at[me, pl.ds(T, 32), pl.ds(0, T)], local_sem.at[3]),
        pltpu.make_async_copy(rt_ref.at[pl.ds(32, 32), :], call.at[me, pl.ds(T, 32), pl.ds(T, T)], local_sem.at[4]),
    ]
    for load in loads[::-1]:
        load.start()

    barrier = pltpu.get_barrier_semaphore()

    def hello(s, carry):
        pl.semaphore_signal(barrier, inc=1, device_id=(xor(me, s),), device_id_type=MESH)
        return carry

    lax.fori_loop(1, N, hello, 0)
    for load in loads[3:]:
        load.wait()
    pl.semaphore_wait(barrier, N - 1)

    def send(src, dst, n, send_sem, recv):
        pltpu.make_async_remote_copy(
            src_ref=src, dst_ref=dst.at[me], send_sem=send_sem.at[0], recv_sem=recv,
            device_id=(xor(me, partner(n)),), device_id_type=MESH).start()

    gather_c = Gather(me, call.at[me], call, False, C_CHUNK, c_send, c_recv, cs_send, cs_recv)
    gather_c.stage0()
    pltpu.make_async_copy(qt_ref.at[me], in_q.at[me], q_recv.at[me]).start()
    dk[...] = jnp.zeros_like(dk)
    qz[...] = jnp.zeros_like(qz)
    dwk_own[...] = jnp.zeros_like(dwk_own)
    dwv_own[...] = jnp.zeros_like(dwv_own)

    def by_head(raw, put):
        def spread(g, carry):
            dv[g] = raw[pl.ds(pl.multiple_of(g * 32, 32), 32)].astype(F32).reshape(TK, D)
            return carry

        lax.fori_loop(0, NT, spread, 0)

        def head(h, carry):
            put(h, jnp.concatenate([dv[g, pl.ds(h, 32, stride=N), :] for g in range(NT)], axis=0).astype(BF16))
            return carry

        lax.fori_loop(0, N, head, 0)

    def put_do(h, x):
        do_heads[h] = x

    def send_q(n, carry):
        send(qt_ref.at[xor(me, partner(n))], in_q, n, q_send, q_recv.at[me])
        return carry

    def send_do(n, carry):
        send(do_heads.at[xor(me, partner(n))], in_do, n, q_send, q_recv.at[me])
        return carry

    lax.fori_loop(1, 4, send_q, 0)
    loads[2].wait()
    by_head(raw_do, put_do)
    pltpu.make_async_copy(do_heads.at[me], in_do.at[me], q_recv.at[me]).start()
    gather_c.stage1()
    gather_c.stage2()

    def send_both(n, carry):
        return send_do(n, send_q(n, carry))

    lax.fori_loop(1, 4, send_do, 0)
    lax.fori_loop(4, N, send_both, 0)
    for load, raw, out in ((loads[0], raw_w.at[0], wuk), (loads[1], raw_w.at[1], wuv)):
        load.wait()
        for half in range(2):
            def put_w(h, x):
                out[pl.ds(half * T, T), pl.ds(pl.multiple_of(h * D, D), D)] = x

            by_head(raw.at[pl.ds(half * T, T)], put_w)
    dv[...] = jnp.zeros_like(dv)
    gather_c.stage3()
    gather_c.finish()

    lanes = pl.ds(pl.multiple_of(me * D, D), D)

    def make_kv(jt, carry):
        wcat = jnp.concatenate([wuk[:, lanes], wuv[:, lanes]], axis=1)
        for half in range(2):
            j = jt * 2 + half
            rows = pl.ds(half * T, T)
            kv = nn_dot(call[j, pl.ds(0, T), :], wcat)
            rt = jnp.concatenate([call[j, pl.ds(T, 32), pl.ds(0, T)], call[j, pl.ds(T, 32), pl.ds(T, T)]], axis=0)
            rtz = jnp.concatenate([rt.astype(F32), jnp.zeros((R, T), F32)], axis=0)
            kcat[jt, rows, pl.ds(0, D)] = kv[:, :D].astype(BF16)
            kcat[jt, rows, pl.ds(D, D)] = transpose(rtz).astype(BF16)
            v[jt, rows, :] = kv[:, D:].astype(BF16)
            kvt = transpose(kv).astype(BF16)
            kt[jt, pl.ds(0, D), rows] = kvt[:D]
            kt[jt, pl.ds(D, R), rows] = rt
            vt[jt, :, rows] = kvt[D:]
        return carry

    lax.fori_loop(0, NT, make_kv, 0)

    def pair(p):
        na = 4 * lax.div(p, 2) + lax.rem(p, 2)
        nb = 4 * lax.div(p, 2) + 3 - lax.rem(p, 2)
        ia, ib = xor(me, partner(na)), xor(me, partner(nb))
        split = lax.div(ia, 2) + 1
        which = [jnp.minimum(lax.div(t, split), 1) for t in range(TILES)]
        tile = [split - 1] + [t - w * split - (1 - w) for t, w in enumerate(which) if t > 0]
        return (na, nb), (ia, ib), which, tile

    def pick(w, rows):
        return jnp.where(w == 1, rows[1], rows[0])

    def forward(p, carry):
        steps, blocks, which, tile = pair(p)
        for b, i in enumerate(blocks):
            wait_bytes(call.at[0, pl.ds(0, 160), :], q_recv.at[i])
            qz[b, pl.ds(0, QK), :] = in_q[i]
            own_do[b] = in_do[i]

        tops = [jnp.full((8, T), -1e30, F32)] * 2
        for t in range(TILES):
            w, jt = which[t], tile[t]
            sc = nn_dot(kcat[jt], qz[w])
            if t in (0, TILES - 1):
                ahead = lax.broadcasted_iota(jnp.int32, sc.shape, 0) - lax.broadcasted_iota(jnp.int32, sc.shape, 1)
                sc = jnp.where(ahead <= blocks[t > 0] * T - jt * TK, sc, -1e30)
            sbuf[t] = sc
            top = fold(sc, jnp.max)
            tops = [jnp.where(w == b, jnp.maximum(tops[b], top), tops[b]) for b in range(2)]
        tops = [jnp.max(x, axis=0, keepdims=True) * EXP_C for x in tops]

        ot[...] = jnp.zeros_like(ot)
        totals = [jnp.zeros((8, T), F32)] * 2
        for t in range(TILES):
            w, jt = which[t], tile[t]
            e = jnp.exp2(sbuf[t] * EXP_C - pick(w, tops))
            sbuf[t] = e
            ot[w] += nn_dot(vt[jt], e.astype(BF16))
            total = fold(e, jnp.sum)
            totals = [jnp.where(w == b, totals[b] + total, totals[b]) for b in range(2)]
        invs = [1.0 / jnp.sum(x, axis=0, keepdims=True) for x in totals]

        for t in range(TILES):
            w, jt = which[t], tile[t]
            prob_t = (sbuf[t] * pick(w, invs)).astype(BF16)
            prob[p * TILES + t] = prob_t
            dv[jt] += nn_dot(prob_t, own_do[w])

        for b, n in enumerate(steps):
            o_t = ot[b] * invs[b]
            stage_o[n] = transpose(o_t).astype(BF16)
            do_t = transpose(own_do[b].astype(F32))
            dot[p * 2 + b] = do_t.astype(BF16)
            delta[p * 2 + b] = jnp.broadcast_to(jnp.sum(o_t * do_t, axis=0, keepdims=True), (8, T))

            @pl.when(n > 0)
            def _():
                send(stage_o.at[n], o_ref, n, o_send, o_recv.at[0])

        return carry

    lax.fori_loop(0, N // 2, forward, 0)
    pltpu.make_async_copy(stage_o.at[0], o_ref.at[me], o_recv.at[0]).start()

    def block_rows(i):
        return pl.ds(pl.multiple_of(lax.rem(i, 2) * T, T), T)

    def grad_v(n, carry):
        i = xor(me, partner(n))
        stage_v[n] = transpose(dv[lax.div(i, 2), block_rows(i), :]).astype(BF16)
        return carry

    def weight_grad(stage, own):
        def step(m, acc):
            lhs = jnp.concatenate([stage[4 * m + r, pl.ds(0, D), :] for r in range(4)], axis=1)
            rhs = jnp.concatenate([call[xor(me, partner(4 * m + r)), pl.ds(0, T), :] for r in range(4)], axis=0)
            return acc + nn_dot(lhs, rhs)

        dwt = lax.fori_loop(0, 4, step, jnp.zeros((D, L), F32))
        own[pl.ds(0, L), :] = transpose(dwt)

    lax.fori_loop(0, N, grad_v, 0)
    pltpu.make_async_copy(stage_v.at[0], in_v.at[me], v_recv.at[0]).start()
    weight_grad(stage_v, dwv_own)
    gather_v = Gather(me, dwv_own, dwv_ref, True, W_CHUNK, gv_send, gv_recv, gvs_send, gvs_recv)
    all_rows = pl.ds(0, 3 * W_CHUNK)
    own_v = pltpu.make_async_copy(dwv_own, gather_v.view(me, all_rows), local_sem.at[5])
    own_v.start()
    gather_v.stage0()

    def send_v(n, carry):
        send(stage_v.at[n], in_v, n, v_send, v_recv.at[0])
        return carry

    lax.fori_loop(1, 8, send_v, 0)

    def backward(p, carry):
        steps, blocks, which, tile = pair(p)
        for b, i in enumerate(blocks):
            qz[b, pl.ds(0, QK), :] = in_q[i]
            qn[b] = transpose(qz[b].astype(F32)).astype(BF16)
        dqt[...] = jnp.zeros_like(dqt)
        deltas = [delta[p * 2 + b, pl.ds(0, 1), :] for b in range(2)]
        for t in range(TILES):
            w, jt = which[t], tile[t]
            dp = nn_dot(v[jt], dot[p * 2 + w])
            ds = (prob[p * TILES + t].astype(F32) * (dp - pick(w, deltas))).astype(BF16)
            dk[jt] += nn_dot(ds, qn[w])
            dqt[w] += nn_dot(kt[jt], ds)

        for b, n in enumerate(steps):
            stage_dq[n] = (dqt[b] * SCALE).astype(BF16)

            @pl.when(n > 0)
            def _():
                send(stage_dq.at[n], dq_ref, n, dq_send, dq_recv.at[0])

        @pl.when(p < 4)
        def _():
            send_v(8 + 2 * p, 0)
            send_v(9 + 2 * p, 0)

        @pl.when(p == 4)
        def _():
            gather_v.stage1()

        return carry

    lax.fori_loop(0, N // 2, backward, 0)
    gather_v.stage2()
    pltpu.make_async_copy(stage_dq.at[0], dq_ref.at[me], dq_recv.at[0]).start()

    def send_k(n, carry):
        send(stage_k.at[n], in_k, n, k_send, k_recv.at[me])
        return carry

    def grad_k(n, carry):
        i = xor(me, partner(n))
        key = transpose(dk[lax.div(i, 2), block_rows(i), :] * SCALE)
        stage_k[n] = key[:D].astype(BF16)
        dr_part[lax.rem(n, 2), lax.div(n, 2)] = key[D:QK].astype(BF16)

        @pl.when(lax.rem(n, 6) > 0)
        def _():
            @pl.when(n < 6)
            def _():
                send_k(n, 0)

        return carry

    lax.fori_loop(0, N, grad_k, 0)
    pltpu.make_async_copy(stage_k.at[0], in_k.at[me], k_recv.at[me]).start()

    give = pltpu.make_async_remote_copy(
        src_ref=dr_part.at[1], dst_ref=dr_sib, send_sem=drs_send.at[0], recv_sem=drs_recv.at[0],
        device_id=(flip(me, 1),), device_id_type=MESH)
    give.start()
    weight_grad(stage_k, dwk_own)
    gather_k = Gather(me, dwk_own, dwk_ref, True, W_CHUNK, gk_send, gk_recv, gks_send, gks_recv)
    own_k = pltpu.make_async_copy(dwk_own, gather_k.view(me, all_rows), local_sem.at[6])
    own_k.start()
    gather_k.stage0()
    give.wait_recv()
    dr_sum[...] = (dr_part[0].astype(F32) + dr_sib[...].astype(F32)).astype(BF16)
    chip = lax.div(me, 2)
    pltpu.make_async_copy(dr_sum.at[0], in_dr.at[chip], dr_recv.at[0]).start()

    def send_dr(k, carry):
        pltpu.make_async_remote_copy(
            src_ref=dr_sum.at[k], dst_ref=in_dr.at[chip], send_sem=dr_send.at[0], recv_sem=dr_recv.at[0],
            device_id=(xor(me, partner(2 * k)),), device_id_type=MESH).start()
        return carry

    lax.fori_loop(1, N // 2, send_dr, 0)
    wait_bytes(in_v, v_recv.at[0])
    dct[...] = jnp.zeros_like(dct)
    gather_k.stage1()
    lax.fori_loop(6, 10, send_k, 0)

    def latent_from_v(g, carry):
        cols = pl.ds(pl.multiple_of(g * 4 * D, 4 * D), 4 * D)
        dct[...] += nn_dot(wuv[:, cols], in_v[pl.ds(4 * g, 4)].reshape(4 * D, T))
        return carry

    lax.fori_loop(0, 4, latent_from_v, 0)
    gather_k.stage2()
    lax.fori_loop(10, N, send_k, 0)
    gather_v.stage3()
    gather_v.finish()
    gather_k.stage3()

    wait_bytes(in_dr, dr_recv.at[0])
    drt_ref[...] = jnp.sum(in_dr[...].astype(F32), axis=0).astype(BF16)

    def latent_from_k(g, carry):
        parts = []
        for r in range(4):
            h = xor(me, partner(4 * g + r))
            wait_bytes(in_k.at[h], k_recv.at[h])
            parts.append(h)
        weights = jnp.concatenate([wuk[:, pl.ds(pl.multiple_of(h * D, D), D)] for h in parts], axis=1)
        grads = jnp.concatenate([in_k[h] for h in parts], axis=0)
        dct[...] += nn_dot(weights, grads)
        return carry

    lax.fori_loop(0, 4, latent_from_k, 0)
    dc_ref[...] = transpose(dct[...]).astype(BF16)
    gather_k.finish()
    own_v.wait()
    own_k.wait()

    wait_bytes(o_ref, o_recv.at[0])
    wait_bytes(dq_ref, dq_recv.at[0])
    others = pl.ds(0, N - 1)
    wait_bytes(qt_ref.at[others], q_send.at[0])
    wait_bytes(do_heads.at[others], q_send.at[0])
    wait_bytes(stage_o.at[others], o_send.at[0])
    wait_bytes(stage_dq.at[others], dq_send.at[0])
    wait_bytes(stage_v.at[others], v_send.at[0])
    wait_bytes(stage_k.at[others], k_send.at[0])
    give.wait_send()
    wait_bytes(dr_sum.at[pl.ds(0, N // 2 - 1)], dr_send.at[0])
    gather_c.drain()
    gather_v.drain()
    gather_k.drain()


def close_kernel(o_ref, dq_ref, dwk_ref, dwv_ref, dc_ref, dr_ref, o_out, dq_out, dwk_out, dwv_out, dc_out, dr_out,
                 o_in, o_rows, o_back, dq_buf, dwk_buf, dwv_buf, dc_buf, dr_buf, sem_in, sem_out):
    moves = []
    for r in range(8):
        for src, dst, buf in ((dwk_ref, dwk_out, dwk_buf), (dwv_ref, dwv_out, dwv_buf)):
            moves.append((src, dst, buf, pl.ds(r * 64, 64)))
    for r in range(4):
        moves.append((dq_ref, dq_out, dq_buf, pl.ds(r * 4, 4)))
    moves.append((dc_ref, dc_out, dc_buf, pl.ds(0, T)))
    moves.append((dr_ref, dr_out, dr_buf, pl.ds(0, R)))
    first = pltpu.make_async_copy(o_ref, o_in, sem_in.at[len(moves)])
    first.start()
    ins = [pltpu.make_async_copy(src.at[rows], buf.at[rows], sem_in.at[m]) for m, (src, dst, buf, rows) in enumerate(moves)]
    outs = [pltpu.make_async_copy(buf.at[rows], dst.at[rows], sem_out.at[m]) for m, (src, dst, buf, rows) in enumerate(moves)]
    for copy in ins:
        copy.start()
    first.wait()

    def head(h, carry):
        x = o_in[h].astype(F32)
        for g in range(NT):
            o_rows[g, pl.ds(h, 32, stride=N), :] = x[g * 32:(g + 1) * 32]
        return carry

    lax.fori_loop(0, N, head, 0)
    for g in range(NT):
        o_back[pl.ds(g * 32, 32)] = o_rows[g].reshape(32, N, D).astype(BF16)
    last = pltpu.make_async_copy(o_back, o_out, sem_out.at[len(moves)])
    last.start()
    for copy, out in zip(ins, outs):
        copy.wait()
        out.start()
    for out in outs:
        out.wait()
    last.wait()


def close(*arrays):
    any_spec = pl.BlockSpec(memory_space=pl.ANY)
    dw = (L, N, D)
    return pl.pallas_call(
        close_kernel, name="close", in_specs=[any_spec] * 6, out_specs=(any_spec,) * 6,
        out_shape=(jax.ShapeDtypeStruct((T, N, D), BF16), jax.ShapeDtypeStruct((N, QK, T), BF16),
                   jax.ShapeDtypeStruct(dw, F32), jax.ShapeDtypeStruct(dw, F32),
                   jax.ShapeDtypeStruct((T, L), BF16), jax.ShapeDtypeStruct((R, T), BF16)),
        scratch_shapes=[pltpu.VMEM((N, T, D), BF16), pltpu.VMEM((NT, TK, D), F32), pltpu.VMEM((T, N, D), BF16),
                        pltpu.VMEM((N, QK, T), BF16), pltpu.VMEM(dw, F32), pltpu.VMEM(dw, F32),
                        pltpu.VMEM((T, L), BF16), pltpu.VMEM((R, T), BF16),
                        pltpu.SemaphoreType.DMA((23,)), pltpu.SemaphoreType.DMA((23,))],
        compiler_params=pltpu.CompilerParams(vmem_limit_bytes=60 << 20))(*arrays)


def solution(mesh):
    seq_spec = P("cp")

    def local_step(queries, latent, key_rope, w_uk, w_uv, d_out):
        any_spec = pl.BlockSpec(memory_space=pl.ANY)
        vmem_spec = pl.BlockSpec(memory_space=pltpu.VMEM)
        dma = pltpu.SemaphoreType.DMA
        o_all, dq_all, dc, drt, dwk, dwv = pl.pallas_call(
            kernel,
            name="mla_core",
            out_shape=(jax.ShapeDtypeStruct((N, T, D), BF16),
                       jax.ShapeDtypeStruct((N, QK, T), BF16),
                       jax.ShapeDtypeStruct((T, L), BF16),
                       jax.ShapeDtypeStruct((R, T), BF16),
                       jax.ShapeDtypeStruct((3 * W_CHUNK, N, 1, D), F32),
                       jax.ShapeDtypeStruct((3 * W_CHUNK, N, 1, D), F32)),
            in_specs=[any_spec] * 6,
            out_specs=(any_spec, any_spec, vmem_spec, vmem_spec, any_spec, any_spec),
            scratch_shapes=[
                pltpu.VMEM((N, QK, T), BF16),
                pltpu.VMEM((N, T, D), BF16),
                pltpu.VMEM((N, T, D), BF16),
                pltpu.VMEM((N, QK, T), BF16),
                pltpu.VMEM((N, D, T), BF16),
                pltpu.VMEM((N, D, T), BF16),
                pltpu.VMEM((N, D, T), BF16),
                pltpu.VMEM((N, D, T), BF16),
                pltpu.VMEM((2, N // 2, R, T), BF16),
                pltpu.VMEM((N // 2, R, T), BF16),
                pltpu.VMEM((N // 2, R, T), BF16),
                pltpu.VMEM((N // 2, R, T), BF16),
                pltpu.VMEM((N, 3 * C_CHUNK, L), BF16),
                pltpu.VMEM((NT, TK, 2 * D), BF16),
                pltpu.VMEM((NT, QK, TK), BF16),
                pltpu.VMEM((NT, TK, D), BF16),
                pltpu.VMEM((NT, D, TK), BF16),
                pltpu.VMEM((TILES, TK, T), F32),
                pltpu.VMEM((N // 2 * TILES, TK, T), BF16),
                pltpu.VMEM((2, 2 * D, T), BF16),
                pltpu.VMEM((2, T, 2 * D), BF16),
                pltpu.VMEM((N, D, T), BF16),
                pltpu.VMEM((2, T, D), BF16),
                pltpu.VMEM((NT, TK, 2 * D), F32),
                pltpu.VMEM((NT, TK, D), F32),
                pltpu.VMEM((2, D, T), F32),
                pltpu.VMEM((2, QK, T), F32),
                pltpu.VMEM((N, 8, T), F32),
                pltpu.VMEM((L, T), F32),
                pltpu.VMEM((2, L, N, D), BF16),
                pltpu.VMEM((T, N, D), BF16),
                pltpu.VMEM((N, T, D), BF16),
                pltpu.VMEM((L, N * D), BF16),
                pltpu.VMEM((L, N * D), BF16),
                pltpu.VMEM((3 * W_CHUNK, D), F32),
                pltpu.VMEM((3 * W_CHUNK, D), F32),
            ] + [dma((1,)), dma((N,))] + [dma((1,))] * 7 + [dma((N,))] + [dma((1,))] * 4 + [dma((8,))] + [dma((1,)), dma((24,)), dma((1,)), dma((1,))] * 3,
            compiler_params=pltpu.CompilerParams(
                collective_id=0, has_side_effects=True, vmem_limit_bytes=67043328),
        )(jnp.transpose(queries, (1, 2, 0)), d_out, latent, jnp.transpose(key_rope, (1, 0)),
          w_uk, w_uv)

        o, dq, dwk, dwv, dc, drt = close(
            o_all, dq_all, dwk.reshape(3 * W_CHUNK, N, D), dwv.reshape(3 * W_CHUNK, N, D), dc, drt)
        return o, jnp.transpose(dq, (2, 0, 1)), dc, jnp.transpose(drt, (1, 0)), dwk, dwv

    return jax.shard_map(local_step, mesh=mesh,
                         in_specs=(seq_spec, seq_spec, seq_spec, P(), P(), seq_spec),
                         out_specs=(seq_spec, seq_spec, seq_spec, seq_spec, P(), P()),
                         check_vma=False)
```

```python
import functools
import math
import jax
import jax.numpy as jnp
from jax import lax
from jax.experimental import pallas as pl
from jax.experimental.pallas import tpu as pltpu
from jax.sharding import PartitionSpec as P

MESH = pl.DeviceIdType.MESH
BF16 = jnp.bfloat16
F32 = jnp.float32

N = 16
T = 256
L = 512
D = 128
R = 64
QK = D + R
TK = 512
NT = 8
C_CHUNK = 96
W_CHUNK = 176
TILES = 9
ORDER = (0, 7, 3, 4, 5, 2, 6, 1)
TABLE = sum(chip << (3 * n) for n, chip in enumerate(ORDER))
SCALE = 1.0 / math.sqrt(QK)
EXP_C = SCALE * math.log2(math.e)


def nt_dot(a, b):
    return lax.dot_general(a, b, (((1,), (1,)), ((), ())), preferred_element_type=F32)


def nn_dot(a, b):
    return lax.dot_general(a, b, (((1,), (0,)), ((), ())), preferred_element_type=F32)


def flip(x, bit):
    return x + bit * (1 - 2 * lax.rem(lax.div(x, bit), 2))


def xor(x, s):
    for bit in (1, 2, 4, 8):
        on = lax.rem(lax.div(s, bit), 2)
        x = x + on * bit * (1 - 2 * lax.rem(lax.div(x, bit), 2))
    return x


def partner(n):
    k = lax.div(n, 2)
    power = (1 + 7 * lax.rem(k, 2)) * (1 + 63 * lax.rem(lax.div(k, 2), 2)) * (1 + 4095 * lax.div(k, 4))
    return 2 * lax.rem(lax.div(TABLE, power), 8) + lax.rem(n, 2)


def fold(x, reduce):
    return reduce(x.reshape(x.shape[0] // 8, 8, x.shape[1]), axis=0)


def transpose(x):
    return jnp.transpose(x, (1, 0))


class Gather:
    def __init__(self, me, own, buf, by_row, chunk, send_sem, recv_sem, sib_send, sib_recv):
        self.me, self.own, self.buf, self.by_row, self.chunk = me, own, buf, by_row, chunk
        self.send_sem, self.recv_sem = send_sem, recv_sem
        self.sib_send, self.sib_recv = sib_send, sib_recv

    def view(self, src, rows):
        return self.buf.at[rows, src, 0, :] if self.by_row else self.buf.at[src, rows, :]

    def axes(self, k):
        out = []
        for t in range(3):
            axis = lax.rem(k + t, 3)
            out.append(2 + axis * (axis + 1))
        return out

    def make(self, k, masks, mask, target, send_sem, recv_sem):
        src = self.me
        for bit in masks:
            src = flip(src, bit)
        rows = pl.ds(k * self.chunk, self.chunk)
        slot = k * 8 + lax.div(mask, 2)
        first = self.own.at[rows, :] if not masks else self.view(src, rows)
        recv = recv_sem.at[0] if recv_sem is self.sib_recv else recv_sem.at[slot]
        return pltpu.make_async_remote_copy(
            src_ref=first, dst_ref=self.view(src, rows), send_sem=send_sem.at[0], recv_sem=recv,
            device_id=(target,), device_id_type=MESH)

    def hop(self, k, masks, bit):
        return self.make(k, masks, sum(masks) + bit, flip(self.me, bit), self.send_sem, self.recv_sem)

    def sib(self, k, masks):
        return self.make(k, masks, sum(masks), flip(self.me, 1), self.sib_send, self.sib_recv)

    def arrived(self, k, masks):
        self.make(k, masks, sum(masks), flip(self.me, 1), self.send_sem, self.recv_sem).wait_recv()

    def stage0(self):
        for t in range(3):
            def send(k, carry):
                self.hop(k, (), self.axes(k)[t]).start()
                return carry
            lax.fori_loop(0, 3, send, 0)

        def send_sib(k, carry):
            self.sib(k, ()).start()
            return carry
        lax.fori_loop(0, 3, send_sib, 0)

    def stage1(self):
        def step(k, carry):
            a, b, c = self.axes(k)
            self.arrived(k, (a,))
            self.hop(k, (a,), b).start()
            self.hop(k, (a,), c).start()
            self.sib(k, (a,)).start()
            return carry
        lax.fori_loop(0, 3, step, 0)

    def stage2(self):
        for both in (False, True):
            def step(k, carry):
                a, b, c = self.axes(k)
                masks = (a, b) if both else (b,)
                self.arrived(k, masks)
                self.hop(k, masks, c).start()
                self.sib(k, masks).start()
                return carry
            lax.fori_loop(0, 3, step, 0)

    def stage3(self):
        for extra in range(4):
            def step(k, carry):
                a, b, c = self.axes(k)
                masks = ((c,), (a, c), (b, c), (a, b, c))[extra]
                self.arrived(k, masks)
                self.sib(k, masks).start()
                return carry
            lax.fori_loop(0, 3, step, 0)

    def wait_items(self, items, sem):
        ref = self.buf.at[:, pl.ds(0, items)] if self.by_row else self.buf.at[pl.ds(0, items)]
        pltpu.make_async_copy(ref, ref, sem.at[0]).wait()

    def finish(self):
        self.wait_items(8, self.sib_recv)

    def drain(self):
        self.wait_items(7, self.send_sem)
        self.wait_items(8, self.sib_send)


def wait_bytes(ref, sem):
    pltpu.make_async_copy(ref, ref, sem).wait()


def kernel(qt_ref, do_ref, c_ref, rt_ref, wuk_ref, wuv_ref,
           o_ref, dq_ref, dc_ref, drt_ref, dwk_ref, dwv_ref,
           in_q, in_do, stage_o, stage_dq, stage_v, stage_k, in_v, in_k, dr_part, dr_sib, dr_sum, in_dr, call, kcat, kt, v, vt, sbuf, prob, qz, qn, dot, own_do, dk, dv,
           ot, dqt, delta, dct, raw_w, raw_do, do_heads, w_own, wuk, wuv, dwk_own, dwv_own,
           q_send, q_recv, o_send, o_recv, dq_send, dq_recv, v_send, v_recv, k_send, k_recv, drs_send, drs_recv, dr_send, dr_recv, local_sem,
           c_send, c_recv, cs_send, cs_recv, gk_send, gk_recv, gks_send, gks_recv, gv_send, gv_recv, gvs_send, gvs_recv):
    me = lax.axis_index("cp")

    loads = [
        pltpu.make_async_copy(wuk_ref, raw_w.at[0], local_sem.at[0]),
        pltpu.make_async_copy(wuv_ref, raw_w.at[1], local_sem.at[1]),
        pltpu.make_async_copy(do_ref, raw_do, local_sem.at[7]),
        pltpu.make_async_copy(c_ref, call.at[me, pl.ds(0, T), :], local_sem.at[2]),
        pltpu.make_async_copy(rt_ref.at[pl.ds(0, 32), :], call.at[me, pl.ds(T, 32), pl.ds(0, T)], local_sem.at[3]),
        pltpu.make_async_copy(rt_ref.at[pl.ds(32, 32), :], call.at[me, pl.ds(T, 32), pl.ds(T, T)], local_sem.at[4]),
    ]
    for load in loads[::-1]:
        load.start()

    barrier = pltpu.get_barrier_semaphore()

    def hello(s, carry):
        pl.semaphore_signal(barrier, inc=1, device_id=(xor(me, s),), device_id_type=MESH)
        return carry

    lax.fori_loop(1, N, hello, 0)
    for load in loads[3:]:
        load.wait()
    pl.semaphore_wait(barrier, N - 1)

    def send(src, dst, n, send_sem, recv):
        pltpu.make_async_remote_copy(
            src_ref=src, dst_ref=dst.at[me], send_sem=send_sem.at[0], recv_sem=recv,
            device_id=(xor(me, partner(n)),), device_id_type=MESH).start()

    gather_c = Gather(me, call.at[me], call, False, C_CHUNK, c_send, c_recv, cs_send, cs_recv)
    gather_c.stage0()
    pltpu.make_async_copy(qt_ref.at[me], in_q.at[me], q_recv.at[me]).start()
    dk[...] = jnp.zeros_like(dk)
    qz[...] = jnp.zeros_like(qz)
    dwk_own[...] = jnp.zeros_like(dwk_own)
    dwv_own[...] = jnp.zeros_like(dwv_own)

    def spread(raw):
        def step(g, carry):
            dv[g] = raw[pl.ds(pl.multiple_of(g * 32, 32), 32)].astype(F32).reshape(TK, D)
            return carry

        lax.fori_loop(0, NT, step, 0)

    def one_head(h):
        return jnp.concatenate([dv[g, pl.ds(h, 32, stride=N), :] for g in range(NT)], axis=0).astype(BF16)

    def by_head(raw, put):
        spread(raw)

        def head(h, carry):
            put(h, one_head(h))
            return carry

        lax.fori_loop(0, N, head, 0)

    def put_do(h, x):
        do_heads[h] = x

    def send_q(n, carry):
        send(qt_ref.at[xor(me, partner(n))], in_q, n, q_send, q_recv.at[me])
        return carry

    def send_do(n, carry):
        send(do_heads.at[xor(me, partner(n))], in_do, n, q_send, q_recv.at[me])
        return carry

    lax.fori_loop(1, 4, send_q, 0)
    loads[2].wait()
    by_head(raw_do, put_do)
    pltpu.make_async_copy(do_heads.at[me], in_do.at[me], q_recv.at[me]).start()
    gather_c.stage1()
    gather_c.stage2()

    def send_both(n, carry):
        return send_do(n, send_q(n, carry))

    lax.fori_loop(1, 4, send_do, 0)
    lax.fori_loop(4, N, send_both, 0)
    for m in range(2):
        loads[m].wait()
        for half in range(2):
            rows = pl.ds(half * T, T)
            spread(raw_w.at[m, rows])
            w_own[rows, pl.ds(m * D, D)] = one_head(me)

    def order_weights(m, out):
        for half in range(2):
            def put_w(h, x):
                out[pl.ds(half * T, T), pl.ds(pl.multiple_of(h * D, D), D)] = x

            by_head(raw_w.at[m, pl.ds(half * T, T)], put_w)

    dv[...] = jnp.zeros_like(dv)
    gather_c.stage3()
    gather_c.finish()

    def make_kv(jt, carry):
        for half in range(2):
            j = jt * 2 + half
            rows = pl.ds(half * T, T)
            kv = nn_dot(call[j, pl.ds(0, T), :], w_own[...])
            rt = jnp.concatenate([call[j, pl.ds(T, 32), pl.ds(0, T)], call[j, pl.ds(T, 32), pl.ds(T, T)]], axis=0)
            rtz = jnp.concatenate([rt.astype(F32), jnp.zeros((R, T), F32)], axis=0)
            kcat[jt, rows, pl.ds(0, D)] = kv[:, :D].astype(BF16)
            kcat[jt, rows, pl.ds(D, D)] = transpose(rtz).astype(BF16)
            v[jt, rows, :] = kv[:, D:].astype(BF16)
            kvt = transpose(kv).astype(BF16)
            kt[jt, pl.ds(0, D), rows] = kvt[:D]
            kt[jt, pl.ds(D, R), rows] = rt
            vt[jt, :, rows] = kvt[D:]
        return carry

    lax.fori_loop(0, NT, make_kv, 0)

    def pair(p):
        na = 4 * lax.div(p, 2) + lax.rem(p, 2)
        nb = 4 * lax.div(p, 2) + 3 - lax.rem(p, 2)
        ia, ib = xor(me, partner(na)), xor(me, partner(nb))
        split = lax.div(ia, 2) + 1
        which = [jnp.minimum(lax.div(t, split), 1) for t in range(TILES)]
        tile = [split - 1] + [t - w * split - (1 - w) for t, w in enumerate(which) if t > 0]
        return (na, nb), (ia, ib), which, tile

    def pick(w, rows):
        return jnp.where(w == 1, rows[1], rows[0])

    def forward(p, carry):
        steps, blocks, which, tile = pair(p)
        for b, i in enumerate(blocks):
            wait_bytes(call.at[0, pl.ds(0, 160), :], q_recv.at[i])
            qz[b, pl.ds(0, QK), :] = in_q[i]
            own_do[b] = in_do[i]

        tile_top, tile_sum = [], []
        for t in range(TILES):
            w, jt = which[t], tile[t]
            sc = nn_dot(kcat[jt], qz[w])
            if t in (0, TILES - 1):
                ahead = lax.broadcasted_iota(jnp.int32, sc.shape, 0) - lax.broadcasted_iota(jnp.int32, sc.shape, 1)
                sc = jnp.where(ahead <= blocks[t > 0] * T - jt * TK, sc, -1e30)
            sbuf[t] = sc
            top = jnp.max(fold(sc, jnp.max), axis=0, keepdims=True) * EXP_C
            e = jnp.exp2(sbuf[t] * EXP_C - top)
            sbuf[t] = e
            tile_top.append(top)
            tile_sum.append(jnp.sum(fold(e, jnp.sum), axis=0, keepdims=True))

        tops = [functools.reduce(jnp.maximum, [jnp.where(w == b, x, -jnp.inf) for w, x in zip(which, tile_top)])
                for b in range(2)]
        factors = [jnp.exp2(x - pick(w, tops)) for w, x in zip(which, tile_top)]
        invs = [1.0 / sum(jnp.where(w == b, x * f, 0.0) for w, x, f in zip(which, tile_sum, factors)) for b in range(2)]

        ot[...] = jnp.zeros_like(ot)
        for t in range(TILES):
            w, jt = which[t], tile[t]
            prob_t = (sbuf[t] * (factors[t] * pick(w, invs))).astype(BF16)
            prob[p * TILES + t] = prob_t
            ot[w] += nn_dot(vt[jt], prob_t)
            dv[jt] += nn_dot(prob_t, own_do[w])

        for b, n in enumerate(steps):
            o_t = ot[b]
            stage_o[n] = transpose(o_t).astype(BF16)
            do_t = transpose(own_do[b].astype(F32))
            dot[p * 2 + b] = do_t.astype(BF16)
            delta[p * 2 + b] = jnp.broadcast_to(jnp.sum(o_t * do_t, axis=0, keepdims=True), (8, T))

            @pl.when(n > 0)
            def _():
                send(stage_o.at[n], o_ref, n, o_send, o_recv.at[0])

        return carry

    lax.fori_loop(0, N // 2, forward, 0)
    pltpu.make_async_copy(stage_o.at[0], o_ref.at[me], o_recv.at[0]).start()

    def block_rows(i):
        return pl.ds(pl.multiple_of(lax.rem(i, 2) * T, T), T)

    def grad_v(n, carry):
        i = xor(me, partner(n))
        stage_v[n] = transpose(dv[lax.div(i, 2), block_rows(i), :]).astype(BF16)
        return carry

    def weight_grad(stage, own):
        def step(m, acc):
            lhs = jnp.concatenate([stage[4 * m + r, pl.ds(0, D), :] for r in range(4)], axis=1)
            rhs = jnp.concatenate([call[xor(me, partner(4 * m + r)), pl.ds(0, T), :] for r in range(4)], axis=0)
            return acc + nn_dot(lhs, rhs)

        dwt = lax.fori_loop(0, 4, step, jnp.zeros((D, L), F32))
        own[pl.ds(0, L), :] = transpose(dwt)

    lax.fori_loop(0, N, grad_v, 0)
    pltpu.make_async_copy(stage_v.at[0], in_v.at[me], v_recv.at[0]).start()
    weight_grad(stage_v, dwv_own)
    gather_v = Gather(me, dwv_own, dwv_ref, True, W_CHUNK, gv_send, gv_recv, gvs_send, gvs_recv)
    all_rows = pl.ds(0, 3 * W_CHUNK)
    own_v = pltpu.make_async_copy(dwv_own, gather_v.view(me, all_rows), local_sem.at[5])
    own_v.start()
    gather_v.stage0()

    def send_v(n, carry):
        send(stage_v.at[n], in_v, n, v_send, v_recv.at[0])
        return carry

    lax.fori_loop(1, 8, send_v, 0)

    def backward(p, carry):
        steps, blocks, which, tile = pair(p)
        for b, i in enumerate(blocks):
            qz[b, pl.ds(0, QK), :] = in_q[i]
            qn[b] = transpose(qz[b].astype(F32)).astype(BF16)
        dqt[...] = jnp.zeros_like(dqt)
        deltas = [delta[p * 2 + b, pl.ds(0, 1), :] for b in range(2)]
        for t in range(TILES):
            w, jt = which[t], tile[t]
            dp = nn_dot(v[jt], dot[p * 2 + w])
            ds = (prob[p * TILES + t].astype(F32) * (dp - pick(w, deltas))).astype(BF16)
            dk[jt] += nn_dot(ds, qn[w])
            dqt[w] += nn_dot(kt[jt], ds)

        for b, n in enumerate(steps):
            stage_dq[n] = (dqt[b] * SCALE).astype(BF16)

            @pl.when(n > 0)
            def _():
                send(stage_dq.at[n], dq_ref, n, dq_send, dq_recv.at[0])

        @pl.when(p < 4)
        def _():
            send_v(8 + 2 * p, 0)
            send_v(9 + 2 * p, 0)

        @pl.when(p == 4)
        def _():
            gather_v.stage1()

        return carry

    lax.fori_loop(0, N // 2, backward, 0)
    gather_v.stage2()
    pltpu.make_async_copy(stage_dq.at[0], dq_ref.at[me], dq_recv.at[0]).start()

    def send_k(n, carry):
        send(stage_k.at[n], in_k, n, k_send, k_recv.at[me])
        return carry

    def grad_k(n, carry):
        i = xor(me, partner(n))
        key = transpose(dk[lax.div(i, 2), block_rows(i), :] * SCALE)
        stage_k[n] = key[:D].astype(BF16)
        dr_part[lax.rem(n, 2), lax.div(n, 2)] = key[D:QK].astype(BF16)

        @pl.when(lax.rem(n, 6) > 0)
        def _():
            @pl.when(n < 6)
            def _():
                send_k(n, 0)

        return carry

    lax.fori_loop(0, N, grad_k, 0)
    pltpu.make_async_copy(stage_k.at[0], in_k.at[me], k_recv.at[me]).start()

    give = pltpu.make_async_remote_copy(
        src_ref=dr_part.at[1], dst_ref=dr_sib, send_sem=drs_send.at[0], recv_sem=drs_recv.at[0],
        device_id=(flip(me, 1),), device_id_type=MESH)
    give.start()
    weight_grad(stage_k, dwk_own)
    gather_k = Gather(me, dwk_own, dwk_ref, True, W_CHUNK, gk_send, gk_recv, gks_send, gks_recv)
    own_k = pltpu.make_async_copy(dwk_own, gather_k.view(me, all_rows), local_sem.at[6])
    own_k.start()
    gather_k.stage0()
    give.wait_recv()
    dr_sum[...] = (dr_part[0].astype(F32) + dr_sib[...].astype(F32)).astype(BF16)
    chip = lax.div(me, 2)
    pltpu.make_async_copy(dr_sum.at[0], in_dr.at[chip], dr_recv.at[0]).start()

    def send_dr(k, carry):
        pltpu.make_async_remote_copy(
            src_ref=dr_sum.at[k], dst_ref=in_dr.at[chip], send_sem=dr_send.at[0], recv_sem=dr_recv.at[0],
            device_id=(xor(me, partner(2 * k)),), device_id_type=MESH).start()
        return carry

    lax.fori_loop(1, N // 2, send_dr, 0)
    order_weights(1, wuv)
    wait_bytes(in_v, v_recv.at[0])
    dct[...] = jnp.zeros_like(dct)
    gather_k.stage1()
    lax.fori_loop(6, 10, send_k, 0)

    def latent_from_v(g, carry):
        cols = pl.ds(pl.multiple_of(g * 4 * D, 4 * D), 4 * D)
        dct[...] += nn_dot(wuv[:, cols], in_v[pl.ds(4 * g, 4)].reshape(4 * D, T))
        return carry

    lax.fori_loop(0, 4, latent_from_v, 0)
    gather_k.stage2()
    lax.fori_loop(10, N, send_k, 0)
    order_weights(0, wuk)
    gather_v.stage3()
    gather_v.finish()
    gather_k.stage3()

    wait_bytes(in_dr, dr_recv.at[0])
    drt_ref[...] = jnp.sum(in_dr[...].astype(F32), axis=0).astype(BF16)

    def latent_from_k(g, carry):
        parts = []
        for r in range(4):
            h = xor(me, partner(4 * g + r))
            wait_bytes(in_k.at[h], k_recv.at[h])
            parts.append(h)
        weights = jnp.concatenate([wuk[:, pl.ds(pl.multiple_of(h * D, D), D)] for h in parts], axis=1)
        grads = jnp.concatenate([in_k[h] for h in parts], axis=0)
        dct[...] += nn_dot(weights, grads)
        return carry

    lax.fori_loop(0, 4, latent_from_k, 0)
    dc_ref[...] = transpose(dct[...]).astype(BF16)
    gather_k.finish()
    own_v.wait()
    own_k.wait()

    wait_bytes(o_ref, o_recv.at[0])
    wait_bytes(dq_ref, dq_recv.at[0])
    others = pl.ds(0, N - 1)
    wait_bytes(qt_ref.at[others], q_send.at[0])
    wait_bytes(do_heads.at[others], q_send.at[0])
    wait_bytes(stage_o.at[others], o_send.at[0])
    wait_bytes(stage_dq.at[others], dq_send.at[0])
    wait_bytes(stage_v.at[others], v_send.at[0])
    wait_bytes(stage_k.at[others], k_send.at[0])
    give.wait_send()
    wait_bytes(dr_sum.at[pl.ds(0, N // 2 - 1)], dr_send.at[0])
    gather_c.drain()
    gather_v.drain()
    gather_k.drain()


def close_kernel(o_ref, dq_ref, dwk_ref, dwv_ref, dc_ref, dr_ref, o_out, dq_out, dwk_out, dwv_out, dc_out, dr_out,
                 o_in, o_rows, o_back, dq_buf, dwk_buf, dwv_buf, dc_buf, dr_buf, sem_in, sem_out):
    moves = []
    for r in range(8):
        for src, dst, buf in ((dwk_ref, dwk_out, dwk_buf), (dwv_ref, dwv_out, dwv_buf)):
            moves.append((src, dst, buf, pl.ds(r * 64, 64)))
    for r in range(4):
        moves.append((dq_ref, dq_out, dq_buf, pl.ds(r * 4, 4)))
    moves.append((dc_ref, dc_out, dc_buf, pl.ds(0, T)))
    moves.append((dr_ref, dr_out, dr_buf, pl.ds(0, R)))
    first = pltpu.make_async_copy(o_ref, o_in, sem_in.at[len(moves)])
    first.start()
    ins = [pltpu.make_async_copy(src.at[rows], buf.at[rows], sem_in.at[m]) for m, (src, dst, buf, rows) in enumerate(moves)]
    outs = [pltpu.make_async_copy(buf.at[rows], dst.at[rows], sem_out.at[m]) for m, (src, dst, buf, rows) in enumerate(moves)]
    for copy in ins:
        copy.start()
    first.wait()

    def head(h, carry):
        x = o_in[h].astype(F32)
        for g in range(NT):
            o_rows[g, pl.ds(h, 32, stride=N), :] = x[g * 32:(g + 1) * 32]
        return carry

    lax.fori_loop(0, N, head, 0)
    for g in range(NT):
        o_back[pl.ds(g * 32, 32)] = o_rows[g].reshape(32, N, D).astype(BF16)
    last = pltpu.make_async_copy(o_back, o_out, sem_out.at[len(moves)])
    last.start()
    for copy, out in zip(ins, outs):
        copy.wait()
        out.start()
    for out in outs:
        out.wait()
    last.wait()


def close(*arrays):
    any_spec = pl.BlockSpec(memory_space=pl.ANY)
    dw = (L, N, D)
    return pl.pallas_call(
        close_kernel, name="close", in_specs=[any_spec] * 6, out_specs=(any_spec,) * 6,
        out_shape=(jax.ShapeDtypeStruct((T, N, D), BF16), jax.ShapeDtypeStruct((N, QK, T), BF16),
                   jax.ShapeDtypeStruct(dw, F32), jax.ShapeDtypeStruct(dw, F32),
                   jax.ShapeDtypeStruct((T, L), BF16), jax.ShapeDtypeStruct((R, T), BF16)),
        scratch_shapes=[pltpu.VMEM((N, T, D), BF16), pltpu.VMEM((NT, TK, D), F32), pltpu.VMEM((T, N, D), BF16),
                        pltpu.VMEM((N, QK, T), BF16), pltpu.VMEM(dw, F32), pltpu.VMEM(dw, F32),
                        pltpu.VMEM((T, L), BF16), pltpu.VMEM((R, T), BF16),
                        pltpu.SemaphoreType.DMA((23,)), pltpu.SemaphoreType.DMA((23,))],
        compiler_params=pltpu.CompilerParams(vmem_limit_bytes=60 << 20))(*arrays)


def solution(mesh):
    seq_spec = P("cp")

    def local_step(queries, latent, key_rope, w_uk, w_uv, d_out):
        any_spec = pl.BlockSpec(memory_space=pl.ANY)
        vmem_spec = pl.BlockSpec(memory_space=pltpu.VMEM)
        dma = pltpu.SemaphoreType.DMA
        o_all, dq_all, dc, drt, dwk, dwv = pl.pallas_call(
            kernel,
            name="mla_core",
            out_shape=(jax.ShapeDtypeStruct((N, T, D), BF16),
                       jax.ShapeDtypeStruct((N, QK, T), BF16),
                       jax.ShapeDtypeStruct((T, L), BF16),
                       jax.ShapeDtypeStruct((R, T), BF16),
                       jax.ShapeDtypeStruct((3 * W_CHUNK, N, 1, D), F32),
                       jax.ShapeDtypeStruct((3 * W_CHUNK, N, 1, D), F32)),
            in_specs=[any_spec] * 6,
            out_specs=(any_spec, any_spec, vmem_spec, vmem_spec, any_spec, any_spec),
            scratch_shapes=[
                pltpu.VMEM((N, QK, T), BF16),
                pltpu.VMEM((N, T, D), BF16),
                pltpu.VMEM((N, T, D), BF16),
                pltpu.VMEM((N, QK, T), BF16),
                pltpu.VMEM((N, D, T), BF16),
                pltpu.VMEM((N, D, T), BF16),
                pltpu.VMEM((N, D, T), BF16),
                pltpu.VMEM((N, D, T), BF16),
                pltpu.VMEM((2, N // 2, R, T), BF16),
                pltpu.VMEM((N // 2, R, T), BF16),
                pltpu.VMEM((N // 2, R, T), BF16),
                pltpu.VMEM((N // 2, R, T), BF16),
                pltpu.VMEM((N, 3 * C_CHUNK, L), BF16),
                pltpu.VMEM((NT, TK, 2 * D), BF16),
                pltpu.VMEM((NT, QK, TK), BF16),
                pltpu.VMEM((NT, TK, D), BF16),
                pltpu.VMEM((NT, D, TK), BF16),
                pltpu.VMEM((TILES, TK, T), F32),
                pltpu.VMEM((N // 2 * TILES, TK, T), BF16),
                pltpu.VMEM((2, 2 * D, T), BF16),
                pltpu.VMEM((2, T, 2 * D), BF16),
                pltpu.VMEM((N, D, T), BF16),
                pltpu.VMEM((2, T, D), BF16),
                pltpu.VMEM((NT, TK, 2 * D), F32),
                pltpu.VMEM((NT, TK, D), F32),
                pltpu.VMEM((2, D, T), F32),
                pltpu.VMEM((2, QK, T), F32),
                pltpu.VMEM((N, 8, T), F32),
                pltpu.VMEM((L, T), F32),
                pltpu.VMEM((2, L, N, D), BF16),
                pltpu.VMEM((T, N, D), BF16),
                pltpu.VMEM((N, T, D), BF16),
                pltpu.VMEM((L, 2 * D), BF16),
                pltpu.VMEM((L, N * D), BF16),
                pltpu.VMEM((L, N * D), BF16),
                pltpu.VMEM((3 * W_CHUNK, D), F32),
                pltpu.VMEM((3 * W_CHUNK, D), F32),
            ] + [dma((1,)), dma((N,))] + [dma((1,))] * 7 + [dma((N,))] + [dma((1,))] * 4 + [dma((8,))] + [dma((1,)), dma((24,)), dma((1,)), dma((1,))] * 3,
            compiler_params=pltpu.CompilerParams(
                collective_id=0, has_side_effects=True, vmem_limit_bytes=67043328),
        )(jnp.transpose(queries, (1, 2, 0)), d_out, latent, jnp.transpose(key_rope, (1, 0)),
          w_uk, w_uv)

        o, dq, dwk, dwv, dc, drt = close(
            o_all, dq_all, dwk.reshape(3 * W_CHUNK, N, D), dwv.reshape(3 * W_CHUNK, N, D), dc, drt)
        return o, jnp.transpose(dq, (2, 0, 1)), dc, jnp.transpose(drt, (1, 0)), dwk, dwv

    return jax.shard_map(local_step, mesh=mesh,
                         in_specs=(seq_spec, seq_spec, seq_spec, P(), P(), seq_spec),
                         out_specs=(seq_spec, seq_spec, seq_spec, seq_spec, P(), P()),
                         check_vma=False)
```

```python
import functools
import math
import jax
import jax.numpy as jnp
from jax import lax
from jax.experimental import pallas as pl
from jax.experimental.pallas import tpu as pltpu
from jax.sharding import PartitionSpec as P

MESH = pl.DeviceIdType.MESH
BF16 = jnp.bfloat16
F32 = jnp.float32

N = 16
T = 256
L = 512
D = 128
R = 64
QK = D + R
TK = 512
NT = 8
C_CHUNK = 96
W_CHUNK = 176
TILES = 9
ORDER = (0, 7, 3, 4, 5, 2, 6, 1)
TABLE = sum(chip << (3 * n) for n, chip in enumerate(ORDER))
SCALE = 1.0 / math.sqrt(QK)
EXP_C = SCALE * math.log2(math.e)


def nt_dot(a, b):
    return lax.dot_general(a, b, (((1,), (1,)), ((), ())), preferred_element_type=F32)


def nn_dot(a, b):
    return lax.dot_general(a, b, (((1,), (0,)), ((), ())), preferred_element_type=F32)


def flip(x, bit):
    return x + bit * (1 - 2 * lax.rem(lax.div(x, bit), 2))


def xor(x, s):
    for bit in (1, 2, 4, 8):
        on = lax.rem(lax.div(s, bit), 2)
        x = x + on * bit * (1 - 2 * lax.rem(lax.div(x, bit), 2))
    return x


def partner(n):
    k = lax.div(n, 2)
    power = (1 + 7 * lax.rem(k, 2)) * (1 + 63 * lax.rem(lax.div(k, 2), 2)) * (1 + 4095 * lax.div(k, 4))
    return 2 * lax.rem(lax.div(TABLE, power), 8) + lax.rem(n, 2)


def fold(x, reduce):
    return reduce(x.reshape(x.shape[0] // 8, 8, x.shape[1]), axis=0)


def transpose(x):
    return jnp.transpose(x, (1, 0))


class Gather:
    def __init__(self, me, own, buf, by_row, chunk, send_sem, recv_sem, sib_send, sib_recv):
        self.me, self.own, self.buf, self.by_row, self.chunk = me, own, buf, by_row, chunk
        self.send_sem, self.recv_sem = send_sem, recv_sem
        self.sib_send, self.sib_recv = sib_send, sib_recv

    def view(self, src, rows):
        return self.buf.at[rows, src, 0, :] if self.by_row else self.buf.at[src, rows, :]

    def axes(self, k):
        out = []
        for t in range(3):
            axis = lax.rem(k + t, 3)
            out.append(2 + axis * (axis + 1))
        return out

    def make(self, k, masks, mask, target, send_sem, recv_sem):
        src = self.me
        for bit in masks:
            src = flip(src, bit)
        rows = pl.ds(k * self.chunk, self.chunk)
        slot = k * 8 + lax.div(mask, 2)
        first = self.own.at[rows, :] if not masks else self.view(src, rows)
        recv = recv_sem.at[0] if recv_sem is self.sib_recv else recv_sem.at[slot]
        return pltpu.make_async_remote_copy(
            src_ref=first, dst_ref=self.view(src, rows), send_sem=send_sem.at[0], recv_sem=recv,
            device_id=(target,), device_id_type=MESH)

    def hop(self, k, masks, bit):
        return self.make(k, masks, sum(masks) + bit, flip(self.me, bit), self.send_sem, self.recv_sem)

    def sib(self, k, masks):
        return self.make(k, masks, sum(masks), flip(self.me, 1), self.sib_send, self.sib_recv)

    def arrived(self, k, masks):
        self.make(k, masks, sum(masks), flip(self.me, 1), self.send_sem, self.recv_sem).wait_recv()

    def stage0(self):
        for t in range(3):
            def send(k, carry):
                self.hop(k, (), self.axes(k)[t]).start()
                return carry
            lax.fori_loop(0, 3, send, 0)

        def send_sib(k, carry):
            self.sib(k, ()).start()
            return carry
        lax.fori_loop(0, 3, send_sib, 0)

    def stage1(self):
        def step(k, carry):
            a, b, c = self.axes(k)
            self.arrived(k, (a,))
            self.hop(k, (a,), b).start()
            self.hop(k, (a,), c).start()
            self.sib(k, (a,)).start()
            return carry
        lax.fori_loop(0, 3, step, 0)

    def stage2(self):
        for both in (False, True):
            def step(k, carry):
                a, b, c = self.axes(k)
                masks = (a, b) if both else (b,)
                self.arrived(k, masks)
                self.hop(k, masks, c).start()
                self.sib(k, masks).start()
                return carry
            lax.fori_loop(0, 3, step, 0)

    def stage3(self):
        for extra in range(4):
            def step(k, carry):
                a, b, c = self.axes(k)
                masks = ((c,), (a, c), (b, c), (a, b, c))[extra]
                self.arrived(k, masks)
                self.sib(k, masks).start()
                return carry
            lax.fori_loop(0, 3, step, 0)

    def wait_items(self, items, sem):
        ref = self.buf.at[:, pl.ds(0, items)] if self.by_row else self.buf.at[pl.ds(0, items)]
        pltpu.make_async_copy(ref, ref, sem.at[0]).wait()

    def finish(self):
        self.wait_items(8, self.sib_recv)

    def drain(self):
        self.wait_items(7, self.send_sem)
        self.wait_items(8, self.sib_send)


def wait_bytes(ref, sem):
    pltpu.make_async_copy(ref, ref, sem).wait()


def kernel(qt_ref, do_ref, c_ref, rt_ref, wuk_ref, wuv_ref,
           o_ref, dq_ref, dc_ref, drt_ref, dwk_ref, dwv_ref,
           in_q, in_do, stage_o, stage_dq, stage_v, stage_k, in_v, in_k, dr_part, dr_sib, dr_sum, in_dr, call, kcat, kt, v, vt, sbuf, prob, qz, qn, dot, own_do, dk, dv,
           ot, dqt, delta, dct, raw_w, raw_do, do_heads, w_own, wuk, wuv, dwk_own, dwv_own,
           q_send, q_recv, o_send, o_recv, dq_send, dq_recv, v_send, v_recv, k_send, k_recv, drs_send, drs_recv, dr_send, dr_recv, local_sem,
           c_send, c_recv, cs_send, cs_recv, gk_send, gk_recv, gks_send, gks_recv, gv_send, gv_recv, gvs_send, gvs_recv):
    me = lax.axis_index("cp")

    loads = [
        pltpu.make_async_copy(wuk_ref, raw_w.at[0], local_sem.at[0]),
        pltpu.make_async_copy(wuv_ref, raw_w.at[1], local_sem.at[1]),
        pltpu.make_async_copy(do_ref, raw_do, local_sem.at[7]),
        pltpu.make_async_copy(c_ref, call.at[me, pl.ds(0, T), :], local_sem.at[2]),
        pltpu.make_async_copy(rt_ref.at[pl.ds(0, 32), :], call.at[me, pl.ds(T, 32), pl.ds(0, T)], local_sem.at[3]),
        pltpu.make_async_copy(rt_ref.at[pl.ds(32, 32), :], call.at[me, pl.ds(T, 32), pl.ds(T, T)], local_sem.at[4]),
    ]
    for load in loads[::-1]:
        load.start()

    barrier = pltpu.get_barrier_semaphore()

    def hello(s, carry):
        pl.semaphore_signal(barrier, inc=1, device_id=(xor(me, s),), device_id_type=MESH)
        return carry

    lax.fori_loop(1, N, hello, 0)
    for load in loads[3:]:
        load.wait()
    pl.semaphore_wait(barrier, N - 1)

    def send(src, dst, n, send_sem, recv):
        pltpu.make_async_remote_copy(
            src_ref=src, dst_ref=dst.at[me], send_sem=send_sem.at[0], recv_sem=recv,
            device_id=(xor(me, partner(n)),), device_id_type=MESH).start()

    gather_c = Gather(me, call.at[me], call, False, C_CHUNK, c_send, c_recv, cs_send, cs_recv)
    gather_c.stage0()
    pltpu.make_async_copy(qt_ref.at[me], in_q.at[me], q_recv.at[me]).start()
    dk[...] = jnp.zeros_like(dk)
    qz[...] = jnp.zeros_like(qz)
    dwk_own[...] = jnp.zeros_like(dwk_own)
    dwv_own[...] = jnp.zeros_like(dwv_own)

    def spread(raw):
        def step(g, carry):
            dv[g] = raw[pl.ds(pl.multiple_of(g * 32, 32), 32)].astype(F32).reshape(TK, D)
            return carry

        lax.fori_loop(0, NT, step, 0)

    def one_head(h):
        return jnp.concatenate([dv[g, pl.ds(h, 32, stride=N), :] for g in range(NT)], axis=0).astype(BF16)

    def by_head(raw, put):
        spread(raw)

        def head(h, carry):
            put(h, one_head(h))
            return carry

        lax.fori_loop(0, N, head, 0)

    def put_do(h, x):
        do_heads[h] = x

    def send_q(n, carry):
        send(qt_ref.at[xor(me, partner(n))], in_q, n, q_send, q_recv.at[me])
        return carry

    def send_do(n, carry):
        send(do_heads.at[xor(me, partner(n))], in_do, n, q_send, q_recv.at[me])
        return carry

    lax.fori_loop(1, 4, send_q, 0)
    loads[2].wait()
    by_head(raw_do, put_do)
    pltpu.make_async_copy(do_heads.at[me], in_do.at[me], q_recv.at[me]).start()
    gather_c.stage1()
    gather_c.stage2()

    def send_both(n, carry):
        return send_do(n, send_q(n, carry))

    lax.fori_loop(1, 4, send_do, 0)
    lax.fori_loop(4, N, send_both, 0)
    for m in range(2):
        loads[m].wait()
        for half in range(2):
            rows = pl.ds(half * T, T)
            spread(raw_w.at[m, rows])
            w_own[rows, pl.ds(m * D, D)] = one_head(me)

    def order_weights(m, out):
        for half in range(2):
            def put_w(h, x):
                out[pl.ds(half * T, T), pl.ds(pl.multiple_of(h * D, D), D)] = x

            by_head(raw_w.at[m, pl.ds(half * T, T)], put_w)

    dv[...] = jnp.zeros_like(dv)
    gather_c.stage3()
    gather_c.finish()

    def make_kv(jt, carry):
        for half in range(2):
            j = jt * 2 + half
            rows = pl.ds(half * T, T)
            kv = nn_dot(call[j, pl.ds(0, T), :], w_own[...])
            rt = jnp.concatenate([call[j, pl.ds(T, 32), pl.ds(0, T)], call[j, pl.ds(T, 32), pl.ds(T, T)]], axis=0)
            rtz = jnp.concatenate([rt.astype(F32), jnp.zeros((R, T), F32)], axis=0)
            kcat[jt, rows, pl.ds(0, D)] = kv[:, :D].astype(BF16)
            kcat[jt, rows, pl.ds(D, D)] = transpose(rtz).astype(BF16)
            v[jt, rows, :] = kv[:, D:].astype(BF16)
            kvt = transpose(kv).astype(BF16)
            kt[jt, pl.ds(0, D), rows] = kvt[:D]
            kt[jt, pl.ds(D, R), rows] = rt
            vt[jt, :, rows] = kvt[D:]
        return carry

    lax.fori_loop(0, NT, make_kv, 0)

    def pair(p):
        na = 4 * lax.div(p, 2) + lax.rem(p, 2)
        nb = 4 * lax.div(p, 2) + 3 - lax.rem(p, 2)
        ia, ib = xor(me, partner(na)), xor(me, partner(nb))
        split = lax.div(ia, 2) + 1
        which = [jnp.minimum(lax.div(t, split), 1) for t in range(TILES)]
        tile = [split - 1] + [t - w * split - (1 - w) for t, w in enumerate(which) if t > 0]
        return (na, nb), (ia, ib), which, tile

    def pick(w, rows):
        return jnp.where(w == 1, rows[1], rows[0])

    def forward(p, carry):
        steps, blocks, which, tile = pair(p)
        for b, i in enumerate(blocks):
            wait_bytes(call.at[0, pl.ds(0, 160), :], q_recv.at[i])
            qz[b, pl.ds(0, QK), :] = in_q[i]
            own_do[b] = in_do[i]

        tile_top, tile_sum = [], []
        for t in range(TILES):
            w, jt = which[t], tile[t]
            sc = nn_dot(kcat[jt], qz[w])
            if t in (0, TILES - 1):
                ahead = lax.broadcasted_iota(jnp.int32, sc.shape, 0) - lax.broadcasted_iota(jnp.int32, sc.shape, 1)
                sc = jnp.where(ahead <= blocks[t > 0] * T - jt * TK, sc, -1e30)
            sbuf[t] = sc
            top = jnp.max(fold(sc, jnp.max), axis=0, keepdims=True) * EXP_C
            e = jnp.exp2(sbuf[t] * EXP_C - top)
            sbuf[t] = e
            tile_top.append(top)
            tile_sum.append(jnp.sum(fold(e, jnp.sum), axis=0, keepdims=True))

        tops = [functools.reduce(jnp.maximum, [jnp.where(w == b, x, -jnp.inf) for w, x in zip(which, tile_top)])
                for b in range(2)]
        factors = [jnp.exp2(x - pick(w, tops)) for w, x in zip(which, tile_top)]
        invs = [1.0 / sum(jnp.where(w == b, x * f, 0.0) for w, x, f in zip(which, tile_sum, factors)) for b in range(2)]

        ot[...] = jnp.zeros_like(ot)
        for t in range(TILES):
            w, jt = which[t], tile[t]
            prob_t = (sbuf[t] * (factors[t] * pick(w, invs))).astype(BF16)
            prob[p * TILES + t] = prob_t
            ot[w] += nn_dot(vt[jt], prob_t)
            dv[jt] += nn_dot(prob_t, own_do[w])

        for b, n in enumerate(steps):
            o_t = ot[b]
            stage_o[n] = transpose(o_t).astype(BF16)
            do_t = transpose(own_do[b].astype(F32))
            dot[p * 2 + b] = do_t.astype(BF16)
            delta[p * 2 + b] = jnp.broadcast_to(jnp.sum(o_t * do_t, axis=0, keepdims=True), (8, T))

            @pl.when(n > 0)
            def _():
                send(stage_o.at[n], o_ref, n, o_send, o_recv.at[0])

        return carry

    lax.fori_loop(0, N // 2, forward, 0)
    pltpu.make_async_copy(stage_o.at[0], o_ref.at[me], o_recv.at[0]).start()

    def block_rows(i):
        return pl.ds(pl.multiple_of(lax.rem(i, 2) * T, T), T)

    def grad_v(n, carry):
        i = xor(me, partner(n))
        stage_v[n] = transpose(dv[lax.div(i, 2), block_rows(i), :]).astype(BF16)
        return carry

    def weight_grad(stage, own):
        def step(m, acc):
            lhs = jnp.concatenate([stage[4 * m + r, pl.ds(0, D), :] for r in range(4)], axis=1)
            rhs = jnp.concatenate([call[xor(me, partner(4 * m + r)), pl.ds(0, T), :] for r in range(4)], axis=0)
            return acc + nn_dot(lhs, rhs)

        dwt = lax.fori_loop(0, 4, step, jnp.zeros((D, L), F32))
        own[pl.ds(0, L), :] = transpose(dwt)

    lax.fori_loop(0, N, grad_v, 0)
    pltpu.make_async_copy(stage_v.at[0], in_v.at[me], v_recv.at[0]).start()
    weight_grad(stage_v, dwv_own)
    gather_v = Gather(me, dwv_own, dwv_ref, False, W_CHUNK, gv_send, gv_recv, gvs_send, gvs_recv)
    all_rows = pl.ds(0, 3 * W_CHUNK)
    own_v = pltpu.make_async_copy(dwv_own, gather_v.view(me, all_rows), local_sem.at[5])
    own_v.start()
    gather_v.stage0()

    def send_v(n, carry):
        send(stage_v.at[n], in_v, n, v_send, v_recv.at[0])
        return carry

    lax.fori_loop(1, 8, send_v, 0)

    def backward(p, carry):
        steps, blocks, which, tile = pair(p)
        for b, i in enumerate(blocks):
            qz[b, pl.ds(0, QK), :] = in_q[i]
            qn[b] = transpose(qz[b].astype(F32)).astype(BF16)
        dqt[...] = jnp.zeros_like(dqt)
        deltas = [delta[p * 2 + b, pl.ds(0, 1), :] for b in range(2)]
        for t in range(TILES):
            w, jt = which[t], tile[t]
            dp = nn_dot(v[jt], dot[p * 2 + w])
            ds = (prob[p * TILES + t].astype(F32) * (dp - pick(w, deltas))).astype(BF16)
            dk[jt] += nn_dot(ds, qn[w])
            dqt[w] += nn_dot(kt[jt], ds)

        for b, n in enumerate(steps):
            stage_dq[n] = (dqt[b] * SCALE).astype(BF16)

            @pl.when(n > 0)
            def _():
                send(stage_dq.at[n], dq_ref, n, dq_send, dq_recv.at[0])

        @pl.when(p < 4)
        def _():
            send_v(8 + 2 * p, 0)
            send_v(9 + 2 * p, 0)

        @pl.when(p == 4)
        def _():
            gather_v.stage1()

        return carry

    lax.fori_loop(0, N // 2, backward, 0)
    gather_v.stage2()
    pltpu.make_async_copy(stage_dq.at[0], dq_ref.at[me], dq_recv.at[0]).start()

    def send_k(n, carry):
        send(stage_k.at[n], in_k, n, k_send, k_recv.at[me])
        return carry

    def grad_k(n, carry):
        i = xor(me, partner(n))
        key = transpose(dk[lax.div(i, 2), block_rows(i), :] * SCALE)
        stage_k[n] = key[:D].astype(BF16)
        dr_part[lax.rem(n, 2), lax.div(n, 2)] = key[D:QK].astype(BF16)

        @pl.when(lax.rem(n, 6) > 0)
        def _():
            @pl.when(n < 6)
            def _():
                send_k(n, 0)

        return carry

    lax.fori_loop(0, N, grad_k, 0)
    pltpu.make_async_copy(stage_k.at[0], in_k.at[me], k_recv.at[me]).start()

    give = pltpu.make_async_remote_copy(
        src_ref=dr_part.at[1], dst_ref=dr_sib, send_sem=drs_send.at[0], recv_sem=drs_recv.at[0],
        device_id=(flip(me, 1),), device_id_type=MESH)
    give.start()
    weight_grad(stage_k, dwk_own)
    gather_k = Gather(me, dwk_own, dwk_ref, False, W_CHUNK, gk_send, gk_recv, gks_send, gks_recv)
    own_k = pltpu.make_async_copy(dwk_own, gather_k.view(me, all_rows), local_sem.at[6])
    own_k.start()
    gather_k.stage0()
    give.wait_recv()
    dr_sum[...] = (dr_part[0].astype(F32) + dr_sib[...].astype(F32)).astype(BF16)
    chip = lax.div(me, 2)
    pltpu.make_async_copy(dr_sum.at[0], in_dr.at[chip], dr_recv.at[0]).start()

    def send_dr(k, carry):
        pltpu.make_async_remote_copy(
            src_ref=dr_sum.at[k], dst_ref=in_dr.at[chip], send_sem=dr_send.at[0], recv_sem=dr_recv.at[0],
            device_id=(xor(me, partner(2 * k)),), device_id_type=MESH).start()
        return carry

    lax.fori_loop(1, N // 2, send_dr, 0)
    order_weights(1, wuv)
    wait_bytes(in_v, v_recv.at[0])
    dct[...] = jnp.zeros_like(dct)
    gather_k.stage1()
    lax.fori_loop(6, 10, send_k, 0)

    def latent_from_v(g, carry):
        cols = pl.ds(pl.multiple_of(g * 4 * D, 4 * D), 4 * D)
        dct[...] += nn_dot(wuv[:, cols], in_v[pl.ds(4 * g, 4)].reshape(4 * D, T))
        return carry

    lax.fori_loop(0, 4, latent_from_v, 0)
    gather_k.stage2()
    lax.fori_loop(10, N, send_k, 0)
    order_weights(0, wuk)
    gather_v.stage3()
    gather_v.finish()
    gather_k.stage3()

    wait_bytes(in_dr, dr_recv.at[0])
    drt_ref[...] = jnp.sum(in_dr[...].astype(F32), axis=0).astype(BF16)

    def latent_from_k(g, carry):
        parts = []
        for r in range(4):
            h = xor(me, partner(4 * g + r))
            wait_bytes(in_k.at[h], k_recv.at[h])
            parts.append(h)
        weights = jnp.concatenate([wuk[:, pl.ds(pl.multiple_of(h * D, D), D)] for h in parts], axis=1)
        grads = jnp.concatenate([in_k[h] for h in parts], axis=0)
        dct[...] += nn_dot(weights, grads)
        return carry

    lax.fori_loop(0, 4, latent_from_k, 0)
    dc_ref[...] = transpose(dct[...]).astype(BF16)
    gather_k.finish()
    own_v.wait()
    own_k.wait()

    wait_bytes(o_ref, o_recv.at[0])
    wait_bytes(dq_ref, dq_recv.at[0])
    others = pl.ds(0, N - 1)
    wait_bytes(qt_ref.at[others], q_send.at[0])
    wait_bytes(do_heads.at[others], q_send.at[0])
    wait_bytes(stage_o.at[others], o_send.at[0])
    wait_bytes(stage_dq.at[others], dq_send.at[0])
    wait_bytes(stage_v.at[others], v_send.at[0])
    wait_bytes(stage_k.at[others], k_send.at[0])
    give.wait_send()
    wait_bytes(dr_sum.at[pl.ds(0, N // 2 - 1)], dr_send.at[0])
    gather_c.drain()
    gather_v.drain()
    gather_k.drain()


def close_kernel(o_ref, dq_ref, dwk_ref, dwv_ref, dc_ref, dr_ref, o_out, dq_out, dwk_out, dwv_out, dc_out, dr_out,
                 o_in, o_rows, o_back, dq_buf, dwk_buf, dwv_buf, dc_buf, dr_buf, sem_in, sem_out):
    moves = []
    rows = pl.ds(0, L)
    for h in range(N):
        for src, dst, buf in ((dwk_ref, dwk_out, dwk_buf), (dwv_ref, dwv_out, dwv_buf)):
            moves.append((src.at[h, rows], dst.at[:, h, 0], buf.at[h]))
    moves.append((dq_ref, dq_out, dq_buf))
    moves.append((dc_ref, dc_out, dc_buf))
    moves.append((dr_ref, dr_out, dr_buf))
    first = pltpu.make_async_copy(o_ref, o_in, sem_in.at[len(moves)])
    first.start()
    ins = [pltpu.make_async_copy(src, buf, sem_in.at[m]) for m, (src, dst, buf) in enumerate(moves)]
    outs = [pltpu.make_async_copy(buf, dst, sem_out.at[m]) for m, (src, dst, buf) in enumerate(moves)]
    for copy in ins:
        copy.start()
    first.wait()

    def head(h, carry):
        x = o_in[h].astype(F32)
        for g in range(NT):
            o_rows[g, pl.ds(h, 32, stride=N), :] = x[g * 32:(g + 1) * 32]
        return carry

    lax.fori_loop(0, N, head, 0)
    for g in range(NT):
        o_back[pl.ds(g * 32, 32)] = o_rows[g].reshape(32, N, D).astype(BF16)
    last = pltpu.make_async_copy(o_back, o_out, sem_out.at[len(moves)])
    last.start()
    for copy, out in zip(ins, outs):
        copy.wait()
        out.start()
    for out in outs:
        out.wait()
    last.wait()


def close(*arrays):
    any_spec = pl.BlockSpec(memory_space=pl.ANY)
    dw = (L, N, 1, D)
    dw_buf = (N, L, D)
    return pl.pallas_call(
        close_kernel, name="close", in_specs=[any_spec] * 6, out_specs=(any_spec,) * 6,
        out_shape=(jax.ShapeDtypeStruct((T, N, D), BF16), jax.ShapeDtypeStruct((N, QK, T), BF16),
                   jax.ShapeDtypeStruct(dw, F32), jax.ShapeDtypeStruct(dw, F32),
                   jax.ShapeDtypeStruct((T, L), BF16), jax.ShapeDtypeStruct((R, T), BF16)),
        scratch_shapes=[pltpu.VMEM((N, T, D), BF16), pltpu.VMEM((NT, TK, D), F32), pltpu.VMEM((T, N, D), BF16),
                        pltpu.VMEM((N, QK, T), BF16), pltpu.VMEM(dw_buf, F32), pltpu.VMEM(dw_buf, F32),
                        pltpu.VMEM((T, L), BF16), pltpu.VMEM((R, T), BF16),
                        pltpu.SemaphoreType.DMA((36,)), pltpu.SemaphoreType.DMA((36,))],
        compiler_params=pltpu.CompilerParams(vmem_limit_bytes=60 << 20))(*arrays)


def solution(mesh):
    seq_spec = P("cp")

    def local_step(queries, latent, key_rope, w_uk, w_uv, d_out):
        any_spec = pl.BlockSpec(memory_space=pl.ANY)
        vmem_spec = pl.BlockSpec(memory_space=pltpu.VMEM)
        dma = pltpu.SemaphoreType.DMA
        o_all, dq_all, dc, drt, dwk, dwv = pl.pallas_call(
            kernel,
            name="mla_core",
            out_shape=(jax.ShapeDtypeStruct((N, T, D), BF16),
                       jax.ShapeDtypeStruct((N, QK, T), BF16),
                       jax.ShapeDtypeStruct((T, L), BF16),
                       jax.ShapeDtypeStruct((R, T), BF16),
                       jax.ShapeDtypeStruct((N, 3 * W_CHUNK, D), F32),
                       jax.ShapeDtypeStruct((N, 3 * W_CHUNK, D), F32)),
            in_specs=[any_spec] * 6,
            out_specs=(any_spec, any_spec, vmem_spec, vmem_spec, any_spec, any_spec),
            scratch_shapes=[
                pltpu.VMEM((N, QK, T), BF16),
                pltpu.VMEM((N, T, D), BF16),
                pltpu.VMEM((N, T, D), BF16),
                pltpu.VMEM((N, QK, T), BF16),
                pltpu.VMEM((N, D, T), BF16),
                pltpu.VMEM((N, D, T), BF16),
                pltpu.VMEM((N, D, T), BF16),
                pltpu.VMEM((N, D, T), BF16),
                pltpu.VMEM((2, N // 2, R, T), BF16),
                pltpu.VMEM((N // 2, R, T), BF16),
                pltpu.VMEM((N // 2, R, T), BF16),
                pltpu.VMEM((N // 2, R, T), BF16),
                pltpu.VMEM((N, 3 * C_CHUNK, L), BF16),
                pltpu.VMEM((NT, TK, 2 * D), BF16),
                pltpu.VMEM((NT, QK, TK), BF16),
                pltpu.VMEM((NT, TK, D), BF16),
                pltpu.VMEM((NT, D, TK), BF16),
                pltpu.VMEM((TILES, TK, T), F32),
                pltpu.VMEM((N // 2 * TILES, TK, T), BF16),
                pltpu.VMEM((2, 2 * D, T), BF16),
                pltpu.VMEM((2, T, 2 * D), BF16),
                pltpu.VMEM((N, D, T), BF16),
                pltpu.VMEM((2, T, D), BF16),
                pltpu.VMEM((NT, TK, 2 * D), F32),
                pltpu.VMEM((NT, TK, D), F32),
                pltpu.VMEM((2, D, T), F32),
                pltpu.VMEM((2, QK, T), F32),
                pltpu.VMEM((N, 8, T), F32),
                pltpu.VMEM((L, T), F32),
                pltpu.VMEM((2, L, N, D), BF16),
                pltpu.VMEM((T, N, D), BF16),
                pltpu.VMEM((N, T, D), BF16),
                pltpu.VMEM((L, 2 * D), BF16),
                pltpu.VMEM((L, N * D), BF16),
                pltpu.VMEM((L, N * D), BF16),
                pltpu.VMEM((3 * W_CHUNK, D), F32),
                pltpu.VMEM((3 * W_CHUNK, D), F32),
            ] + [dma((1,)), dma((N,))] + [dma((1,))] * 7 + [dma((N,))] + [dma((1,))] * 4 + [dma((8,))] + [dma((1,)), dma((24,)), dma((1,)), dma((1,))] * 3,
            compiler_params=pltpu.CompilerParams(
                collective_id=0, has_side_effects=True, vmem_limit_bytes=67043328),
        )(jnp.transpose(queries, (1, 2, 0)), d_out, latent, jnp.transpose(key_rope, (1, 0)),
          w_uk, w_uv)

        o, dq, dwk, dwv, dc, drt = close(
            o_all, dq_all, dwk, dwv, dc, drt)
        return o, jnp.transpose(dq, (2, 0, 1)), dc, jnp.transpose(drt, (1, 0)), dwk.reshape(L, N, D), dwv.reshape(L, N, D)

    return jax.shard_map(local_step, mesh=mesh,
                         in_specs=(seq_spec, seq_spec, seq_spec, P(), P(), seq_spec),
                         out_specs=(seq_spec, seq_spec, seq_spec, seq_spec, P(), P()),
                         check_vma=False)
```

```python
import functools
import math
import jax
import jax.numpy as jnp
from jax import lax
from jax.experimental import pallas as pl
from jax.experimental.pallas import tpu as pltpu
from jax.sharding import PartitionSpec as P

MESH = pl.DeviceIdType.MESH
BF16 = jnp.bfloat16
F32 = jnp.float32

N = 16
T = 256
L = 512
D = 128
R = 64
QK = D + R
TK = 512
NT = 8
C_CHUNK = 96
W_CHUNK = 176
TILES = 9
ORDER = (0, 7, 3, 4, 5, 2, 6, 1)
TABLE = sum(chip << (3 * n) for n, chip in enumerate(ORDER))
SCALE = 1.0 / math.sqrt(QK)
EXP_C = SCALE * math.log2(math.e)


def nt_dot(a, b):
    return lax.dot_general(a, b, (((1,), (1,)), ((), ())), preferred_element_type=F32)


def nn_dot(a, b):
    return lax.dot_general(a, b, (((1,), (0,)), ((), ())), preferred_element_type=F32)


def flip(x, bit):
    return x + bit * (1 - 2 * lax.rem(lax.div(x, bit), 2))


def xor(x, s):
    for bit in (1, 2, 4, 8):
        on = lax.rem(lax.div(s, bit), 2)
        x = x + on * bit * (1 - 2 * lax.rem(lax.div(x, bit), 2))
    return x


def partner(n):
    k = lax.div(n, 2)
    power = (1 + 7 * lax.rem(k, 2)) * (1 + 63 * lax.rem(lax.div(k, 2), 2)) * (1 + 4095 * lax.div(k, 4))
    return 2 * lax.rem(lax.div(TABLE, power), 8) + lax.rem(n, 2)


def fold(x, reduce):
    return reduce(x.reshape(x.shape[0] // 8, 8, x.shape[1]), axis=0)


def transpose(x):
    return jnp.transpose(x, (1, 0))


class Gather:
    def __init__(self, me, own, buf, by_row, chunk, send_sem, recv_sem, sib_send, sib_recv):
        self.me, self.own, self.buf, self.by_row, self.chunk = me, own, buf, by_row, chunk
        self.send_sem, self.recv_sem = send_sem, recv_sem
        self.sib_send, self.sib_recv = sib_send, sib_recv

    def view(self, src, rows):
        return self.buf.at[rows, src, 0, :] if self.by_row else self.buf.at[src, rows, :]

    def axes(self, k):
        out = []
        for t in range(3):
            axis = lax.rem(k + t, 3)
            out.append(2 + axis * (axis + 1))
        return out

    def make(self, k, masks, mask, target, send_sem, recv_sem):
        src = self.me
        for bit in masks:
            src = flip(src, bit)
        rows = pl.ds(k * self.chunk, self.chunk)
        slot = k * 8 + lax.div(mask, 2)
        first = self.own.at[rows, :] if not masks else self.view(src, rows)
        recv = recv_sem.at[0] if recv_sem is self.sib_recv else recv_sem.at[slot]
        return pltpu.make_async_remote_copy(
            src_ref=first, dst_ref=self.view(src, rows), send_sem=send_sem.at[0], recv_sem=recv,
            device_id=(target,), device_id_type=MESH)

    def hop(self, k, masks, bit):
        return self.make(k, masks, sum(masks) + bit, flip(self.me, bit), self.send_sem, self.recv_sem)

    def sib(self, k, masks):
        return self.make(k, masks, sum(masks), flip(self.me, 1), self.sib_send, self.sib_recv)

    def arrived(self, k, masks):
        self.make(k, masks, sum(masks), flip(self.me, 1), self.send_sem, self.recv_sem).wait_recv()

    def stage0(self):
        for t in range(3):
            def send(k, carry):
                self.hop(k, (), self.axes(k)[t]).start()
                return carry
            lax.fori_loop(0, 3, send, 0)

        def send_sib(k, carry):
            self.sib(k, ()).start()
            return carry
        lax.fori_loop(0, 3, send_sib, 0)

    def stage1(self):
        def step(k, carry):
            a, b, c = self.axes(k)
            self.arrived(k, (a,))
            self.hop(k, (a,), b).start()
            self.hop(k, (a,), c).start()
            self.sib(k, (a,)).start()
            return carry
        lax.fori_loop(0, 3, step, 0)

    def stage2(self):
        for both in (False, True):
            def step(k, carry):
                a, b, c = self.axes(k)
                masks = (a, b) if both else (b,)
                self.arrived(k, masks)
                self.hop(k, masks, c).start()
                self.sib(k, masks).start()
                return carry
            lax.fori_loop(0, 3, step, 0)

    def stage3(self):
        for extra in range(4):
            def step(k, carry):
                a, b, c = self.axes(k)
                masks = ((c,), (a, c), (b, c), (a, b, c))[extra]
                self.arrived(k, masks)
                self.sib(k, masks).start()
                return carry
            lax.fori_loop(0, 3, step, 0)

    def wait_items(self, items, sem):
        ref = self.buf.at[:, pl.ds(0, items)] if self.by_row else self.buf.at[pl.ds(0, items)]
        pltpu.make_async_copy(ref, ref, sem.at[0]).wait()

    def finish(self):
        self.wait_items(8, self.sib_recv)

    def drain(self):
        self.wait_items(7, self.send_sem)
        self.wait_items(8, self.sib_send)


def wait_bytes(ref, sem):
    pltpu.make_async_copy(ref, ref, sem).wait()


def kernel(qt_ref, do_ref, c_ref, rt_ref, wuk_ref, wuv_ref,
           o_ref, dq_ref, dc_ref, drt_ref, dwk_ref, dwv_ref,
           in_q, in_do, stage_o, stage_dq, stage_v, in_v, in_k, dr_part, dr_sib, dr_sum, in_dr, call, kcat, kt, v, vt, sbuf, prob, qz, qn, dot, own_do, dk, dv,
           ot, dqt, delta, raw_w, raw_do, do_heads, w_own, wuk, wuv, dwk_own, dwv_own,
           q_send, q_recv, o_send, o_recv, dq_send, dq_recv, v_send, v_recv, k_send, k_recv, drs_send, drs_recv, dr_send, dr_recv, local_sem,
           c_send, c_recv, cs_send, cs_recv, gk_send, gk_recv, gks_send, gks_recv, gv_send, gv_recv, gvs_send, gvs_recv):
    me = lax.axis_index("cp")
    stage_k, dct = dot, sbuf.at[0]

    loads = [
        pltpu.make_async_copy(wuk_ref, raw_w.at[0], local_sem.at[0]),
        pltpu.make_async_copy(wuv_ref, raw_w.at[1], local_sem.at[1]),
        pltpu.make_async_copy(do_ref, raw_do, local_sem.at[7]),
        pltpu.make_async_copy(c_ref, call.at[me, pl.ds(0, T), :], local_sem.at[2]),
        pltpu.make_async_copy(rt_ref.at[pl.ds(0, 32), :], call.at[me, pl.ds(T, 32), pl.ds(0, T)], local_sem.at[3]),
        pltpu.make_async_copy(rt_ref.at[pl.ds(32, 32), :], call.at[me, pl.ds(T, 32), pl.ds(T, T)], local_sem.at[4]),
    ]
    for load in loads[::-1]:
        load.start()

    barrier = pltpu.get_barrier_semaphore()

    def hello(s, carry):
        pl.semaphore_signal(barrier, inc=1, device_id=(xor(me, s),), device_id_type=MESH)
        return carry

    lax.fori_loop(1, N, hello, 0)
    for load in loads[3:]:
        load.wait()
    pl.semaphore_wait(barrier, N - 1)

    def send(src, dst, n, send_sem, recv):
        pltpu.make_async_remote_copy(
            src_ref=src, dst_ref=dst.at[me], send_sem=send_sem.at[0], recv_sem=recv,
            device_id=(xor(me, partner(n)),), device_id_type=MESH).start()

    gather_c = Gather(me, call.at[me], call, False, C_CHUNK, c_send, c_recv, cs_send, cs_recv)
    gather_c.stage0()
    pltpu.make_async_copy(qt_ref.at[me], in_q.at[me], q_recv.at[me]).start()
    dk[...] = jnp.zeros_like(dk)
    qz[...] = jnp.zeros_like(qz)
    dwk_own[...] = jnp.zeros_like(dwk_own)
    dwv_own[...] = jnp.zeros_like(dwv_own)

    def spread(raw):
        def step(g, carry):
            dv[g] = raw[pl.ds(pl.multiple_of(g * 32, 32), 32)].astype(F32).reshape(TK, D)
            return carry

        lax.fori_loop(0, NT, step, 0)

    def one_head(h):
        return jnp.concatenate([dv[g, pl.ds(h, 32, stride=N), :] for g in range(NT)], axis=0).astype(BF16)

    def by_head(raw, put):
        spread(raw)

        def head(h, carry):
            put(h, one_head(h))
            return carry

        lax.fori_loop(0, N, head, 0)

    def put_do(h, x):
        do_heads[h] = x

    def send_q(n, carry):
        send(qt_ref.at[xor(me, partner(n))], in_q, n, q_send, q_recv.at[me])
        return carry

    def send_do(n, carry):
        send(do_heads.at[xor(me, partner(n))], in_do, n, q_send, q_recv.at[me])
        return carry

    lax.fori_loop(1, 4, send_q, 0)
    loads[2].wait()
    by_head(raw_do, put_do)
    pltpu.make_async_copy(do_heads.at[me], in_do.at[me], q_recv.at[me]).start()
    gather_c.stage1()
    gather_c.stage2()

    def send_both(n, carry):
        return send_do(n, send_q(n, carry))

    lax.fori_loop(1, 4, send_do, 0)
    lax.fori_loop(4, N, send_both, 0)
    for m in range(2):
        loads[m].wait()
        for half in range(2):
            rows = pl.ds(half * T, T)
            spread(raw_w.at[m, rows])
            w_own[rows, pl.ds(m * D, D)] = one_head(me)

    def order_weights(m, out):
        for half in range(2):
            def put_w(h, x):
                out[pl.ds(half * T, T), pl.ds(pl.multiple_of(h * D, D), D)] = x

            by_head(raw_w.at[m, pl.ds(half * T, T)], put_w)

    dv[...] = jnp.zeros_like(dv)
    gather_c.stage3()
    gather_c.finish()

    def make_kv(jt, carry):
        for half in range(2):
            j = jt * 2 + half
            rows = pl.ds(half * T, T)
            kv = nn_dot(call[j, pl.ds(0, T), :], w_own[...])
            rt = jnp.concatenate([call[j, pl.ds(T, 32), pl.ds(0, T)], call[j, pl.ds(T, 32), pl.ds(T, T)]], axis=0)
            rtz = jnp.concatenate([rt.astype(F32), jnp.zeros((R, T), F32)], axis=0)
            kcat[jt, rows, pl.ds(0, D)] = kv[:, :D].astype(BF16)
            kcat[jt, rows, pl.ds(D, D)] = transpose(rtz).astype(BF16)
            v[jt, rows, :] = kv[:, D:].astype(BF16)
            kvt = transpose(kv).astype(BF16)
            kt[jt, pl.ds(0, D), rows] = kvt[:D]
            kt[jt, pl.ds(D, R), rows] = rt
            vt[jt, :, rows] = kvt[D:]
        return carry

    def make_kv_two(jt, carry):
        return make_kv(2 * jt + 1, make_kv(2 * jt, carry))

    lax.fori_loop(0, NT // 2, make_kv_two, 0)

    def pair(p):
        na = 4 * lax.div(p, 2) + lax.rem(p, 2)
        nb = 4 * lax.div(p, 2) + 3 - lax.rem(p, 2)
        ia, ib = xor(me, partner(na)), xor(me, partner(nb))
        split = lax.div(ia, 2) + 1
        which = [jnp.minimum(lax.div(t, split), 1) for t in range(TILES)]
        tile = [split - 1] + [t - w * split - (1 - w) for t, w in enumerate(which) if t > 0]
        return (na, nb), (ia, ib), which, tile

    def pick(w, rows):
        return jnp.where(w == 1, rows[1], rows[0])

    def forward(p, carry):
        steps, blocks, which, tile = pair(p)
        for b, i in enumerate(blocks):
            wait_bytes(call.at[0, pl.ds(0, 160), :], q_recv.at[i])
            qz[b, pl.ds(0, QK), :] = in_q[i]
            own_do[b] = in_do[i]

        tile_top, tile_sum = [], []
        for t in range(TILES):
            w, jt = which[t], tile[t]
            sc = nn_dot(kcat[jt], qz[w])
            if t in (0, TILES - 1):
                ahead = lax.broadcasted_iota(jnp.int32, sc.shape, 0) - lax.broadcasted_iota(jnp.int32, sc.shape, 1)
                sc = jnp.where(ahead <= blocks[t > 0] * T - jt * TK, sc, -1e30)
            sbuf[t] = sc
            top = jnp.max(fold(sc, jnp.max), axis=0, keepdims=True) * EXP_C
            e = jnp.exp2(sbuf[t] * EXP_C - top)
            sbuf[t] = e
            tile_top.append(top)
            tile_sum.append(jnp.sum(fold(e, jnp.sum), axis=0, keepdims=True))

        tops = [functools.reduce(jnp.maximum, [jnp.where(w == b, x, -jnp.inf) for w, x in zip(which, tile_top)])
                for b in range(2)]
        factors = [jnp.exp2(x - pick(w, tops)) for w, x in zip(which, tile_top)]
        invs = [1.0 / sum(jnp.where(w == b, x * f, 0.0) for w, x, f in zip(which, tile_sum, factors)) for b in range(2)]

        ot[...] = jnp.zeros_like(ot)
        for t in range(TILES):
            w, jt = which[t], tile[t]
            prob_t = (sbuf[t] * (factors[t] * pick(w, invs))).astype(BF16)
            prob[p * TILES + t] = prob_t
            ot[w] += nn_dot(vt[jt], prob_t)
            dv[jt] += nn_dot(prob_t, own_do[w])

        for b, n in enumerate(steps):
            o_t = ot[b]
            stage_o[n] = transpose(o_t).astype(BF16)
            do_t = transpose(own_do[b].astype(F32))
            dot[p * 2 + b] = do_t.astype(BF16)
            delta[p * 2 + b] = jnp.broadcast_to(jnp.sum(o_t * do_t, axis=0, keepdims=True), (8, T))

            @pl.when(n > 0)
            def _():
                send(stage_o.at[n], o_ref, n, o_send, o_recv.at[0])

        return carry

    def forward_two(p, carry):
        return forward(2 * p + 1, forward(2 * p, carry))

    lax.fori_loop(0, N // 4, forward_two, 0)
    pltpu.make_async_copy(stage_o.at[0], o_ref.at[me], o_recv.at[0]).start()

    def block_rows(i):
        return pl.ds(pl.multiple_of(lax.rem(i, 2) * T, T), T)

    def grad_v(n, carry):
        i = xor(me, partner(n))
        stage_v[n] = transpose(dv[lax.div(i, 2), block_rows(i), :]).astype(BF16)
        return carry

    def weight_grad(stage, own):
        def step(m, acc):
            lhs = jnp.concatenate([stage[4 * m + r, pl.ds(0, D), :] for r in range(4)], axis=1)
            rhs = jnp.concatenate([call[xor(me, partner(4 * m + r)), pl.ds(0, T), :] for r in range(4)], axis=0)
            return acc + nn_dot(lhs, rhs)

        dwt = lax.fori_loop(0, 4, step, jnp.zeros((D, L), F32))
        own[pl.ds(0, L), :] = transpose(dwt)

    lax.fori_loop(0, N, grad_v, 0)
    pltpu.make_async_copy(stage_v.at[0], in_v.at[me], v_recv.at[0]).start()
    weight_grad(stage_v, dwv_own)
    gather_v = Gather(me, dwv_own, dwv_ref, True, W_CHUNK, gv_send, gv_recv, gvs_send, gvs_recv)
    all_rows = pl.ds(0, 3 * W_CHUNK)
    own_v = pltpu.make_async_copy(dwv_own, gather_v.view(me, all_rows), local_sem.at[5])
    own_v.start()
    gather_v.stage0()

    def send_v(n, carry):
        send(stage_v.at[n], in_v, n, v_send, v_recv.at[0])
        return carry

    lax.fori_loop(1, 8, send_v, 0)

    def backward(p, carry):
        steps, blocks, which, tile = pair(p)
        for b, i in enumerate(blocks):
            qz[b, pl.ds(0, QK), :] = in_q[i]
            qn[b] = transpose(qz[b].astype(F32)).astype(BF16)
        dqt[...] = jnp.zeros_like(dqt)
        deltas = [delta[p * 2 + b, pl.ds(0, 1), :] for b in range(2)]
        for t in range(TILES):
            w, jt = which[t], tile[t]
            dp = nn_dot(v[jt], dot[p * 2 + w])
            ds = (prob[p * TILES + t].astype(F32) * (dp - pick(w, deltas))).astype(BF16)
            dk[jt] += nn_dot(ds, qn[w])
            dqt[w] += nn_dot(kt[jt], ds)

        for b, n in enumerate(steps):
            stage_dq[n] = (dqt[b] * SCALE).astype(BF16)

            @pl.when(n > 0)
            def _():
                send(stage_dq.at[n], dq_ref, n, dq_send, dq_recv.at[0])

        @pl.when(p < 4)
        def _():
            send_v(8 + 2 * p, 0)
            send_v(9 + 2 * p, 0)

        @pl.when(p == 4)
        def _():
            gather_v.stage1()

        return carry

    lax.fori_loop(0, N // 2, backward, 0)
    gather_v.stage2()
    pltpu.make_async_copy(stage_dq.at[0], dq_ref.at[me], dq_recv.at[0]).start()

    def send_k(n, carry):
        send(stage_k.at[n], in_k, n, k_send, k_recv.at[me])
        return carry

    def grad_k(n, carry):
        i = xor(me, partner(n))
        key = transpose(dk[lax.div(i, 2), block_rows(i), :] * SCALE)
        stage_k[n] = key[:D].astype(BF16)
        dr_part[lax.rem(n, 2), lax.div(n, 2)] = key[D:QK].astype(BF16)

        @pl.when(lax.rem(n, 6) > 0)
        def _():
            @pl.when(n < 6)
            def _():
                send_k(n, 0)

        return carry

    lax.fori_loop(0, N, grad_k, 0)
    pltpu.make_async_copy(stage_k.at[0], in_k.at[me], k_recv.at[me]).start()

    give = pltpu.make_async_remote_copy(
        src_ref=dr_part.at[1], dst_ref=dr_sib, send_sem=drs_send.at[0], recv_sem=drs_recv.at[0],
        device_id=(flip(me, 1),), device_id_type=MESH)
    give.start()
    weight_grad(stage_k, dwk_own)
    gather_k = Gather(me, dwk_own, dwk_ref, True, W_CHUNK, gk_send, gk_recv, gks_send, gks_recv)
    own_k = pltpu.make_async_copy(dwk_own, gather_k.view(me, all_rows), local_sem.at[6])
    own_k.start()
    gather_k.stage0()
    give.wait_recv()
    dr_sum[...] = (dr_part[0].astype(F32) + dr_sib[...].astype(F32)).astype(BF16)
    chip = lax.div(me, 2)
    pltpu.make_async_copy(dr_sum.at[0], in_dr.at[chip], dr_recv.at[0]).start()

    def send_dr(k, carry):
        pltpu.make_async_remote_copy(
            src_ref=dr_sum.at[k], dst_ref=in_dr.at[chip], send_sem=dr_send.at[0], recv_sem=dr_recv.at[0],
            device_id=(xor(me, partner(2 * k)),), device_id_type=MESH).start()
        return carry

    lax.fori_loop(1, N // 2, send_dr, 0)
    order_weights(1, wuv)
    wait_bytes(in_v, v_recv.at[0])
    dct[...] = jnp.zeros_like(dct)
    gather_k.stage1()
    lax.fori_loop(6, 10, send_k, 0)

    def latent_from_v(g, carry):
        cols = pl.ds(pl.multiple_of(g * 4 * D, 4 * D), 4 * D)
        dct[...] += nn_dot(wuv[:, cols], in_v[pl.ds(4 * g, 4)].reshape(4 * D, T))
        return carry

    lax.fori_loop(0, 4, latent_from_v, 0)
    gather_k.stage2()
    lax.fori_loop(10, N, send_k, 0)
    order_weights(0, wuk)
    gather_v.stage3()
    gather_v.finish()
    gather_k.stage3()

    wait_bytes(in_dr, dr_recv.at[0])
    drt_ref[...] = jnp.sum(in_dr[...].astype(F32), axis=0).astype(BF16)

    def latent_from_k(g, carry):
        parts = []
        for r in range(4):
            h = xor(me, partner(4 * g + r))
            wait_bytes(in_k.at[h], k_recv.at[h])
            parts.append(h)
        weights = jnp.concatenate([wuk[:, pl.ds(pl.multiple_of(h * D, D), D)] for h in parts], axis=1)
        grads = jnp.concatenate([in_k[h] for h in parts], axis=0)
        dct[...] += nn_dot(weights, grads)
        return carry

    lax.fori_loop(0, 4, latent_from_k, 0)
    dc_ref[...] = transpose(dct[...]).astype(BF16)
    gather_k.finish()
    own_v.wait()
    own_k.wait()

    wait_bytes(o_ref, o_recv.at[0])
    wait_bytes(dq_ref, dq_recv.at[0])
    others = pl.ds(0, N - 1)
    wait_bytes(qt_ref.at[others], q_send.at[0])
    wait_bytes(do_heads.at[others], q_send.at[0])
    wait_bytes(stage_o.at[others], o_send.at[0])
    wait_bytes(stage_dq.at[others], dq_send.at[0])
    wait_bytes(stage_v.at[others], v_send.at[0])
    wait_bytes(stage_k.at[others], k_send.at[0])
    give.wait_send()
    wait_bytes(dr_sum.at[pl.ds(0, N // 2 - 1)], dr_send.at[0])
    gather_c.drain()
    gather_v.drain()
    gather_k.drain()


def close_kernel(o_ref, dq_ref, dwk_ref, dwv_ref, dc_ref, dr_ref, o_out, dq_out, dwk_out, dwv_out, dc_out, dr_out,
                 o_in, o_rows, o_back, dq_buf, dwk_buf, dwv_buf, dc_buf, dr_buf, sem_in, sem_out):
    moves = []
    for r in range(8):
        for src, dst, buf in ((dwk_ref, dwk_out, dwk_buf), (dwv_ref, dwv_out, dwv_buf)):
            moves.append((src, dst, buf, pl.ds(r * 64, 64)))
    for r in range(4):
        moves.append((dq_ref, dq_out, dq_buf, pl.ds(r * 4, 4)))
    moves.append((dc_ref, dc_out, dc_buf, pl.ds(0, T)))
    moves.append((dr_ref, dr_out, dr_buf, pl.ds(0, R)))
    first = pltpu.make_async_copy(o_ref, o_in, sem_in.at[len(moves)])
    first.start()
    ins = [pltpu.make_async_copy(src.at[rows], buf.at[rows], sem_in.at[m]) for m, (src, dst, buf, rows) in enumerate(moves)]
    outs = [pltpu.make_async_copy(buf.at[rows], dst.at[rows], sem_out.at[m]) for m, (src, dst, buf, rows) in enumerate(moves)]
    for copy in ins:
        copy.start()
    first.wait()

    def head(h, carry):
        x = o_in[h].astype(F32)
        for g in range(NT):
            o_rows[g, pl.ds(h, 32, stride=N), :] = x[g * 32:(g + 1) * 32]
        return carry

    lax.fori_loop(0, N, head, 0)
    for g in range(NT):
        o_back[pl.ds(g * 32, 32)] = o_rows[g].reshape(32, N, D).astype(BF16)
    last = pltpu.make_async_copy(o_back, o_out, sem_out.at[len(moves)])
    last.start()
    for copy, out in zip(ins, outs):
        copy.wait()
        out.start()
    for out in outs:
        out.wait()
    last.wait()


def close(*arrays):
    any_spec = pl.BlockSpec(memory_space=pl.ANY)
    dw = (L, N, D)
    return pl.pallas_call(
        close_kernel, name="close", in_specs=[any_spec] * 6, out_specs=(any_spec,) * 6,
        out_shape=(jax.ShapeDtypeStruct((T, N, D), BF16), jax.ShapeDtypeStruct((N, QK, T), BF16),
                   jax.ShapeDtypeStruct(dw, F32), jax.ShapeDtypeStruct(dw, F32),
                   jax.ShapeDtypeStruct((T, L), BF16), jax.ShapeDtypeStruct((R, T), BF16)),
        scratch_shapes=[pltpu.VMEM((N, T, D), BF16), pltpu.VMEM((NT, TK, D), F32), pltpu.VMEM((T, N, D), BF16),
                        pltpu.VMEM((N, QK, T), BF16), pltpu.VMEM(dw, F32), pltpu.VMEM(dw, F32),
                        pltpu.VMEM((T, L), BF16), pltpu.VMEM((R, T), BF16),
                        pltpu.SemaphoreType.DMA((23,)), pltpu.SemaphoreType.DMA((23,))],
        compiler_params=pltpu.CompilerParams(vmem_limit_bytes=60 << 20))(*arrays)


def solution(mesh):
    seq_spec = P("cp")

    def local_step(queries, latent, key_rope, w_uk, w_uv, d_out):
        any_spec = pl.BlockSpec(memory_space=pl.ANY)
        vmem_spec = pl.BlockSpec(memory_space=pltpu.VMEM)
        dma = pltpu.SemaphoreType.DMA
        o_all, dq_all, dc, drt, dwk, dwv = pl.pallas_call(
            kernel,
            name="mla_core",
            out_shape=(jax.ShapeDtypeStruct((N, T, D), BF16),
                       jax.ShapeDtypeStruct((N, QK, T), BF16),
                       jax.ShapeDtypeStruct((T, L), BF16),
                       jax.ShapeDtypeStruct((R, T), BF16),
                       jax.ShapeDtypeStruct((3 * W_CHUNK, N, 1, D), F32),
                       jax.ShapeDtypeStruct((3 * W_CHUNK, N, 1, D), F32)),
            in_specs=[any_spec] * 6,
            out_specs=(any_spec, any_spec, vmem_spec, vmem_spec, any_spec, any_spec),
            scratch_shapes=[
                pltpu.VMEM((N, QK, T), BF16),
                pltpu.VMEM((N, T, D), BF16),
                pltpu.VMEM((N, T, D), BF16),
                pltpu.VMEM((N, QK, T), BF16),
                pltpu.VMEM((N, D, T), BF16),
                pltpu.VMEM((N, D, T), BF16),
                pltpu.VMEM((N, D, T), BF16),
                pltpu.VMEM((2, N // 2, R, T), BF16),
                pltpu.VMEM((N // 2, R, T), BF16),
                pltpu.VMEM((N // 2, R, T), BF16),
                pltpu.VMEM((N // 2, R, T), BF16),
                pltpu.VMEM((N, 3 * C_CHUNK, L), BF16),
                pltpu.VMEM((NT, TK, 2 * D), BF16),
                pltpu.VMEM((NT, QK, TK), BF16),
                pltpu.VMEM((NT, TK, D), BF16),
                pltpu.VMEM((NT, D, TK), BF16),
                pltpu.VMEM((TILES, TK, T), F32),
                pltpu.VMEM((N // 2 * TILES, TK, T), BF16),
                pltpu.VMEM((2, 2 * D, T), BF16),
                pltpu.VMEM((2, T, 2 * D), BF16),
                pltpu.VMEM((N, D, T), BF16),
                pltpu.VMEM((2, T, D), BF16),
                pltpu.VMEM((NT, TK, 2 * D), F32),
                pltpu.VMEM((NT, TK, D), F32),
                pltpu.VMEM((2, D, T), F32),
                pltpu.VMEM((2, QK, T), F32),
                pltpu.VMEM((N, 8, T), F32),
                pltpu.VMEM((2, L, N, D), BF16),
                pltpu.VMEM((T, N, D), BF16),
                pltpu.VMEM((N, T, D), BF16),
                pltpu.VMEM((L, 2 * D), BF16),
                pltpu.VMEM((L, N * D), BF16),
                pltpu.VMEM((L, N * D), BF16),
                pltpu.VMEM((3 * W_CHUNK, D), F32),
                pltpu.VMEM((3 * W_CHUNK, D), F32),
            ] + [dma((1,)), dma((N,))] + [dma((1,))] * 7 + [dma((N,))] + [dma((1,))] * 4 + [dma((8,))] + [dma((1,)), dma((24,)), dma((1,)), dma((1,))] * 3,
            compiler_params=pltpu.CompilerParams(
                collective_id=0, has_side_effects=True, vmem_limit_bytes=67043328),
        )(jnp.transpose(queries, (1, 2, 0)), d_out, latent, jnp.transpose(key_rope, (1, 0)),
          w_uk, w_uv)

        o, dq, dwk, dwv, dc, drt = close(
            o_all, dq_all, dwk.reshape(3 * W_CHUNK, N, D), dwv.reshape(3 * W_CHUNK, N, D), dc, drt)
        return o, jnp.transpose(dq, (2, 0, 1)), dc, jnp.transpose(drt, (1, 0)), dwk, dwv

    return jax.shard_map(local_step, mesh=mesh,
                         in_specs=(seq_spec, seq_spec, seq_spec, P(), P(), seq_spec),
                         out_specs=(seq_spec, seq_spec, seq_spec, seq_spec, P(), P()),
                         check_vma=False)
```
